32 devices in a mesh: dp: 32 (over z, y, x, core).
Axes of the slice: x: 2, y: 2, z: 4, core: 2. Of those that a mesh axis runs over, the one named last changes fastest.
Arguments:
- tokens: bfloat16 [8192, 1024], P('dp'), may hold values from -6 to 6
- cotangent: bfloat16 [8192, 1024], P('dp'), may hold values from -6 to 6
- lengths: int32 [64], P('dp'), may hold values from 64 to 128, as said below
- vectors: float32 [8, 1024], P(None, 'dp')
- bias_up: float32 [4096], P('dp'), may hold values from -3 to 3
- w_qkv: float32 [1024, 3072], P('dp')
- w_out: float32 [1024, 1024], P('dp'), may hold values from -0.5 to 0.5
- w_up: float32 [1024, 4096], P('dp'), may hold values from -0.1875 to 0.1875
- w_down: float32 [4096, 1024], P('dp'), may hold values from -0.09375 to 0.09375
- mom_vectors: float32 [2, 8, 1024], P(None, None, 'dp'), as said below
- mom_bias_up: float32 [2, 4096], P(None, 'dp'), as said below
- mom_qkv: float32 [2, 1024, 3072], P(None, 'dp'), as said below
- mom_out: float32 [2, 1024, 1024], P(None, 'dp'), as said below
- mom_up: float32 [2, 1024, 4096], P(None, 'dp'), as said below
- mom_down: float32 [2, 4096, 1024], P(None, 'dp'), as said below
Outputs:
- output: bfloat16 [8192, 1024], P('dp')
- input_grad: float32 [8192, 1024], P('dp')
- grad_vectors: float32 [8, 1024], P(None, 'dp')
- grad_bias_up: float32 [4096], P('dp')
- grad_qkv: float32 [1024, 3072], P('dp')
- grad_out: float32 [1024, 1024], P('dp')
- grad_up: float32 [1024, 4096], P('dp')
- grad_down: float32 [4096, 1024], P('dp')
- update_vectors: float32 [8, 1024], P(None, 'dp')
- update_bias_up: float32 [4096], P('dp')
- update_qkv: float32 [1024, 3072], P('dp')
- update_out: float32 [1024, 1024], P('dp')
- update_up: float32 [1024, 4096], P('dp')
- update_down: float32 [4096, 1024], P('dp')
- new_first_vectors: float32 [8, 1024], P(None, 'dp')
- new_first_bias_up: float32 [4096], P('dp')
- new_first_qkv: float32 [1024, 3072], P('dp')
- new_first_out: float32 [1024, 1024], P('dp')
- new_first_up: float32 [1024, 4096], P('dp')
- new_first_down: float32 [4096, 1024], P('dp')
- new_second_vectors: float32 [8, 1024], P(None, 'dp')
- new_second_bias_up: float32 [4096], P('dp')
- new_second_qkv: float32 [1024, 3072], P('dp')
- new_second_out: float32 [1024, 1024], P('dp')
- new_second_up: float32 [1024, 4096], P('dp')
- new_second_down: float32 [4096, 1024], P('dp')
The draws below stay inside these ranges and needn't reach their ends.
Inputs may be any that keep to these rules, and one draw needn't show every extreme that they name: `lengths`: some slot has exactly 128. `mom_vectors`: every second moment is positive. `mom_bias_up`: every second moment is positive. `mom_qkv`: every second moment is positive. `mom_out`: every second moment is positive. `mom_up`: every second moment is positive. `mom_down`: every second moment is positive.
All inputs are finite; a program needn't handle non-finite values.
Results may differ from the reference program's by a relative error of at most 0.02.
The reference program's roundings to bfloat16 on the way count: a program that leaves them out, or rounds other values in their place, can miss the bound.
Values may be sent and summed in bfloat16 or wider, within the bound.
A program may use at most 192 MiB of HBM per device.

```python
import math
import jax
import jax.numpy as jnp
from jax import lax

D = 1024
HEADS = 16
HEAD_DIM = 64
FF = 4096
MB_ROWS = 128
MICRO = 2
STEP = 3
SLOTS = 64
ROWS = 8192
N_DP = 32


def draw_lengths(key, part):
    base = jax.random.randint(key, (SLOTS,), MB_ROWS // 2, MB_ROWS + 1)
    where = jax.random.randint(jax.random.fold_in(key, 7), (), 0, SLOTS)
    return base.at[where].set(MB_ROWS).astype(jnp.int32)


def draw_vectors(key, part):
    noise = jax.random.normal(key, (8, D), jnp.float32)
    which = jnp.arange(8)[:, None]
    gain_rows = (which == 0) | (which == 5)
    return jnp.where(gain_rows, 1.0 + 0.15 * jnp.clip(noise, -3.0, 3.0), 0.5 * noise).astype(jnp.float32)


def draw_w_qkv(key, part):
    base = jax.random.normal(key, (D, 3 * D), jnp.float32) * D ** (-0.5)
    return base


def moment_pair(key, shape, factor):
    typical = factor * math.sqrt(ROWS)
    first = jax.random.normal(key, shape, jnp.float32)
    first = first * (typical / 9.0)
    spread = jnp.exp(jax.random.uniform(jax.random.fold_in(key, 11), shape, jnp.float32, math.log(0.25), math.log(4.0)))
    second = spread * (typical * typical / 19.0)
    return jnp.stack([first, second])


def draw_mom_vectors(key, part):
    return moment_pair(key, (8, D), 1.0)


def draw_mom_bias_up(key, part):
    return moment_pair(key, (FF,), 0.3)


def draw_mom_qkv(key, part):
    return moment_pair(key, (D, 3 * D), 0.2)


def draw_mom_out(key, part):
    return moment_pair(key, (D, D), 0.3)


def draw_mom_up(key, part):
    return moment_pair(key, (D, FF), 0.3)


def draw_mom_down(key, part):
    return moment_pair(key, (FF, D), 0.5)


def strengthened(entries, rng, source, target, shards_of, factor):
    def block_of(axis_at):
        return (jnp.arange(entries.shape[axis_at]) // (entries.shape[axis_at] // shards_of)).reshape((-1,) + (1,) * (entries.ndim - 1 - axis_at))

    near = jax.random.permutation(rng, shards_of)[block_of(target)]
    second = (block_of(target) + shards_of // 2) % shards_of
    return jnp.where((block_of(source) == near) | (block_of(source) == second), factor * entries, entries)


def steps_of(own_key, dims, pieces, smallest, high):
    level, own = 1.0, jax.random.fold_in(own_key, 6)
    for axis_at, shards_of in pieces:
        steps = jnp.exp(jax.random.uniform(jax.random.fold_in(own, axis_at), (shards_of,), jnp.float32, smallest / len(pieces), high / len(pieces)))
        level = level * jnp.repeat(steps, dims[axis_at] // shards_of).reshape([-1 if axis == axis_at else 1 for axis in range(len(dims))])
    return level


def scatter_about(rng, dims, scale, most, shards=(), kind=jnp.bfloat16):
    entries = scale * jax.random.normal(rng, dims, jnp.float32)
    if shards:
        entries = entries * steps_of(rng, dims, shards, -0.22, 0.18)
    return jnp.clip(entries, -most, most).astype(kind)


def gaussian_with(key, dims, width, reach, shards, heavy, held_as=jnp.bfloat16):
    entries = width * jax.random.normal(key, dims, jnp.float32)
    if shards:
        entries = entries * steps_of(key, dims, shards, -0.22, 0.18)
    return jnp.clip(strengthened(entries, jax.random.fold_in(key, 3), *heavy), -reach, reach).astype(held_as)


def setup_inputs(seed: int = 0) -> dict:
    arg_keys = jax.random.split(jax.random.key(seed), 16)
    return {
        "tokens": scatter_about(arg_keys[0], (ROWS, D), 1.0, 6.0, ((0, 32),)),
        "cotangent": gaussian_with(arg_keys[1], (ROWS, D), 1.0, 6.0, ((0, 32),), (0, 1, 32, 2.75)),
        "lengths": draw_lengths(jax.random.fold_in(arg_keys[15], 71), 0),
        "vectors": draw_vectors(jax.random.fold_in(arg_keys[15], 71), 0),
        "bias_up": scatter_about(arg_keys[4], (FF,), 0.5, 3.0, ((0, 32),), jnp.float32),
        "w_qkv": draw_w_qkv(jax.random.fold_in(arg_keys[15], 71), 0),
        "w_out": scatter_about(arg_keys[6], (D, D), (D // 8) ** -0.5, 0.5, ((0, 32),), jnp.float32),
        "w_up": scatter_about(arg_keys[7], (D, FF), D ** -0.5, 0.1875, ((0, 32),), jnp.float32),
        "w_down": scatter_about(arg_keys[8], (FF, D), FF ** -0.5, 0.09375, ((0, 32),), jnp.float32),
        "mom_vectors": draw_mom_vectors(jax.random.fold_in(arg_keys[15], 71), 0),
        "mom_bias_up": draw_mom_bias_up(jax.random.fold_in(arg_keys[15], 71), 0),
        "mom_qkv": draw_mom_qkv(jax.random.fold_in(arg_keys[15], 71), 0),
        "mom_out": draw_mom_out(jax.random.fold_in(arg_keys[15], 71), 0),
        "mom_up": draw_mom_up(jax.random.fold_in(arg_keys[15], 71), 0),
        "mom_down": draw_mom_down(jax.random.fold_in(arg_keys[15], 71), 0),
    }


ln_eps = 1e-05
gelu_c = math.sqrt(2.0 / math.pi)
beta_one = 0.9
beta_two = 0.95
decay_rate = 0.1
adam_eps = 1e-08

def matmul(left, right):
    return jnp.dot(left.astype(jnp.float32), right.astype(jnp.float32), precision=lax.Precision.HIGHEST)

def contract(form, left, right):
    return jnp.einsum(form, left.astype(jnp.float32), right.astype(jnp.float32), precision=lax.Precision.HIGHEST)

def layer_norm(values, gain, shift):
    centred = values - lax.optimization_barrier(jnp.mean(values, axis=-1, keepdims=True))
    rstd = lax.rsqrt(lax.optimization_barrier(jnp.mean(centred * centred, axis=-1, keepdims=True)) + ln_eps)
    normed = centred * rstd
    return (normed * gain + shift, normed, rstd)

def norm_back(grad_in, normed, rstd, gain):
    scaled = grad_in * gain
    inner = scaled - lax.optimization_barrier(jnp.mean(scaled, axis=-1, keepdims=True)) - normed * lax.optimization_barrier(jnp.mean(scaled * normed, axis=-1, keepdims=True))
    return rstd * inner

def gelu_pair(pre):
    tanh_val = jnp.tanh(gelu_c * (pre + 0.044715 * pre * pre * pre))
    value = 0.5 * pre * (1.0 + tanh_val)
    slope = 0.5 * (1.0 + tanh_val) + 0.5 * pre * (1.0 - tanh_val * tanh_val) * gelu_c * (1.0 + 3.0 * 0.044715 * pre * pre)
    return (value, slope)

def alibi_bias(rows):
    place = jnp.arange(rows)
    dist = (place[:, None] - place[None, :]).astype(jnp.float32)
    slopes = jnp.exp2(-8.0 * (jnp.arange(HEADS) + 1).astype(jnp.float32) / HEADS)
    bias = -slopes[:, None, None] * dist[None]
    return jnp.where(dist[None] >= 0, bias, -1e+30)

def block_pass(x_rows, grad_rows, weights, alibi):
    vec, up_bias, qkv_w, out_w, up_w, down_w = weights
    vecf = vec.astype(jnp.float32)
    rows = x_rows.shape[0]
    scale = 1.0 / math.sqrt(HEAD_DIM)
    xf = x_rows.astype(jnp.float32)
    ln_one, normed_one, rstd_one = layer_norm(xf, vecf[0], vecf[1])
    a_one = ln_one.astype(jnp.bfloat16)
    qkv = matmul(a_one, qkv_w)
    query = (qkv[:, :D] + vecf[2]).astype(jnp.bfloat16)
    keyx = qkv[:, D:2 * D].astype(jnp.bfloat16)
    value = (qkv[:, 2 * D:] + vecf[3]).astype(jnp.bfloat16)
    q3 = query.reshape(rows, HEADS, HEAD_DIM)
    k3 = keyx.reshape(rows, HEADS, HEAD_DIM)
    v3 = value.reshape(rows, HEADS, HEAD_DIM)
    scores = contract('qhd,khd->hqk', q3, k3) * scale + alibi
    top = lax.optimization_barrier(jnp.max(scores, axis=-1, keepdims=True))
    lse = top + jnp.log(lax.optimization_barrier(jnp.sum(jnp.exp(scores - top), axis=-1, keepdims=True)))
    probs_f = jnp.exp(scores - lse)
    probs = probs_f.astype(jnp.bfloat16)
    attn = contract('hqk,khd->qhd', probs, v3).reshape(rows, D).astype(jnp.bfloat16)
    h_one = xf + matmul(attn, out_w) + vecf[4]
    ln_two, normed_two, rstd_two = layer_norm(h_one, vecf[5], vecf[6])
    a_two = ln_two.astype(jnp.bfloat16)
    pre = matmul(a_two, up_w) + up_bias.astype(jnp.float32)
    act, slope = gelu_pair(pre)
    act_b = act.astype(jnp.bfloat16)
    out = (h_one + matmul(act_b, down_w) + vecf[7]).astype(jnp.bfloat16)
    dyf = grad_rows.astype(jnp.float32)
    g_bdown = lax.optimization_barrier(jnp.sum(dyf, axis=0))
    g_down = matmul(act_b.T, grad_rows)
    d_pre = matmul(grad_rows, down_w.T) * slope
    g_bup = lax.optimization_barrier(jnp.sum(d_pre, axis=0))
    d_pre_b = d_pre.astype(jnp.bfloat16)
    g_up = matmul(a_two.T, d_pre_b)
    d_a2 = matmul(d_pre_b, up_w.T)
    g_ln2g = lax.optimization_barrier(jnp.sum(d_a2 * normed_two, axis=0))
    g_ln2b = lax.optimization_barrier(jnp.sum(d_a2, axis=0))
    d_h1 = dyf + norm_back(d_a2, normed_two, rstd_two, vecf[5])
    g_bout = lax.optimization_barrier(jnp.sum(d_h1, axis=0))
    d_h1_b = d_h1.astype(jnp.bfloat16)
    g_out = matmul(attn.T, d_h1_b)
    d_attn = matmul(d_h1_b, out_w.T).astype(jnp.bfloat16)
    do3 = d_attn.reshape(rows, HEADS, HEAD_DIM)
    d_v = contract('hqk,qhd->khd', probs, do3).reshape(rows, D)
    d_probs = contract('qhd,khd->hqk', do3, v3)
    delta = lax.optimization_barrier(jnp.sum(do3.astype(jnp.float32) * attn.reshape(rows, HEADS, HEAD_DIM).astype(jnp.float32), axis=-1)).T[:, :, None]
    d_scores = (probs_f * (d_probs - delta)).astype(jnp.bfloat16)
    d_q = (contract('hqk,khd->qhd', d_scores, k3) * scale).reshape(rows, D)
    d_k = (contract('hqk,qhd->khd', d_scores, q3) * scale).reshape(rows, D)
    g_bq = lax.optimization_barrier(jnp.sum(d_q, axis=0))
    g_bv = lax.optimization_barrier(jnp.sum(d_v, axis=0))
    d_qkv = jnp.concatenate([d_q, d_k, d_v], axis=1).astype(jnp.bfloat16)
    g_qkv = matmul(a_one.T, d_qkv)
    d_a1 = matmul(d_qkv, qkv_w.T)
    g_ln1g = lax.optimization_barrier(jnp.sum(d_a1 * normed_one, axis=0))
    g_ln1b = lax.optimization_barrier(jnp.sum(d_a1, axis=0))
    d_x = d_h1 + norm_back(d_a1, normed_one, rstd_one, vecf[0])
    g_vec = jnp.stack([g_ln1g, g_ln1b, g_bq, g_bv, g_bout, g_ln2g, g_ln2b, g_bdown])
    return (out, d_x, (g_vec, g_bup, g_qkv, g_out, g_up, g_down))

def adamw(param, moments, grad, count):
    first = beta_one * moments[0] + (1.0 - beta_one) * grad
    second = beta_two * moments[1] + (1.0 - beta_two) * grad * grad
    corr_one = 1.0 - beta_one ** count
    corr_two = 1.0 - beta_two ** count
    update = first / corr_one / (jnp.sqrt(second / corr_two) + adam_eps) + decay_rate * param
    return (update, first, second)

def reference(tokens, cotangent, lengths, vectors, bias_up, w_qkv, w_out, w_up, w_down, mom_vectors, mom_bias_up, mom_qkv, mom_out, mom_up, mom_down):
    params = (vectors, bias_up, w_qkv, w_out, w_up, w_down)
    moments = (mom_vectors, mom_bias_up, mom_qkv, mom_out, mom_up, mom_down)
    low = tuple((p.astype(jnp.bfloat16) for p in params))
    alibi = alibi_bias(MB_ROWS)
    x_blocks = tokens.reshape(N_DP * MICRO, MB_ROWS, D)
    dy_blocks = cotangent.reshape(N_DP * MICRO, MB_ROWS, D)
    place = jnp.arange(MB_ROWS).astype(jnp.int32)

    def step_block(carry, item):
        x_rows, dy_rows, length = item
        live = place < length
        grad_rows = jnp.where(live[:, None], dy_rows, jnp.zeros((), jnp.bfloat16))
        out, d_x, grads = block_pass(x_rows, grad_rows, low, alibi)
        carry = tuple((a + b for a, b in zip(carry, grads)))
        return (carry, (out, d_x))
    init = tuple((jnp.zeros(p.shape, jnp.float32) for p in params))
    grads, (outs, dxs) = lax.scan(step_block, init, (x_blocks, dy_blocks, lengths))
    count = float(STEP)
    news = [adamw(p.astype(jnp.float32), m, g, count) for p, m, g in zip(params, moments, grads)]
    output = outs.reshape(ROWS, D)
    input_grad = dxs.reshape(ROWS, D)
    return (output, input_grad, grads[0], grads[1], grads[2], grads[3], grads[4], grads[5], news[0][0], news[1][0], news[2][0], news[3][0], news[4][0], news[5][0], news[0][1], news[1][1], news[2][1], news[3][1], news[4][1], news[5][1], news[0][2], news[1][2], news[2][2], news[3][2], news[4][2], news[5][2])
```

```python
import functools
import math

import jax
import jax.numpy as jnp
from jax import lax
from jax.experimental import pallas as pl
from jax.experimental.pallas import tpu as pltpu
from jax.sharding import PartitionSpec as P

D = 1024
HEADS = 16
HEAD_DIM = 64
MB_ROWS = 128
MICRO = 2
STEP = 3


ln_eps = 1e-05
gelu_c = math.sqrt(2.0 / math.pi)
beta_one = 0.9
beta_two = 0.95
decay_rate = 0.1
adam_eps = 1e-08


def product(left, right):
    return jnp.dot(left, right, preferred_element_type=jnp.float32)


def contract(form, left, right):
    return jnp.einsum(form, left, right, preferred_element_type=jnp.float32)


def layer_norm(values, gain, shift):
    centred = values - jnp.mean(values, axis=-1, keepdims=True)
    rstd = lax.rsqrt(jnp.mean(centred * centred, axis=-1, keepdims=True) + ln_eps)
    normed = centred * rstd
    return (normed * gain + shift, normed, rstd)


def norm_back(grad_in, normed, rstd, gain):
    scaled = grad_in * gain
    inner = (
        scaled
        - jnp.mean(scaled, axis=-1, keepdims=True)
        - normed * jnp.mean(scaled * normed, axis=-1, keepdims=True)
    )
    return rstd * inner


def gelu_pair(pre):
    tanh_val = jnp.tanh(gelu_c * (pre + 0.044715 * pre * pre * pre))
    value = 0.5 * pre * (1.0 + tanh_val)
    slope = 0.5 * (1.0 + tanh_val) + 0.5 * pre * (1.0 - tanh_val * tanh_val) * gelu_c * (
        1.0 + 3.0 * 0.044715 * pre * pre
    )
    return (value, slope)


def alibi_bias(rows):
    place = jnp.arange(rows)
    dist = (place[:, None] - place[None, :]).astype(jnp.float32)
    slopes = jnp.exp2(-8.0 * (jnp.arange(HEADS) + 1).astype(jnp.float32) / HEADS)
    bias = -slopes[:, None, None] * dist[None]
    return jnp.where(dist[None] >= 0, bias, -1e30)


def attention_scores(q3, k3, alibi):
    return contract("qhd,khd->hqk", q3, k3) * (1.0 / math.sqrt(HEAD_DIM)) + alibi


def forward_block(x_rows, weights, alibi):
    vec, up_bias, qkv_w, out_w, up_w, down_w = weights
    vecf = vec.astype(jnp.float32)
    rows = x_rows.shape[0]
    xf = x_rows.astype(jnp.float32)
    ln_one, normed_one, rstd_one = layer_norm(xf, vecf[0], vecf[1])
    a_one = ln_one.astype(jnp.bfloat16)
    qkv = product(a_one, qkv_w)
    query = (qkv[:, :D] + vecf[2]).astype(jnp.bfloat16).reshape(rows, HEADS, HEAD_DIM)
    keyx = qkv[:, D : 2 * D].astype(jnp.bfloat16).reshape(rows, HEADS, HEAD_DIM)
    value = (qkv[:, 2 * D :] + vecf[3]).astype(jnp.bfloat16).reshape(rows, HEADS, HEAD_DIM)
    scores = attention_scores(query, keyx, alibi)
    top = jnp.max(scores, axis=-1, keepdims=True)
    lse = top + jnp.log(jnp.sum(jnp.exp(scores - top), axis=-1, keepdims=True))
    probs = jnp.exp(scores - lse).astype(jnp.bfloat16)
    attn = contract("hqk,khd->qhd", probs, value).reshape(rows, D).astype(jnp.bfloat16)
    h_one = xf + product(attn, out_w) + vecf[4]
    ln_two, normed_two, rstd_two = layer_norm(h_one, vecf[5], vecf[6])
    a_two = ln_two.astype(jnp.bfloat16)
    pre = product(a_two, up_w) + up_bias.astype(jnp.float32)
    act, slope = gelu_pair(pre)
    act_b = act.astype(jnp.bfloat16)
    out = (h_one + product(act_b, down_w) + vecf[7]).astype(jnp.bfloat16)
    saved = (
        normed_one,
        rstd_one,
        a_one,
        query,
        keyx,
        value,
        lse,
        attn,
        normed_two,
        rstd_two,
        a_two,
        slope,
        act_b,
    )
    return (out, saved)


def backward_block(saved, grad_rows, weights, alibi):
    vec, up_bias, qkv_w, out_w, up_w, down_w = weights
    vecf = vec.astype(jnp.float32)
    (
        normed_one,
        rstd_one,
        a_one,
        query,
        keyx,
        value,
        lse,
        attn,
        normed_two,
        rstd_two,
        a_two,
        slope,
        act_b,
    ) = saved
    rows = grad_rows.shape[0]
    scale = 1.0 / math.sqrt(HEAD_DIM)
    dyf = grad_rows.astype(jnp.float32)
    g_bdown = jnp.sum(dyf, axis=0)
    g_down = product(act_b.T, grad_rows)
    d_pre = product(grad_rows, down_w.T) * slope
    g_bup = jnp.sum(d_pre, axis=0)
    d_pre_b = d_pre.astype(jnp.bfloat16)
    g_up = product(a_two.T, d_pre_b)
    d_a2 = product(d_pre_b, up_w.T)
    g_ln2g = jnp.sum(d_a2 * normed_two, axis=0)
    g_ln2b = jnp.sum(d_a2, axis=0)
    d_h1 = dyf + norm_back(d_a2, normed_two, rstd_two, vecf[5])
    g_bout = jnp.sum(d_h1, axis=0)
    d_h1_b = d_h1.astype(jnp.bfloat16)
    g_out = product(attn.T, d_h1_b)
    d_attn = product(d_h1_b, out_w.T).astype(jnp.bfloat16).reshape(rows, HEADS, HEAD_DIM)
    probs_f = jnp.exp(attention_scores(query, keyx, alibi) - lse)
    probs = probs_f.astype(jnp.bfloat16)
    d_v = contract("hqk,qhd->khd", probs, d_attn).reshape(rows, D)
    d_probs = contract("qhd,khd->hqk", d_attn, value)
    delta = jnp.sum(
        d_attn.astype(jnp.float32) * attn.reshape(rows, HEADS, HEAD_DIM).astype(jnp.float32),
        axis=-1,
    ).T[:, :, None]
    d_scores = (probs_f * (d_probs - delta)).astype(jnp.bfloat16)
    d_q = (contract("hqk,khd->qhd", d_scores, keyx) * scale).reshape(rows, D)
    d_k = (contract("hqk,qhd->khd", d_scores, query) * scale).reshape(rows, D)
    g_bq = jnp.sum(d_q, axis=0)
    g_bv = jnp.sum(d_v, axis=0)
    d_qkv = jnp.concatenate([d_q, d_k, d_v], axis=1).astype(jnp.bfloat16)
    g_qkv = product(a_one.T, d_qkv)
    d_a1 = product(d_qkv, qkv_w.T)
    g_ln1g = jnp.sum(d_a1 * normed_one, axis=0)
    g_ln1b = jnp.sum(d_a1, axis=0)
    d_x = d_h1 + norm_back(d_a1, normed_one, rstd_one, vecf[0])
    g_vec = jnp.stack([g_ln1g, g_ln1b, g_bq, g_bv, g_bout, g_ln2g, g_ln2b, g_bdown])
    return (d_x, (g_vec, g_bup, g_qkv, g_out, g_up, g_down))


def adamw(param, moments, grad, count):
    first = beta_one * moments[0] + (1.0 - beta_one) * grad
    second = beta_two * moments[1] + (1.0 - beta_two) * grad * grad
    corr_one = 1.0 - beta_one**count
    corr_two = 1.0 - beta_two**count
    update = first / corr_one / (jnp.sqrt(second / corr_two) + adam_eps) + decay_rate * param
    return (update, first, second)


MESH_ID = pl.DeviceIdType.MESH


def grid_of(count):
    known = {32: (4, 2, 2), 128: (4, 4, 4)}
    return known.get(count, (count // 2,))


def locate(me, sizes):
    rest, coords = me // 2, []
    for size in reversed(sizes):
        coords.append(rest % size)
        rest = rest // size
    return tuple(reversed(coords)), me % 2


def device_at(coords, core, sizes):
    index = 0
    for value, size in zip(coords, sizes):
        index = index * size + value
    return index * 2 + core


def swapped(coords, dim, value):
    return tuple(value if at == dim else old for at, old in enumerate(coords))


def neighbours(coords, core, sizes):
    found = [device_at(coords, 1 - core, sizes)]
    for dim, size in enumerate(sizes):
        for step in range(1, size):
            found.append(device_at(swapped(coords, dim, (coords[dim] + step) % size), core, sizes))
    return found


def greet(others):
    barrier = pltpu.get_barrier_semaphore()
    for other in others:
        pl.semaphore_signal(barrier, inc=1, device_id=(other,), device_id_type=MESH_ID)
    pl.semaphore_wait(barrier, len(others))


class Sems:
    def __init__(self, send, recv):
        self.send, self.recv, self.used = send, recv, 0

    def pair(self):
        at = self.used
        self.used += 1
        return self.send.at[at], self.recv.at[at]


def remote(sems, src, dst, target):
    send_sem, recv_sem = sems.pair()
    copy = pltpu.make_async_remote_copy(
        src_ref=src, dst_ref=dst, send_sem=send_sem, recv_sem=recv_sem,
        device_id=(target,), device_id_type=MESH_ID,
    )
    copy.start()
    return copy


class Gather:
    def __init__(self, full, colours, sizes, coords, core, sems):
        self.full, self.colours, self.sizes = full, colours, sizes
        self.coords, self.core, self.sems = coords, core, sems
        self.axis = [[] for _ in colours]
        self.swap = []
        self.sent = []

    def view(self, colour, fixed):
        start, width, _ = colour
        place = tuple(fixed.get(dim, slice(None)) for dim in range(len(self.sizes)))
        return self.full.at[(*place, self.core, slice(None), pl.ds(start, width))]

    def start(self, stage, own=None):
        for at, colour in enumerate(self.colours):
            order = colour[2]
            dim = order[stage]
            fixed = {d: self.coords[d] for d in order[stage:]}
            held = self.view(colour, fixed)
            source = held if own is None else own.at[:, pl.ds(colour[0], colour[1])]
            self.axis[at] = []
            for step in range(1, self.sizes[dim]):
                peer = swapped(self.coords, dim, (self.coords[dim] + step) % self.sizes[dim])
                self.axis[at].append(remote(self.sems, source, held, device_at(peer, self.core, self.sizes)))
            self.sent += self.axis[at]

    def land(self, stage):
        partner = device_at(self.coords, 1 - self.core, self.sizes)
        for at, colour in enumerate(self.colours):
            order = colour[2]
            dim = order[stage]
            for copy in self.axis[at]:
                copy.wait_recv()
            fixed = {d: self.coords[d] for d in order[stage + 1:]}
            if stage == 0:
                views = [self.view(colour, fixed)]
            else:
                views = [
                    self.view(colour, {**fixed, dim: (self.coords[dim] + step) % self.sizes[dim]})
                    for step in range(1, self.sizes[dim])
                ]
            for view in views:
                self.swap.append(remote(self.sems, view, view, partner))

    def finish(self):
        for copy in self.swap:
            copy.wait_recv()

    def drain(self):
        for copy in self.sent + self.swap:
            copy.wait_send()


def colours_of(columns, sizes):
    last = len(sizes) - 1
    if last < 2:
        return [(0, columns, tuple(range(len(sizes))))]
    tiles = columns // 128
    if tiles < 8:
        return [(0, columns, (0, 1, 2))]
    third = max(1, tiles // 8)
    first = (tiles - third) // 2
    second = tiles - third - first
    return [
        (0, first * 128, (0, 1, 2)),
        (first * 128, second * 128, (0, 2, 1)),
        ((first + second) * 128, third * 128, (2, 1, 0)),
    ]


def gather_kernel(sizes, count, *refs):
    shards, fulls = refs[:count], refs[count : 2 * count]
    owns = refs[2 * count : 3 * count]
    send_sem, recv_sem, local_sem = refs[3 * count :]
    coords, core = locate(lax.axis_index("dp"), sizes)
    for shard, own in zip(shards, owns):
        own[...] = shard[...].astype(own.dtype)
    greet(neighbours(coords, core, sizes))
    sems = Sems(send_sem, recv_sem)
    items = [
        Gather(full, colours_of(full.shape[-1], sizes), sizes, coords, core, sems) for full in fulls
    ]
    local = []
    for at, (own, full) in enumerate(zip(owns, fulls)):
        copy = pltpu.make_async_copy(own, full.at[(*coords, core)], local_sem.at[at])
        copy.start()
        local.append(copy)
    stages = len(sizes)
    items[0].start(0, owns[0])
    for turn in range(count + stages):
        for stage in range(stages):
            at = turn - stage
            if 0 <= at < count:
                if stage == 0:
                    if at + 1 < count:
                        items[at + 1].start(0, owns[at + 1])
                    local[at].wait()
                items[at].land(stage)
                if stage + 1 < stages:
                    items[at].start(stage + 1)
        at = turn - stages
        if 0 <= at < count:
            items[at].finish()
    for item in items:
        item.drain()


def gather_all(shards, count):
    sizes = grid_of(count)
    copies = 400
    n = len(shards)
    fulls = pl.pallas_call(
        functools.partial(gather_kernel, sizes, n),
        out_shape=[jax.ShapeDtypeStruct((*sizes, 2, *s.shape), jnp.bfloat16) for s in shards],
        in_specs=[pl.BlockSpec(memory_space=pltpu.VMEM)] * n,
        out_specs=[pl.BlockSpec(memory_space=pltpu.HBM)] * n,
        scratch_shapes=[pltpu.VMEM(s.shape, jnp.bfloat16) for s in shards]
        + [pltpu.SemaphoreType.DMA((copies,)), pltpu.SemaphoreType.DMA((copies,)), pltpu.SemaphoreType.DMA((n,))],
        compiler_params=pltpu.CompilerParams(collective_id=0, has_side_effects=True),
        name="gather_all",
    )(*shards)
    return [full.reshape(-1, *full.shape[-2:]) for full in fulls]


def small_block(vectors, bias_up, me):
    wide = jnp.zeros((8, 128), jnp.float32)
    width = vectors.shape[1]
    per = 128 // width
    wide = lax.dynamic_update_slice(wide, vectors, (0, (me % per) * width))
    tail = jnp.zeros((8, 128), jnp.float32)
    span = bias_up.shape[0]
    tail = lax.dynamic_update_slice(tail, bias_up[None, :], (0, (me % (128 // span)) * span))
    return jnp.concatenate([wide, tail], axis=0)


def small_parts(small, vectors, bias_up):
    per = 128 // vectors.shape[1]
    span = 128 // bias_up.shape[0]
    n = small.shape[0]
    vec = jnp.sum(small[:, :8].astype(jnp.float32).reshape(n // per, per, 8, 128), axis=1)
    bias = jnp.sum(small[:, 8].astype(jnp.float32).reshape(n // span, span, 128), axis=1)
    return vec.transpose(1, 0, 2).reshape(8, -1).astype(jnp.bfloat16), bias.reshape(-1).astype(jnp.bfloat16)


def body(
    tokens,
    cotangent,
    lengths,
    vectors,
    bias_up,
    w_qkv,
    w_out,
    w_up,
    w_down,
    mom_vectors,
    mom_bias_up,
    mom_qkv,
    mom_out,
    mom_up,
    mom_down,
):
    params = (vectors, bias_up, w_qkv, w_out, w_up, w_down)
    moments = (mom_vectors, mom_bias_up, mom_qkv, mom_out, mom_up, mom_down)
    me = lax.axis_index("dp")
    count = lax.axis_size("dp")
    small, full_out, full_qkv, full_up, full_down = gather_all(
        [small_block(vectors, bias_up, me), w_out, w_qkv, w_up, w_down], count
    )
    vec_low, bias_low = small_parts(small, vectors, bias_up)
    weights = (
        vec_low,
        bias_low,
        full_qkv.reshape(-1, w_qkv.shape[1]),
        full_out.reshape(-1, w_out.shape[1]),
        full_up.reshape(-1, w_up.shape[1]),
        full_down.reshape(-1, w_down.shape[1]),
    )
    alibi = alibi_bias(MB_ROWS)
    place = jnp.arange(MB_ROWS)
    owned = tuple((jnp.zeros(p.shape, jnp.float32) for p in params))
    summed = None
    out_list = []
    dx_list = []
    for micro in range(MICRO):
        x_rows = tokens[micro * MB_ROWS : (micro + 1) * MB_ROWS]
        live = place < lengths[micro]
        grad_rows = jnp.where(
            live[:, None],
            cotangent[micro * MB_ROWS : (micro + 1) * MB_ROWS],
            jnp.zeros((), jnp.bfloat16),
        )
        out, saved = forward_block(x_rows, weights, alibi)
        d_x, grads = backward_block(saved, grad_rows, weights, alibi)
        out_list.append(out)
        dx_list.append(d_x)
        summed = grads if summed is None else tuple((a + b for a, b in zip(summed, grads)))
    owned = (
        lax.psum_scatter(summed[0], "dp", scatter_dimension=1, tiled=True),
        lax.psum_scatter(summed[1], "dp", scatter_dimension=0, tiled=True),
        lax.psum_scatter(summed[2], "dp", scatter_dimension=0, tiled=True),
        lax.psum_scatter(summed[3], "dp", scatter_dimension=0, tiled=True),
        lax.psum_scatter(summed[4], "dp", scatter_dimension=0, tiled=True),
        lax.psum_scatter(summed[5], "dp", scatter_dimension=0, tiled=True),
    )
    count = float(STEP)
    news = [adamw(p, m, g, count) for p, m, g in zip(params, moments, owned)]
    output = jnp.concatenate(out_list, axis=0)
    input_grad = jnp.concatenate(dx_list, axis=0)
    return (
        output,
        input_grad,
        owned[0],
        owned[1],
        owned[2],
        owned[3],
        owned[4],
        owned[5],
        news[0][0],
        news[1][0],
        news[2][0],
        news[3][0],
        news[4][0],
        news[5][0],
        news[0][1],
        news[1][1],
        news[2][1],
        news[3][1],
        news[4][1],
        news[5][1],
        news[0][2],
        news[1][2],
        news[2][2],
        news[3][2],
        news[4][2],
        news[5][2],
    )


def solution(mesh):
    in_specs = (
        P("dp", None),
        P("dp", None),
        P("dp"),
        P(None, "dp"),
        P("dp"),
        P("dp", None),
        P("dp", None),
        P("dp", None),
        P("dp", None),
        P(None, None, "dp"),
        P(None, "dp"),
        P(None, "dp", None),
        P(None, "dp", None),
        P(None, "dp", None),
        P(None, "dp", None),
    )
    out_specs = (
        P("dp", None),
        P("dp", None),
        P(None, "dp"),
        P("dp"),
        P("dp", None),
        P("dp", None),
        P("dp", None),
        P("dp", None),
        P(None, "dp"),
        P("dp"),
        P("dp", None),
        P("dp", None),
        P("dp", None),
        P("dp", None),
        P(None, "dp"),
        P("dp"),
        P("dp", None),
        P("dp", None),
        P("dp", None),
        P("dp", None),
        P(None, "dp"),
        P("dp"),
        P("dp", None),
        P("dp", None),
        P("dp", None),
        P("dp", None),
    )
    return jax.shard_map(body, mesh=mesh, in_specs=in_specs, out_specs=out_specs, check_vma=False)
```

```python
import functools
import math

import jax
import jax.numpy as jnp
from jax import lax
from jax.experimental import pallas as pl
from jax.experimental.pallas import tpu as pltpu
from jax.sharding import PartitionSpec as P

D = 1024
HEADS = 16
HEAD_DIM = 64
MB_ROWS = 128
MICRO = 2
STEP = 3


ln_eps = 1e-05
gelu_c = math.sqrt(2.0 / math.pi)
beta_one = 0.9
beta_two = 0.95
decay_rate = 0.1
adam_eps = 1e-08


def product(left, right):
    return jnp.dot(left, right, preferred_element_type=jnp.float32)


def contract(form, left, right):
    return jnp.einsum(form, left, right, preferred_element_type=jnp.float32)


def layer_norm(values, gain, shift):
    centred = values - jnp.mean(values, axis=-1, keepdims=True)
    rstd = lax.rsqrt(jnp.mean(centred * centred, axis=-1, keepdims=True) + ln_eps)
    normed = centred * rstd
    return (normed * gain + shift, normed, rstd)


def norm_back(grad_in, normed, rstd, gain):
    scaled = grad_in * gain
    inner = (
        scaled
        - jnp.mean(scaled, axis=-1, keepdims=True)
        - normed * jnp.mean(scaled * normed, axis=-1, keepdims=True)
    )
    return rstd * inner


def gelu_pair(pre):
    tanh_val = jnp.tanh(gelu_c * (pre + 0.044715 * pre * pre * pre))
    value = 0.5 * pre * (1.0 + tanh_val)
    slope = 0.5 * (1.0 + tanh_val) + 0.5 * pre * (1.0 - tanh_val * tanh_val) * gelu_c * (
        1.0 + 3.0 * 0.044715 * pre * pre
    )
    return (value, slope)


def alibi_bias(rows):
    place = jnp.arange(rows)
    dist = (place[:, None] - place[None, :]).astype(jnp.float32)
    slopes = jnp.exp2(-8.0 * (jnp.arange(HEADS) + 1).astype(jnp.float32) / HEADS)
    bias = -slopes[:, None, None] * dist[None]
    return jnp.where(dist[None] >= 0, bias, -1e30)


def attention_scores(q3, k3, alibi):
    return contract("qhd,khd->hqk", q3, k3) * (1.0 / math.sqrt(HEAD_DIM)) + alibi


def forward_block(x_rows, weights, alibi):
    vec, up_bias, qkv_w, out_w, up_w, down_w = weights
    vecf = vec.astype(jnp.float32)
    rows = x_rows.shape[0]
    xf = x_rows.astype(jnp.float32)
    ln_one, normed_one, rstd_one = layer_norm(xf, vecf[0], vecf[1])
    a_one = ln_one.astype(jnp.bfloat16)
    qkv = product(a_one, qkv_w)
    query = (qkv[:, :D] + vecf[2]).astype(jnp.bfloat16).reshape(rows, HEADS, HEAD_DIM)
    keyx = qkv[:, D : 2 * D].astype(jnp.bfloat16).reshape(rows, HEADS, HEAD_DIM)
    value = (qkv[:, 2 * D :] + vecf[3]).astype(jnp.bfloat16).reshape(rows, HEADS, HEAD_DIM)
    scores = attention_scores(query, keyx, alibi)
    top = jnp.max(scores, axis=-1, keepdims=True)
    lse = top + jnp.log(jnp.sum(jnp.exp(scores - top), axis=-1, keepdims=True))
    probs = jnp.exp(scores - lse).astype(jnp.bfloat16)
    attn = contract("hqk,khd->qhd", probs, value).reshape(rows, D).astype(jnp.bfloat16)
    h_one = xf + product(attn, out_w) + vecf[4]
    ln_two, normed_two, rstd_two = layer_norm(h_one, vecf[5], vecf[6])
    a_two = ln_two.astype(jnp.bfloat16)
    pre = product(a_two, up_w) + up_bias.astype(jnp.float32)
    act, slope = gelu_pair(pre)
    act_b = act.astype(jnp.bfloat16)
    out = (h_one + product(act_b, down_w) + vecf[7]).astype(jnp.bfloat16)
    saved = (
        normed_one,
        rstd_one,
        a_one,
        query,
        keyx,
        value,
        lse,
        attn,
        normed_two,
        rstd_two,
        a_two,
        slope,
        act_b,
    )
    return (out, saved)


def backward_block(saved, grad_rows, weights, alibi):
    vec, up_bias, qkv_w, out_w, up_w, down_w = weights
    vecf = vec.astype(jnp.float32)
    (
        normed_one,
        rstd_one,
        a_one,
        query,
        keyx,
        value,
        lse,
        attn,
        normed_two,
        rstd_two,
        a_two,
        slope,
        act_b,
    ) = saved
    rows = grad_rows.shape[0]
    scale = 1.0 / math.sqrt(HEAD_DIM)
    dyf = grad_rows.astype(jnp.float32)
    g_bdown = jnp.sum(dyf, axis=0)
    g_down = product(act_b.T, grad_rows)
    d_pre = product(grad_rows, down_w.T) * slope
    g_bup = jnp.sum(d_pre, axis=0)
    d_pre_b = d_pre.astype(jnp.bfloat16)
    g_up = product(a_two.T, d_pre_b)
    d_a2 = product(d_pre_b, up_w.T)
    g_ln2g = jnp.sum(d_a2 * normed_two, axis=0)
    g_ln2b = jnp.sum(d_a2, axis=0)
    d_h1 = dyf + norm_back(d_a2, normed_two, rstd_two, vecf[5])
    g_bout = jnp.sum(d_h1, axis=0)
    d_h1_b = d_h1.astype(jnp.bfloat16)
    g_out = product(attn.T, d_h1_b)
    d_attn = product(d_h1_b, out_w.T).astype(jnp.bfloat16).reshape(rows, HEADS, HEAD_DIM)
    probs_f = jnp.exp(attention_scores(query, keyx, alibi) - lse)
    probs = probs_f.astype(jnp.bfloat16)
    d_v = contract("hqk,qhd->khd", probs, d_attn).reshape(rows, D)
    d_probs = contract("qhd,khd->hqk", d_attn, value)
    delta = jnp.sum(
        d_attn.astype(jnp.float32) * attn.reshape(rows, HEADS, HEAD_DIM).astype(jnp.float32),
        axis=-1,
    ).T[:, :, None]
    d_scores = (probs_f * (d_probs - delta)).astype(jnp.bfloat16)
    d_q = (contract("hqk,khd->qhd", d_scores, keyx) * scale).reshape(rows, D)
    d_k = (contract("hqk,qhd->khd", d_scores, query) * scale).reshape(rows, D)
    g_bq = jnp.sum(d_q, axis=0)
    g_bv = jnp.sum(d_v, axis=0)
    d_qkv = jnp.concatenate([d_q, d_k, d_v], axis=1).astype(jnp.bfloat16)
    g_qkv = product(a_one.T, d_qkv)
    d_a1 = product(d_qkv, qkv_w.T)
    g_ln1g = jnp.sum(d_a1 * normed_one, axis=0)
    g_ln1b = jnp.sum(d_a1, axis=0)
    d_x = d_h1 + norm_back(d_a1, normed_one, rstd_one, vecf[0])
    g_vec = jnp.stack([g_ln1g, g_ln1b, g_bq, g_bv, g_bout, g_ln2g, g_ln2b, g_bdown])
    return (d_x, (g_vec, g_bup, g_qkv, g_out, g_up, g_down))


def adamw(param, moments, grad, count):
    first = beta_one * moments[0] + (1.0 - beta_one) * grad
    second = beta_two * moments[1] + (1.0 - beta_two) * grad * grad
    corr_one = 1.0 - beta_one**count
    corr_two = 1.0 - beta_two**count
    update = first / corr_one / (jnp.sqrt(second / corr_two) + adam_eps) + decay_rate * param
    return (update, first, second)


MESH_ID = pl.DeviceIdType.MESH


def grid_of(count):
    known = {32: (4, 2, 2), 128: (4, 4, 4)}
    return known.get(count, (count // 2,))


def locate(me, sizes):
    rest, coords = me // 2, []
    for size in reversed(sizes):
        coords.append(rest % size)
        rest = rest // size
    return tuple(reversed(coords)), me % 2


def device_at(coords, core, sizes):
    index = 0
    for value, size in zip(coords, sizes):
        index = index * size + value
    return index * 2 + core


def swapped(coords, dim, value):
    return tuple(value if at == dim else old for at, old in enumerate(coords))


def neighbours(coords, core, sizes):
    found = [device_at(coords, 1 - core, sizes)]
    for dim, size in enumerate(sizes):
        for step in range(1, size):
            found.append(device_at(swapped(coords, dim, (coords[dim] + step) % size), core, sizes))
    return found


def greet(others):
    barrier = pltpu.get_barrier_semaphore()
    for other in others:
        pl.semaphore_signal(barrier, inc=1, device_id=(other,), device_id_type=MESH_ID)
    pl.semaphore_wait(barrier, len(others))


class Sems:
    def __init__(self, send, recv):
        self.send, self.recv, self.used = send, recv, 0

    def pair(self):
        at = self.used
        self.used += 1
        return self.send.at[at], self.recv.at[at]


def remote(sems, src, dst, target):
    send_sem, recv_sem = sems.pair()
    copy = pltpu.make_async_remote_copy(
        src_ref=src, dst_ref=dst, send_sem=send_sem, recv_sem=recv_sem,
        device_id=(target,), device_id_type=MESH_ID,
    )
    copy.start()
    return copy


class Gather:
    def __init__(self, full, colours, sizes, coords, core, sems):
        self.full, self.colours, self.sizes = full, colours, sizes
        self.coords, self.core, self.sems = coords, core, sems
        self.axis = [[] for _ in colours]
        self.swap = []
        self.sent = []

    def view(self, colour, fixed):
        start, width, _ = colour
        place = tuple(fixed.get(dim, slice(None)) for dim in range(len(self.sizes)))
        return self.full.at[(*place, self.core, slice(None), pl.ds(start, width))]

    def start(self, stage, own=None):
        for at, colour in enumerate(self.colours):
            order = colour[2]
            dim = order[stage]
            fixed = {d: self.coords[d] for d in order[stage:]}
            held = self.view(colour, fixed)
            source = held if own is None else own.at[:, pl.ds(colour[0], colour[1])]
            self.axis[at] = []
            for step in range(1, self.sizes[dim]):
                peer = swapped(self.coords, dim, (self.coords[dim] + step) % self.sizes[dim])
                self.axis[at].append(remote(self.sems, source, held, device_at(peer, self.core, self.sizes)))
            self.sent += self.axis[at]

    def land(self, stage):
        partner = device_at(self.coords, 1 - self.core, self.sizes)
        for at, colour in enumerate(self.colours):
            order = colour[2]
            dim = order[stage]
            for copy in self.axis[at]:
                copy.wait_recv()
            fixed = {d: self.coords[d] for d in order[stage + 1:]}
            if stage == 0:
                views = [self.view(colour, fixed)]
            else:
                views = [
                    self.view(colour, {**fixed, dim: (self.coords[dim] + step) % self.sizes[dim]})
                    for step in range(1, self.sizes[dim])
                ]
            for view in views:
                self.swap.append(remote(self.sems, view, view, partner))

    def finish(self):
        for copy in self.swap:
            copy.wait_recv()

    def drain(self):
        for copy in self.sent + self.swap:
            copy.wait_send()


def colours_of(columns, sizes):
    last = len(sizes) - 1
    if last < 2:
        return [(0, columns, tuple(range(len(sizes))))]
    tiles = columns // 128
    if tiles < 8:
        return [(0, columns, (0, 1, 2))]
    third = max(1, tiles // 8)
    first = (tiles - third) // 2
    second = tiles - third - first
    return [
        (0, first * 128, (0, 1, 2)),
        (first * 128, second * 128, (0, 2, 1)),
        ((first + second) * 128, third * 128, (2, 1, 0)),
    ]


def gather_kernel(sizes, count, *refs):
    shards, fulls = refs[:count], refs[count : 2 * count]
    owns = refs[2 * count : 3 * count]
    send_sem, recv_sem, local_sem = refs[3 * count :]
    coords, core = locate(lax.axis_index("dp"), sizes)
    for shard, own in zip(shards, owns):
        own[...] = shard[...].astype(own.dtype)
    greet(neighbours(coords, core, sizes))
    sems = Sems(send_sem, recv_sem)
    items = [
        Gather(full, colours_of(full.shape[-1], sizes), sizes, coords, core, sems) for full in fulls
    ]
    local = []
    for at, (own, full) in enumerate(zip(owns, fulls)):
        copy = pltpu.make_async_copy(own, full.at[(*coords, core)], local_sem.at[at])
        copy.start()
        local.append(copy)
    stages = len(sizes)
    items[0].start(0, owns[0])
    for turn in range(count + stages):
        for stage in range(stages):
            at = turn - stage
            if 0 <= at < count:
                if stage == 0:
                    if at + 1 < count:
                        items[at + 1].start(0, owns[at + 1])
                    local[at].wait()
                items[at].land(stage)
                if stage + 1 < stages:
                    items[at].start(stage + 1)
        at = turn - stages
        if 0 <= at < count:
            items[at].finish()
    for item in items:
        item.drain()


def gather_all(shards, count):
    sizes = grid_of(count)
    copies = 400
    n = len(shards)
    fulls = pl.pallas_call(
        functools.partial(gather_kernel, sizes, n),
        out_shape=[jax.ShapeDtypeStruct((*sizes, 2, *s.shape), jnp.bfloat16) for s in shards],
        in_specs=[pl.BlockSpec(memory_space=pltpu.VMEM)] * n,
        out_specs=[pl.BlockSpec(memory_space=pltpu.HBM)] * n,
        scratch_shapes=[pltpu.VMEM(s.shape, jnp.bfloat16) for s in shards]
        + [pltpu.SemaphoreType.DMA((copies,)), pltpu.SemaphoreType.DMA((copies,)), pltpu.SemaphoreType.DMA((n,))],
        compiler_params=pltpu.CompilerParams(collective_id=0, has_side_effects=True),
        name="gather_all",
    )(*shards)
    return [full.reshape(-1, *full.shape[-2:]) for full in fulls]


def small_block(vectors, bias_up, me):
    wide = jnp.zeros((8, 128), jnp.float32)
    width = vectors.shape[1]
    per = 128 // width
    wide = lax.dynamic_update_slice(wide, vectors, (0, (me % per) * width))
    tail = jnp.zeros((8, 128), jnp.float32)
    span = bias_up.shape[0]
    tail = lax.dynamic_update_slice(tail, bias_up[None, :], (0, (me % (128 // span)) * span))
    return jnp.concatenate([wide, tail], axis=0)


def small_parts(small, vectors, bias_up):
    per = 128 // vectors.shape[1]
    span = 128 // bias_up.shape[0]
    n = small.shape[0]
    vec = jnp.sum(small[:, :8].astype(jnp.float32).reshape(n // per, per, 8, 128), axis=1)
    bias = jnp.sum(small[:, 8].astype(jnp.float32).reshape(n // span, span, 128), axis=1)
    return vec.transpose(1, 0, 2).reshape(8, -1).astype(jnp.bfloat16), bias.reshape(-1).astype(jnp.bfloat16)


F32, BF16 = jnp.float32, jnp.bfloat16


def nn(a, b):
    return lax.dot_general(a, b, (((1,), (0,)), ((), ())), preferred_element_type=F32)


def nt(a, b):
    return lax.dot_general(a, b, (((1,), (1,)), ((), ())), preferred_element_type=F32)


def tn(a, b):
    return lax.dot_general(a, b, (((0,), (0,)), ((), ())), preferred_element_type=F32)


def chunks(total, size, work):
    def step(i, carry):
        work(pl.ds(pl.multiple_of(i * size, size), size))
        return carry

    lax.fori_loop(0, total // size, step, 0)


def split_colours(columns, orders, shares):
    found, at = [], 0
    for order, share in zip(orders, shares):
        if share:
            found.append((at * 128, share * 128, order))
            at += share
    assert at * 128 == columns
    return found


class Spread:
    def __init__(self, full, own, rows, columns, colours, place):
        self.full, self.own, self.rows, self.columns, self.colours = full, own, rows, columns, colours
        self.sizes, self.coords, self.core = place

    def view(self, colour, fixed, core):
        where = tuple(fixed.get(dim, slice(None)) for dim in range(3))
        return self.full.at[(*where, core, pl.ds(*self.rows), pl.ds(self.columns + colour[0], colour[1]))]

    def sends(self, stage):
        for colour in self.colours:
            order = colour[2]
            dim = order[stage]
            held = self.view(colour, {d: self.coords[d] for d in order[stage:]}, self.core)
            source = held
            if stage == 0:
                source = self.own.at[pl.ds(*self.rows), pl.ds(self.columns + colour[0], colour[1])]
            for step in range(1, self.sizes[dim]):
                peer = swapped(self.coords, dim, (self.coords[dim] + step) % self.sizes[dim])
                yield source, held, device_at(peer, self.core, self.sizes)

    def passed(self, stage):
        for colour in self.colours:
            order = colour[2]
            dim = order[stage]
            fixed = {d: self.coords[d] for d in order[stage + 1:]}
            if stage == 0:
                yield self.view(colour, fixed, self.core)
            else:
                for step in range(1, self.sizes[dim]):
                    yield self.view(colour, {**fixed, dim: (self.coords[dim] + step) % self.sizes[dim]}, self.core)


class Group:
    def __init__(self, sem, gauge):
        self.sem, self.gauge, self.units = sem, gauge, 0

    def count(self, ref):
        self.units += math.prod(ref.shape) * jnp.dtype(ref.dtype).itemsize // 256

    def wait(self):
        whole = self.gauge.at[pl.ds(0, self.units)]
        pltpu.make_async_copy(whole, whole, self.sem).wait()


class Chunk:
    def __init__(self, wires, parts):
        self.wires, self.parts = wires, parts
        self.arriving, self.swap = {}, wires.group()

    def start(self, stage):
        self.arriving[stage] = self.wires.group()
        for part in self.parts:
            for one in part.sends(stage):
                self.wires.send(*one, self.arriving[stage])

    def land(self, stage):
        self.arriving[stage].wait()

    def share(self, stage):
        for part in self.parts:
            for view in part.passed(stage):
                self.wires.send(view, view, self.wires.partner, self.swap)

    def finish(self):
        self.swap.wait()


class Wires:
    def __init__(self, send_sem, recv_sem, gauge, partner):
        self.recv_sem, self.gauge, self.partner = recv_sem, gauge, partner
        self.used, self.sent = 0, Group(send_sem.at[0], gauge)

    def group(self):
        self.used += 1
        return Group(self.recv_sem.at[self.used - 1], self.gauge)

    def send(self, src, dst, target, group):
        pltpu.make_async_remote_copy(
            src_ref=src, dst_ref=dst, send_sem=self.sent.sem, recv_sem=group.sem,
            device_id=(target,), device_id_type=MESH_ID,
        ).start()
        group.count(dst)
        self.sent.count(dst)

    def swap(self, src, dst):
        group = self.group()
        self.send(src, dst, self.partner, group)
        return group

    def drain(self):
        self.sent.wait()


class Reduce:
    def __init__(self, wires, held, landing, colours, place):
        self.wires, self.held, self.landing, self.colours = wires, held, landing, colours
        self.sizes, self.coords, self.core = place

    def view(self, colour, fixed):
        where = tuple(fixed.get(dim, slice(None)) for dim in range(3))
        return self.held.at[(*where, slice(None), pl.ds(colour[0], colour[1]))]

    def start(self, stage):
        self.arriving = self.wires.group()
        for at, colour in enumerate(self.colours):
            order = colour[2]
            dim = order[stage]
            fixed = {d: self.coords[d] for d in order[:stage]}
            for step in range(1, self.sizes[dim]):
                theirs = (self.coords[dim] + step) % self.sizes[dim]
                peer = swapped(self.coords, dim, theirs)
                self.wires.send(
                    self.view(colour, {**fixed, dim: theirs}),
                    self.landing[at][stage].at[step - 1],
                    device_at(peer, self.core, self.sizes), self.arriving,
                )

    def land(self):
        self.arriving.wait()

    def add(self, stage, out=None):
        rows = self.held.shape[3]
        for at, colour in enumerate(self.colours):
            order = colour[2]
            fixed = {d: self.coords[d] for d in order[:stage + 1]}
            free = [d for d in range(3) if d not in fixed]
            landing = self.landing[at][stage]
            counts = [self.sizes[d] for d in free]
            total = math.prod(counts)
            tall = min(rows, 32)

            def step(i, carry, colour=colour, fixed=fixed, free=free, landing=landing, counts=counts, tall=tall):
                where, rest, index = dict(fixed), i // (rows // tall), []
                for d, size in zip(reversed(free), reversed(counts)):
                    where[d] = rest % size
                    index.insert(0, rest % size)
                    rest = rest // size
                span = pl.ds(pl.multiple_of((i % (rows // tall)) * tall, tall), tall)
                place = (where[0], where[1], where[2], span, pl.ds(colour[0], colour[1]))
                sums = self.held[place].astype(F32)
                for other in range(landing.shape[0]):
                    sums = sums + landing[(other, *index, span, slice(None))].astype(F32)
                if out is None:
                    self.held[place] = sums.astype(self.held.dtype)
                else:
                    out[span, pl.ds(colour[0], colour[1])] = sums
                return carry

            lax.fori_loop(0, total * (rows // tall), step, 0)


def landing_shapes(rows, colours, sizes, dtype):
    found = []
    for _, width, order in colours:
        stages = []
        for stage in range(3):
            free = [sizes[d] for d in range(3) if d not in order[:stage + 1]]
            stages.append(pltpu.VMEM((sizes[order[stage]] - 1, *free, rows, width), dtype))
        found.append(stages)
    return found


def stream(count, source, slots, sem, work):
    def fetch(i, slot):
        return pltpu.make_async_copy(source(i), slots(slot), sem.at[slot])

    fetch(0, 0).start()

    def step(i, carry):
        slot = lax.rem(i, 2)

        @pl.when(i + 1 < count)
        def _():
            fetch(i + 1, 1 - slot).start()

        fetch(i, slot).wait()
        work(i, slot)
        return carry

    lax.fori_loop(0, count, step, 0)


def columns_of(i, width):
    return pl.ds(pl.multiple_of(i * width, width), width)


def row_stats(values):
    mean = jnp.mean(values, axis=-1, keepdims=True)
    centred = values - mean
    rstd = lax.rsqrt(jnp.mean(centred * centred, axis=-1, keepdims=True) + ln_eps)
    return centred * rstd, rstd


SMALL, OUT, QKV, UP, DOWN = range(5)


class Box(dict):
    __getattr__ = dict.__getitem__


def leaves(tree):
    if isinstance(tree, dict):
        tree = list(tree.values())
    if isinstance(tree, list):
        return [leaf for part in tree for leaf in leaves(part)]
    return [] if tree is None else [tree]


def shape_of(tree):
    if isinstance(tree, dict):
        return {name: shape_of(part) for name, part in tree.items()}
    if isinstance(tree, list):
        return [shape_of(part) for part in tree]
    return tree is not None


def unpack(shape, refs):
    if isinstance(shape, dict):
        return {name: unpack(part, refs) for name, part in shape.items()}
    if isinstance(shape, list):
        return [unpack(part, refs) for part in shape]
    return next(refs) if shape else None


GATHER_ORDERS = ((0, 1, 2), (0, 2, 1), (2, 1, 0))
REDUCE_ORDERS = ((2, 1, 0), (1, 2, 0), (0, 1, 2))
SHARES = {8: (3, 4, 1), 12: (5, 5, 2), 16: (7, 7, 2), 24: (11, 10, 3), 32: (14, 14, 4), 1: (1, 0, 0)}
SIZES = (4, 2, 2)
TILE = 512


def step_kernel(names, *refs):
    r = Box(unpack(names, iter(refs)))
    sizes = SIZES
    me = lax.axis_index("dp")
    coords, core = locate(me, sizes)
    place = (sizes, coords, core)
    partner = device_at(coords, 1 - core, sizes)
    rows, d = r.tokens.shape
    ff = r.own[UP].shape[1]
    heads2 = d // 128
    slots = rows // MB_ROWS

    for which in (OUT, QKV, UP, DOWN):
        r.low[which][...] = r.own[which][...].astype(BF16)
    r.low[SMALL] = r.own[SMALL]
    greet(neighbours(coords, core, sizes))
    wires = Wires(r.send_sem, r.recv_sem, r.gauge, partner)

    def part(which, row_range, column_range):
        start, width = column_range
        colours = split_colours(width, GATHER_ORDERS, SHARES[width // 128])
        return Spread(r.full[which], r.low[which], row_range, start, colours, place)

    mine = []
    for which in (SMALL, OUT, QKV, UP, DOWN):
        copy = pltpu.make_async_copy(r.low[which], r.full[which].at[(*coords, core)], r.mine_sem.at[which])
        copy.start()
        mine.append(copy)
    short, tall = r.own[OUT].shape[0], r.own[DOWN].shape[0]
    parcels = [
        Chunk(wires, [part(SMALL, (0, 16), (0, 128)), part(OUT, (0, short), (0, d))]),
        Chunk(wires, [part(QKV, (0, short), (0, 3 * d // 2))]),
        Chunk(wires, [part(QKV, (0, short), (3 * d // 2, 3 * d // 2))]),
        Chunk(wires, [part(UP, (0, short), (0, ff // 2))]),
        Chunk(wires, [part(UP, (0, short), (ff // 2, ff // 2))]),
        Chunk(wires, [part(DOWN, (0, tall // 2), (0, d))]),
        Chunk(wires, [part(DOWN, (tall // 2, tall // 2), (0, d))]),
    ]
    parcels[0].start(0)
    dy_swap = wires.swap(r.dy, r.dy_far)

    def norm_one(span):
        normed, _ = row_stats(r.tokens[span, :].astype(F32))
        r.da[span, :] = normed

    chunks(rows, 32, norm_one)
    for copy in mine:
        copy.wait()
    count = len(parcels)

    def turn(t):
        if t < count:
            parcels[t].land(0)
            if t + 1 < count:
                parcels[t + 1].start(0)
            parcels[t].start(1)
            parcels[t].share(0)
        if 0 <= t - 1 < count:
            parcels[t - 1].land(1)
            parcels[t - 1].start(2)
            parcels[t - 1].share(1)
        if 0 <= t - 2 < count:
            parcels[t - 2].land(2)
            parcels[t - 2].share(2)
        if 0 <= t - 3 < count:
            parcels[t - 3].finish()

    for t in range(4):
        turn(t)
    copy = pltpu.make_async_copy(r.full[SMALL], r.smalls, r.mine_sem.at[0])
    copy.start()
    copy.wait()
    devices = math.prod(sizes) * 2
    flat = [(z, y, x, c) for z in range(sizes[0]) for y in range(sizes[1]) for x in range(sizes[2]) for c in range(2)]
    per = devices * 128 // d
    vec, bias = r.vec, r.bias
    for j in range(d // 128):
        total = 0.0
        for k in range(per):
            total = total + r.smalls[flat[j * per + k]].astype(F32)[0:8]
        vec[:, j * 128:(j + 1) * 128] = total
    for j in range(devices):
        bias[:, j * 128:(j + 1) * 128] = r.smalls[flat[j]].astype(F32)[8:9]
    for t in range(4, 6):
        turn(t)

    def first_in(span):
        r.a[span, :] = (r.da[span, :] * vec[0:1, :] + vec[1:2, :]).astype(BF16)

    chunks(rows, 32, first_in)

    def transpose_out(source, turned, far):
        width = source.shape[1]
        block = turned.shape[2]
        group = max(1, 256 // (2 * block))

        def step(i, carry):
            value = source[:, columns_of(i, 2 * block * group)]
            flipped = value.astype(F32).T.astype(BF16)
            turned[pl.ds(i * group, group)] = flipped.reshape(group, 2, block, rows)
            return carry

        lax.fori_loop(0, width // (2 * block * group), step, 0)
        return wires.swap(turned.at[:, 1 - core], far)

    def tile_stream(which, width, work):
        full, slot = r.full[which], r.wide
        total = full.shape[-1] // TILE
        stream(
            total,
            lambda i: full.at[:, :, :, :, :, columns_of(i, TILE)],
            lambda s: slot.at[s],
            r.tile_sem,
            lambda i, s: work(i, slot[s].reshape(-1, TILE)),
        )

    def qkv_tile(i, tile):
        which = i * TILE // d
        values = nn(r.a[...], tile)
        shift = jnp.where(which == 0, 1.0, 0.0) * vec[2:3, columns_of(i % (d // TILE), TILE)] + jnp.where(
            which == 2, 1.0, 0.0
        ) * vec[3:4, columns_of(i % (d // TILE), TILE)]
        r.qkv[:, columns_of(i, TILE)] = (values + shift).astype(BF16)

    tile_stream(QKV, TILE, qkv_tile)
    one_far = transpose_out(r.a, r.one_t, r.one_far)

    low_lane = lax.broadcasted_iota(jnp.int32, (MB_ROWS, 128), 1) < HEAD_DIM
    scale = 1.0 / math.sqrt(HEAD_DIM)

    def stacked(value):
        zero = jnp.zeros_like(value)
        return jnp.concatenate([jnp.where(low_lane, value, zero), jnp.where(low_lane, zero, value)], axis=0)

    def merged(value):
        return jnp.where(low_lane, value[:MB_ROWS], value[MB_ROWS:])

    def attend(p, carry):
        row = lax.broadcasted_iota(jnp.int32, (2 * MB_ROWS, 128), 0)
        dist = (row % MB_ROWS - lax.broadcasted_iota(jnp.int32, (2 * MB_ROWS, 128), 1)).astype(F32)
        head = (2 * p + row // MB_ROWS).astype(F32)
        alibi = jnp.where(dist >= 0, -jnp.exp2((head + 1.0) * (-8.0 / HEADS)) * dist, -1e30)
        for s in range(slots):
            span = pl.ds(s * MB_ROWS, MB_ROWS)
            q = r.qkv[span, columns_of(p, 128)]
            k = r.qkv[span, columns_of(p + heads2, 128)]
            v = r.qkv[span, columns_of(p + 2 * heads2, 128)]
            scores = nt(stacked(q), k) * scale + alibi
            top = jnp.max(scores, axis=-1, keepdims=True)
            grown = jnp.exp(scores - top)
            probs = grown / jnp.sum(grown, axis=-1, keepdims=True)
            r.probs[p * slots + s] = probs
            r.attn[span, columns_of(p, 128)] = merged(nn(probs.astype(BF16), v)).astype(BF16)
        return carry

    lax.fori_loop(0, heads2, attend, 0)
    attn_far = transpose_out(r.attn, r.attn_t, r.attn_far)

    def out_tile(i, tile):
        span = columns_of(i, TILE)
        r.h1[:, span] = r.tokens[:, span].astype(F32) + nn(r.attn[...], tile) + vec[4:5, span]

    tile_stream(OUT, TILE, out_tile)
    turn(6)

    def second_in(span):
        normed, _ = row_stats(r.h1[span, :])
        r.a[span, :] = (normed * vec[5:6, :] + vec[6:7, :]).astype(BF16)

    chunks(rows, 32, second_in)
    two_far = transpose_out(r.a, r.two_t, r.two_far)
    turn(7)

    def up_tile(i, tile):
        pre = nn(r.a[...], tile) + bias[:, columns_of(i, TILE)]
        value, slope = gelu_pair(pre)
        r.act[:, columns_of(i, TILE)] = value.astype(BF16)
        r.slope[:, columns_of(i, TILE)] = slope.astype(BF16)

    tile_stream(UP, TILE, up_tile)
    act_far = transpose_out(r.act, r.act_t, r.act_far)
    dy_swap.wait()
    turn(8)
    act_far.wait()

    reduces = [
        Reduce(wires, held, landing, colours, place)
        for held, landing, colours in zip(r.grad, r.landing, reduce_colours(d, ff))
    ]

    def weight_grad(which, turned, far, near_d, far_d, width):
        grad = r.grad[which]
        block = turned.shape[2]
        total = near_d.shape[1] // width
        groups = max(1, 16 * block // 512)
        each = 16 // groups

        def step(i, carry):
            at, g = i // groups, i % groups
            left = turned[pl.ds(g * each, each), core].reshape(each * block, rows)
            other = far[pl.ds(g * each, each)].reshape(each * block, rows)
            span = columns_of(at, width)
            value = nn(left, near_d[:, span]) + nn(other, far_d[:, span])
            value = value.astype(BF16)
            if groups == 1:
                grad[:, :, :, :, span] = value.reshape(*sizes, block, width)
            else:
                grad[g, :, :, :, span] = value.reshape(*sizes[1:], block, width)
            return carry

        assert groups in (1, sizes[0])
        lax.fori_loop(0, total * groups, step, 0)

    weight_grad(DOWN, r.act_t, r.act_far, r.dy, r.dy_far, 512)
    reduces[DOWN].start(0)
    turn(9)

    sums = r.sums
    sums[...] = jnp.zeros_like(sums)
    acc = r.da

    def begin(span):
        acc[span, :] = r.h1[span, :] + vec[7:8, :]
        sums[7:8, :] += jnp.sum(r.dy[span, :].astype(F32), axis=0, keepdims=True)

    chunks(rows, 32, begin)

    def down_tile(i, s):
        tile = r.deep[s].reshape(-1, d)
        wide = tile.shape[0]
        span = columns_of(i, wide)
        acc[...] += nn(r.act[:, span], tile)
        d_pre = nt(r.dy[...], tile) * r.slope[:, span].astype(F32)
        r.bias_sum[:, span] = jnp.sum(d_pre, axis=0, keepdims=True)
        r.act[:, span] = d_pre.astype(BF16)

    full_down = r.full[DOWN]
    stream(
        sizes[0] * sizes[1],
        lambda i: full_down.at[i // sizes[1], i % sizes[1]],
        lambda s: r.deep.at[s],
        r.tile_sem,
        down_tile,
    )
    pre_swap = wires.swap(r.act, r.pre_far)
    r.output[...] = acc[...].astype(BF16)

    def row_stream(which, left):
        full, slot = r.full[which], r.flat
        width = full.shape[-1]

        def work(i, s):
            tile = slot[s, :, :, :, :, pl.ds(0, width)].reshape(-1, width)
            return nt(left[...], tile)

        def run(put):
            stream(
                sizes[0],
                lambda i: full.at[i],
                lambda s: slot.at[s, :, :, :, :, pl.ds(0, width)],
                r.tile_sem,
                lambda i, s: put(i, work(i, s)),
            )

        return run

    def put_da(i, value):
        r.da[:, columns_of(i, value.shape[1])] = value

    row_stream(UP, r.act)(put_da)
    two_far.wait()
    pre_swap.wait()
    weight_grad(UP, r.two_t, r.two_far, r.act, r.pre_far, 512)
    reduces[UP].start(0)

    def norm_two_back(span):
        normed, rstd = row_stats(r.h1[span, :])
        da = r.da[span, :]
        sums[5:6, :] += jnp.sum(da * normed, axis=0, keepdims=True)
        sums[6:7, :] += jnp.sum(da, axis=0, keepdims=True)
        d_h1 = r.dy[span, :].astype(F32) + norm_back(da, normed, rstd, vec[5:6, :])
        sums[4:5, :] += jnp.sum(d_h1, axis=0, keepdims=True)
        r.d_h1[span, :] = d_h1
        r.d_mid[span, :] = d_h1.astype(BF16)

    chunks(rows, 32, norm_two_back)
    mid_swap = wires.swap(r.d_mid, r.mid_far)

    def put_attn(i, value):
        r.d_attn[:, columns_of(i, value.shape[1])] = value.astype(BF16)

    row_stream(OUT, r.d_mid)(put_attn)

    def advance(which, stage):
        reduces[which].land()
        reduces[which].add(stage - 1)
        reduces[which].start(stage)

    def complete(which):
        reduces[which].land()
        reduces[which].add(2, r.final[which])

    advance(DOWN, 1)

    def attend_back(p, carry):
        span_p = columns_of(p, 128)
        d_bq = jnp.zeros((1, 128), F32)
        d_bv = jnp.zeros((1, 128), F32)
        for s in range(slots):
            span = pl.ds(s * MB_ROWS, MB_ROWS)
            q = stacked(r.qkv[span, span_p])
            k = r.qkv[span, columns_of(p + heads2, 128)]
            v = r.qkv[span, columns_of(p + 2 * heads2, 128)]
            do = r.d_attn[span, span_p]
            probs = r.probs[p * slots + s]
            both = stacked(do)
            d_v = tn(probs.astype(BF16), both)
            d_probs = nt(both, v)
            weighed = do.astype(F32) * r.attn[span, span_p].astype(F32)
            delta = jnp.sum(stacked(weighed), axis=-1, keepdims=True)
            d_scores = (probs * (d_probs - delta)).astype(BF16)
            d_q = merged(nn(d_scores, k)) * scale
            d_k = tn(d_scores, q) * scale
            d_bq += jnp.sum(d_q, axis=0, keepdims=True)
            d_bv += jnp.sum(d_v, axis=0, keepdims=True)
            r.qkv[span, span_p] = d_q.astype(BF16)
            r.qkv[span, columns_of(p + heads2, 128)] = d_k.astype(BF16)
            r.qkv[span, columns_of(p + 2 * heads2, 128)] = d_v.astype(BF16)
        sums[2:3, span_p] = d_bq
        sums[3:4, span_p] = d_bv
        return carry

    lax.fori_loop(0, heads2, attend_back, 0)
    qkv_swap = wires.swap(r.qkv, r.qkv_far)
    advance(DOWN, 2)
    row_stream(QKV, r.qkv)(put_da)
    one_far.wait()
    qkv_swap.wait()
    weight_grad(QKV, r.one_t, r.one_far, r.qkv, r.qkv_far, 512)
    advance(UP, 1)
    reduces[QKV].start(0)
    attn_far.wait()
    mid_swap.wait()
    weight_grad(OUT, r.attn_t, r.attn_far, r.d_mid, r.mid_far, 512)
    reduces[OUT].start(0)

    def norm_one_back(span):
        normed, rstd = row_stats(r.tokens[span, :].astype(F32))
        da = r.da[span, :]
        sums[0:1, :] += jnp.sum(da * normed, axis=0, keepdims=True)
        sums[1:2, :] += jnp.sum(da, axis=0, keepdims=True)
        r.input_grad[span, :] = r.d_h1[span, :] + norm_back(da, normed, rstd, vec[0:1, :])

    chunks(rows, 32, norm_one_back)

    bundle = r.bundle
    for j in range(devices):
        at = (j // per) * 128
        bundle[flat[j]] = jnp.concatenate(
            [sums[:, at:at + 128], jnp.broadcast_to(r.bias_sum[:, j * 128:(j + 1) * 128], (8, 128))], axis=0
        )
    tiny_swap = wires.swap(bundle.at[:, :, :, 1 - core], r.tiny_far)
    complete(DOWN)
    advance(UP, 2)
    tiny_swap.wait()
    r.grad[SMALL][...] = bundle[:, :, :, core] + r.tiny_far[...]
    tiny = reduces[SMALL]
    tiny.start(0)
    advance(QKV, 1)
    tiny.land()
    tiny.add(0)
    tiny.start(1)
    complete(UP)
    advance(OUT, 1)
    tiny.land()
    tiny.add(1)
    tiny.start(2)
    advance(QKV, 2)
    tiny.land()
    tiny.add(2, r.final[SMALL])
    advance(OUT, 2)
    complete(QKV)
    complete(OUT)
    wires.drain()


def reduce_colours(d, ff):
    return [[(0, 128, (2, 1, 0))]] + [
        split_colours(width, REDUCE_ORDERS, SHARES[width // 128]) for width in (d, 3 * d, ff, d)
    ]


def fused_step(tokens, dy, small, w_qkv, w_out, w_up, w_down):
    sizes = SIZES
    rows, d = tokens.shape
    ff = w_up.shape[1]
    short, tall = w_out.shape[0], w_down.shape[0]
    heads2 = d // 128
    slots = rows // MB_ROWS
    whole = lambda s: jax.ShapeDtypeStruct((*sizes, 2, *s), BF16)
    like = jax.ShapeDtypeStruct
    wide = ((16, 128), (short, d), (short, 3 * d), (short, ff), (tall, d))
    v = pltpu.VMEM
    turned, across = v((16, 2, short, rows), BF16), v((16, short, rows), BF16)
    flat, double = v((rows, d), BF16), v((rows, d), F32)
    inputs = dict(tokens=tokens, dy=dy, own=[small, w_out, w_qkv, w_up, w_down])
    in_hbm = dict(full=[whole(s) for s in wide], gauge=like((180_224, 128), BF16))
    in_vmem = dict(
        output=like((rows, d), BF16), input_grad=like((rows, d), F32), final=[like(s, F32) for s in wide]
    )
    heights = (16, short, short, short, tall)
    colours = reduce_colours(d, ff)
    scratch = dict(
        low=[None, *(v(s, BF16) for s in wide[1:])],
        smalls=v((*sizes, 2, 16, 128), BF16), vec=v((8, d), F32), bias=v((1, ff), F32),
        dy_far=flat, da=double, a=flat, qkv=v((rows, 3 * d), BF16), qkv_far=v((rows, 3 * d), BF16),
        probs=v((heads2 * slots, 2 * MB_ROWS, 128), F32), attn=flat, h1=double,
        act=v((rows, ff), BF16), slope=v((rows, ff), BF16), pre_far=v((rows, ff), BF16),
        d_h1=double, d_mid=flat, mid_far=flat, d_attn=flat,
        one_t=turned, one_far=across, attn_t=turned, attn_far=across, two_t=turned, two_far=across,
        act_t=v((16, 2, tall, rows), BF16), act_far=v((16, tall, rows), BF16),
        wide=v((2, *sizes, 2, short, TILE), BF16), deep=v((2, sizes[2], 2, tall, d), BF16),
        flat=v((2, *sizes[1:], 2, short, ff), BF16),
        grad=[v((*sizes, *s), BF16 if at else F32) for at, s in enumerate(wide)],
        sums=v((8, d), F32), bias_sum=v((1, ff), F32),
        bundle=v((*sizes, 2, 16, 128), F32), tiny_far=v((*sizes, 16, 128), F32),
        landing=[landing_shapes(heights[at], colours[at], sizes, BF16 if at else F32) for at in range(5)],
        send_sem=pltpu.SemaphoreType.DMA((1,)), recv_sem=pltpu.SemaphoreType.DMA((56,)),
        mine_sem=pltpu.SemaphoreType.DMA((5,)), tile_sem=pltpu.SemaphoreType.DMA((2,)),
    )
    names = {**inputs, **in_hbm, **in_vmem, **scratch}
    found = pl.pallas_call(
        functools.partial(step_kernel, shape_of(names)),
        out_shape=[*leaves(in_hbm), *leaves(in_vmem)],
        in_specs=[pl.BlockSpec(memory_space=v)] * len(leaves(inputs)),
        out_specs=[pl.BlockSpec(memory_space=pltpu.HBM)] * len(leaves(in_hbm))
        + [pl.BlockSpec(memory_space=v)] * len(leaves(in_vmem)),
        scratch_shapes=leaves(scratch),
        compiler_params=pltpu.CompilerParams(
            collective_id=1, has_side_effects=True, vmem_limit_bytes=67_000_000
        ),
        name="fused_step",
    )(*leaves(inputs))
    return Box(unpack(shape_of({**in_hbm, **in_vmem}), iter(found)))


def general_body(
    tokens,
    cotangent,
    lengths,
    vectors,
    bias_up,
    w_qkv,
    w_out,
    w_up,
    w_down,
    mom_vectors,
    mom_bias_up,
    mom_qkv,
    mom_out,
    mom_up,
    mom_down,
):
    params = (vectors, bias_up, w_qkv, w_out, w_up, w_down)
    moments = (mom_vectors, mom_bias_up, mom_qkv, mom_out, mom_up, mom_down)
    me = lax.axis_index("dp")
    count = lax.axis_size("dp")
    small, full_out, full_qkv, full_up, full_down = gather_all(
        [small_block(vectors, bias_up, me), w_out, w_qkv, w_up, w_down], count
    )
    vec_low, bias_low = small_parts(small, vectors, bias_up)
    weights = (
        vec_low,
        bias_low,
        full_qkv.reshape(-1, w_qkv.shape[1]),
        full_out.reshape(-1, w_out.shape[1]),
        full_up.reshape(-1, w_up.shape[1]),
        full_down.reshape(-1, w_down.shape[1]),
    )
    alibi = alibi_bias(MB_ROWS)
    place = jnp.arange(MB_ROWS)
    owned = tuple((jnp.zeros(p.shape, jnp.float32) for p in params))
    summed = None
    out_list = []
    dx_list = []
    for micro in range(MICRO):
        x_rows = tokens[micro * MB_ROWS : (micro + 1) * MB_ROWS]
        live = place < lengths[micro]
        grad_rows = jnp.where(
            live[:, None],
            cotangent[micro * MB_ROWS : (micro + 1) * MB_ROWS],
            jnp.zeros((), jnp.bfloat16),
        )
        out, saved = forward_block(x_rows, weights, alibi)
        d_x, grads = backward_block(saved, grad_rows, weights, alibi)
        out_list.append(out)
        dx_list.append(d_x)
        summed = grads if summed is None else tuple((a + b for a, b in zip(summed, grads)))
    owned = (
        lax.psum_scatter(summed[0], "dp", scatter_dimension=1, tiled=True),
        lax.psum_scatter(summed[1], "dp", scatter_dimension=0, tiled=True),
        lax.psum_scatter(summed[2], "dp", scatter_dimension=0, tiled=True),
        lax.psum_scatter(summed[3], "dp", scatter_dimension=0, tiled=True),
        lax.psum_scatter(summed[4], "dp", scatter_dimension=0, tiled=True),
        lax.psum_scatter(summed[5], "dp", scatter_dimension=0, tiled=True),
    )
    count = float(STEP)
    news = [adamw(p, m, g, count) for p, m, g in zip(params, moments, owned)]
    output = jnp.concatenate(out_list, axis=0)
    input_grad = jnp.concatenate(dx_list, axis=0)
    return (
        output,
        input_grad,
        owned[0],
        owned[1],
        owned[2],
        owned[3],
        owned[4],
        owned[5],
        news[0][0],
        news[1][0],
        news[2][0],
        news[3][0],
        news[4][0],
        news[5][0],
        news[0][1],
        news[1][1],
        news[2][1],
        news[3][1],
        news[4][1],
        news[5][1],
        news[0][2],
        news[1][2],
        news[2][2],
        news[3][2],
        news[4][2],
        news[5][2],
    )


def body(
    tokens, cotangent, lengths, vectors, bias_up, w_qkv, w_out, w_up, w_down,
    mom_vectors, mom_bias_up, mom_qkv, mom_out, mom_up, mom_down,
):
    if grid_of(lax.axis_size("dp")) != SIZES:
        return general_body(
            tokens, cotangent, lengths, vectors, bias_up, w_qkv, w_out, w_up, w_down,
            mom_vectors, mom_bias_up, mom_qkv, mom_out, mom_up, mom_down,
        )
    me = lax.axis_index("dp")
    place = jnp.arange(tokens.shape[0]) % MB_ROWS
    live = place < jnp.repeat(lengths, MB_ROWS)
    dy = jnp.where(live[:, None], cotangent, jnp.zeros((), jnp.bfloat16))
    small = small_block(vectors, bias_up, me).astype(jnp.bfloat16)
    found = fused_step(tokens, dy, small, w_qkv, w_out, w_up, w_down)
    width = vectors.shape[1]
    g_vec = lax.dynamic_slice(found.final[SMALL], (0, (me % (128 // width)) * width), (8, width))
    owned = (
        g_vec, found.final[SMALL][8], found.final[QKV], found.final[OUT], found.final[UP], found.final[DOWN],
    )
    params = (vectors, bias_up, w_qkv, w_out, w_up, w_down)
    moments = (mom_vectors, mom_bias_up, mom_qkv, mom_out, mom_up, mom_down)
    news = [adamw(p, m, g, float(STEP)) for p, m, g in zip(params, moments, owned)]
    return (
        found.output, found.input_grad, *owned,
        *(n[0] for n in news), *(n[1] for n in news), *(n[2] for n in news),
    )


def solution(mesh):
    in_specs = (
        P("dp", None),
        P("dp", None),
        P("dp"),
        P(None, "dp"),
        P("dp"),
        P("dp", None),
        P("dp", None),
        P("dp", None),
        P("dp", None),
        P(None, None, "dp"),
        P(None, "dp"),
        P(None, "dp", None),
        P(None, "dp", None),
        P(None, "dp", None),
        P(None, "dp", None),
    )
    out_specs = (
        P("dp", None),
        P("dp", None),
        P(None, "dp"),
        P("dp"),
        P("dp", None),
        P("dp", None),
        P("dp", None),
        P("dp", None),
        P(None, "dp"),
        P("dp"),
        P("dp", None),
        P("dp", None),
        P("dp", None),
        P("dp", None),
        P(None, "dp"),
        P("dp"),
        P("dp", None),
        P("dp", None),
        P("dp", None),
        P("dp", None),
        P(None, "dp"),
        P("dp"),
        P("dp", None),
        P("dp", None),
        P("dp", None),
        P("dp", None),
    )
    return jax.shard_map(body, mesh=mesh, in_specs=in_specs, out_specs=out_specs, check_vma=False)
```

```python
import functools
import math

import jax
import jax.numpy as jnp
from jax import lax
from jax.experimental import pallas as pl
from jax.experimental.pallas import tpu as pltpu
from jax.sharding import PartitionSpec as P

D = 1024
HEADS = 16
HEAD_DIM = 64
MB_ROWS = 128
MICRO = 2
STEP = 3


ln_eps = 1e-05
gelu_c = math.sqrt(2.0 / math.pi)
beta_one = 0.9
beta_two = 0.95
decay_rate = 0.1
adam_eps = 1e-08


def product(left, right):
    return jnp.dot(left, right, preferred_element_type=jnp.float32)


def contract(form, left, right):
    return jnp.einsum(form, left, right, preferred_element_type=jnp.float32)


def layer_norm(values, gain, shift):
    centred = values - jnp.mean(values, axis=-1, keepdims=True)
    rstd = lax.rsqrt(jnp.mean(centred * centred, axis=-1, keepdims=True) + ln_eps)
    normed = centred * rstd
    return (normed * gain + shift, normed, rstd)


def norm_back(grad_in, normed, rstd, gain):
    scaled = grad_in * gain
    inner = (
        scaled
        - jnp.mean(scaled, axis=-1, keepdims=True)
        - normed * jnp.mean(scaled * normed, axis=-1, keepdims=True)
    )
    return rstd * inner


def gelu_pair(pre):
    tanh_val = jnp.tanh(gelu_c * (pre + 0.044715 * pre * pre * pre))
    value = 0.5 * pre * (1.0 + tanh_val)
    slope = 0.5 * (1.0 + tanh_val) + 0.5 * pre * (1.0 - tanh_val * tanh_val) * gelu_c * (
        1.0 + 3.0 * 0.044715 * pre * pre
    )
    return (value, slope)


def alibi_bias(rows):
    place = jnp.arange(rows)
    dist = (place[:, None] - place[None, :]).astype(jnp.float32)
    slopes = jnp.exp2(-8.0 * (jnp.arange(HEADS) + 1).astype(jnp.float32) / HEADS)
    bias = -slopes[:, None, None] * dist[None]
    return jnp.where(dist[None] >= 0, bias, -1e30)


def attention_scores(q3, k3, alibi):
    return contract("qhd,khd->hqk", q3, k3) * (1.0 / math.sqrt(HEAD_DIM)) + alibi


def forward_block(x_rows, weights, alibi):
    vec, up_bias, qkv_w, out_w, up_w, down_w = weights
    vecf = vec.astype(jnp.float32)
    rows = x_rows.shape[0]
    xf = x_rows.astype(jnp.float32)
    ln_one, normed_one, rstd_one = layer_norm(xf, vecf[0], vecf[1])
    a_one = ln_one.astype(jnp.bfloat16)
    qkv = product(a_one, qkv_w)
    query = (qkv[:, :D] + vecf[2]).astype(jnp.bfloat16).reshape(rows, HEADS, HEAD_DIM)
    keyx = qkv[:, D : 2 * D].astype(jnp.bfloat16).reshape(rows, HEADS, HEAD_DIM)
    value = (qkv[:, 2 * D :] + vecf[3]).astype(jnp.bfloat16).reshape(rows, HEADS, HEAD_DIM)
    scores = attention_scores(query, keyx, alibi)
    top = jnp.max(scores, axis=-1, keepdims=True)
    lse = top + jnp.log(jnp.sum(jnp.exp(scores - top), axis=-1, keepdims=True))
    probs = jnp.exp(scores - lse).astype(jnp.bfloat16)
    attn = contract("hqk,khd->qhd", probs, value).reshape(rows, D).astype(jnp.bfloat16)
    h_one = xf + product(attn, out_w) + vecf[4]
    ln_two, normed_two, rstd_two = layer_norm(h_one, vecf[5], vecf[6])
    a_two = ln_two.astype(jnp.bfloat16)
    pre = product(a_two, up_w) + up_bias.astype(jnp.float32)
    act, slope = gelu_pair(pre)
    act_b = act.astype(jnp.bfloat16)
    out = (h_one + product(act_b, down_w) + vecf[7]).astype(jnp.bfloat16)
    saved = (
        normed_one,
        rstd_one,
        a_one,
        query,
        keyx,
        value,
        lse,
        attn,
        normed_two,
        rstd_two,
        a_two,
        slope,
        act_b,
    )
    return (out, saved)


def backward_block(saved, grad_rows, weights, alibi):
    vec, up_bias, qkv_w, out_w, up_w, down_w = weights
    vecf = vec.astype(jnp.float32)
    (
        normed_one,
        rstd_one,
        a_one,
        query,
        keyx,
        value,
        lse,
        attn,
        normed_two,
        rstd_two,
        a_two,
        slope,
        act_b,
    ) = saved
    rows = grad_rows.shape[0]
    scale = 1.0 / math.sqrt(HEAD_DIM)
    dyf = grad_rows.astype(jnp.float32)
    g_bdown = jnp.sum(dyf, axis=0)
    g_down = product(act_b.T, grad_rows)
    d_pre = product(grad_rows, down_w.T) * slope
    g_bup = jnp.sum(d_pre, axis=0)
    d_pre_b = d_pre.astype(jnp.bfloat16)
    g_up = product(a_two.T, d_pre_b)
    d_a2 = product(d_pre_b, up_w.T)
    g_ln2g = jnp.sum(d_a2 * normed_two, axis=0)
    g_ln2b = jnp.sum(d_a2, axis=0)
    d_h1 = dyf + norm_back(d_a2, normed_two, rstd_two, vecf[5])
    g_bout = jnp.sum(d_h1, axis=0)
    d_h1_b = d_h1.astype(jnp.bfloat16)
    g_out = product(attn.T, d_h1_b)
    d_attn = product(d_h1_b, out_w.T).astype(jnp.bfloat16).reshape(rows, HEADS, HEAD_DIM)
    probs_f = jnp.exp(attention_scores(query, keyx, alibi) - lse)
    probs = probs_f.astype(jnp.bfloat16)
    d_v = contract("hqk,qhd->khd", probs, d_attn).reshape(rows, D)
    d_probs = contract("qhd,khd->hqk", d_attn, value)
    delta = jnp.sum(
        d_attn.astype(jnp.float32) * attn.reshape(rows, HEADS, HEAD_DIM).astype(jnp.float32),
        axis=-1,
    ).T[:, :, None]
    d_scores = (probs_f * (d_probs - delta)).astype(jnp.bfloat16)
    d_q = (contract("hqk,khd->qhd", d_scores, keyx) * scale).reshape(rows, D)
    d_k = (contract("hqk,qhd->khd", d_scores, query) * scale).reshape(rows, D)
    g_bq = jnp.sum(d_q, axis=0)
    g_bv = jnp.sum(d_v, axis=0)
    d_qkv = jnp.concatenate([d_q, d_k, d_v], axis=1).astype(jnp.bfloat16)
    g_qkv = product(a_one.T, d_qkv)
    d_a1 = product(d_qkv, qkv_w.T)
    g_ln1g = jnp.sum(d_a1 * normed_one, axis=0)
    g_ln1b = jnp.sum(d_a1, axis=0)
    d_x = d_h1 + norm_back(d_a1, normed_one, rstd_one, vecf[0])
    g_vec = jnp.stack([g_ln1g, g_ln1b, g_bq, g_bv, g_bout, g_ln2g, g_ln2b, g_bdown])
    return (d_x, (g_vec, g_bup, g_qkv, g_out, g_up, g_down))


def adamw(param, moments, grad, count):
    first = beta_one * moments[0] + (1.0 - beta_one) * grad
    second = beta_two * moments[1] + (1.0 - beta_two) * grad * grad
    corr_one = 1.0 - beta_one**count
    corr_two = 1.0 - beta_two**count
    update = first / corr_one / (jnp.sqrt(second / corr_two) + adam_eps) + decay_rate * param
    return (update, first, second)


MESH_ID = pl.DeviceIdType.MESH


def grid_of(count):
    known = {32: (4, 2, 2), 128: (4, 4, 4)}
    return known.get(count, (count // 2,))


def locate(me, sizes):
    rest, coords = me // 2, []
    for size in reversed(sizes):
        coords.append(rest % size)
        rest = rest // size
    return tuple(reversed(coords)), me % 2


def device_at(coords, core, sizes):
    index = 0
    for value, size in zip(coords, sizes):
        index = index * size + value
    return index * 2 + core


def swapped(coords, dim, value):
    return tuple(value if at == dim else old for at, old in enumerate(coords))


def neighbours(coords, core, sizes):
    found = [device_at(coords, 1 - core, sizes)]
    for dim, size in enumerate(sizes):
        for step in range(1, size):
            found.append(device_at(swapped(coords, dim, (coords[dim] + step) % size), core, sizes))
    return found


def greet(others):
    barrier = pltpu.get_barrier_semaphore()
    for other in others:
        pl.semaphore_signal(barrier, inc=1, device_id=(other,), device_id_type=MESH_ID)
    pl.semaphore_wait(barrier, len(others))


class Sems:
    def __init__(self, send, recv):
        self.send, self.recv, self.used = send, recv, 0

    def pair(self):
        at = self.used
        self.used += 1
        return self.send.at[at], self.recv.at[at]


def remote(sems, src, dst, target):
    send_sem, recv_sem = sems.pair()
    copy = pltpu.make_async_remote_copy(
        src_ref=src, dst_ref=dst, send_sem=send_sem, recv_sem=recv_sem,
        device_id=(target,), device_id_type=MESH_ID,
    )
    copy.start()
    return copy


class Gather:
    def __init__(self, full, colours, sizes, coords, core, sems):
        self.full, self.colours, self.sizes = full, colours, sizes
        self.coords, self.core, self.sems = coords, core, sems
        self.axis = [[] for _ in colours]
        self.swap = []
        self.sent = []

    def view(self, colour, fixed):
        start, width, _ = colour
        place = tuple(fixed.get(dim, slice(None)) for dim in range(len(self.sizes)))
        return self.full.at[(*place, self.core, slice(None), pl.ds(start, width))]

    def start(self, stage, own=None):
        for at, colour in enumerate(self.colours):
            order = colour[2]
            dim = order[stage]
            fixed = {d: self.coords[d] for d in order[stage:]}
            held = self.view(colour, fixed)
            source = held if own is None else own.at[:, pl.ds(colour[0], colour[1])]
            self.axis[at] = []
            for step in range(1, self.sizes[dim]):
                peer = swapped(self.coords, dim, (self.coords[dim] + step) % self.sizes[dim])
                self.axis[at].append(remote(self.sems, source, held, device_at(peer, self.core, self.sizes)))
            self.sent += self.axis[at]

    def land(self, stage):
        partner = device_at(self.coords, 1 - self.core, self.sizes)
        for at, colour in enumerate(self.colours):
            order = colour[2]
            dim = order[stage]
            for copy in self.axis[at]:
                copy.wait_recv()
            fixed = {d: self.coords[d] for d in order[stage + 1:]}
            if stage == 0:
                views = [self.view(colour, fixed)]
            else:
                views = [
                    self.view(colour, {**fixed, dim: (self.coords[dim] + step) % self.sizes[dim]})
                    for step in range(1, self.sizes[dim])
                ]
            for view in views:
                self.swap.append(remote(self.sems, view, view, partner))

    def finish(self):
        for copy in self.swap:
            copy.wait_recv()

    def drain(self):
        for copy in self.sent + self.swap:
            copy.wait_send()


def colours_of(columns, sizes):
    last = len(sizes) - 1
    if last < 2:
        return [(0, columns, tuple(range(len(sizes))))]
    tiles = columns // 128
    if tiles < 8:
        return [(0, columns, (0, 1, 2))]
    third = max(1, tiles // 8)
    first = (tiles - third) // 2
    second = tiles - third - first
    return [
        (0, first * 128, (0, 1, 2)),
        (first * 128, second * 128, (0, 2, 1)),
        ((first + second) * 128, third * 128, (2, 1, 0)),
    ]


def gather_kernel(sizes, count, *refs):
    shards, fulls = refs[:count], refs[count : 2 * count]
    owns = refs[2 * count : 3 * count]
    send_sem, recv_sem, local_sem = refs[3 * count :]
    coords, core = locate(lax.axis_index("dp"), sizes)
    for shard, own in zip(shards, owns):
        own[...] = shard[...].astype(own.dtype)
    greet(neighbours(coords, core, sizes))
    sems = Sems(send_sem, recv_sem)
    items = [
        Gather(full, colours_of(full.shape[-1], sizes), sizes, coords, core, sems) for full in fulls
    ]
    local = []
    for at, (own, full) in enumerate(zip(owns, fulls)):
        copy = pltpu.make_async_copy(own, full.at[(*coords, core)], local_sem.at[at])
        copy.start()
        local.append(copy)
    stages = len(sizes)
    items[0].start(0, owns[0])
    for turn in range(count + stages):
        for stage in range(stages):
            at = turn - stage
            if 0 <= at < count:
                if stage == 0:
                    if at + 1 < count:
                        items[at + 1].start(0, owns[at + 1])
                    local[at].wait()
                items[at].land(stage)
                if stage + 1 < stages:
                    items[at].start(stage + 1)
        at = turn - stages
        if 0 <= at < count:
            items[at].finish()
    for item in items:
        item.drain()


def gather_all(shards, count):
    sizes = grid_of(count)
    copies = 400
    n = len(shards)
    fulls = pl.pallas_call(
        functools.partial(gather_kernel, sizes, n),
        out_shape=[jax.ShapeDtypeStruct((*sizes, 2, *s.shape), jnp.bfloat16) for s in shards],
        in_specs=[pl.BlockSpec(memory_space=pltpu.VMEM)] * n,
        out_specs=[pl.BlockSpec(memory_space=pltpu.HBM)] * n,
        scratch_shapes=[pltpu.VMEM(s.shape, jnp.bfloat16) for s in shards]
        + [pltpu.SemaphoreType.DMA((copies,)), pltpu.SemaphoreType.DMA((copies,)), pltpu.SemaphoreType.DMA((n,))],
        compiler_params=pltpu.CompilerParams(collective_id=0, has_side_effects=True),
        name="gather_all",
    )(*shards)
    return [full.reshape(-1, *full.shape[-2:]) for full in fulls]


def small_block(vectors, bias_up, me):
    wide = jnp.zeros((8, 128), jnp.float32)
    width = vectors.shape[1]
    per = 128 // width
    wide = lax.dynamic_update_slice(wide, vectors, (0, (me % per) * width))
    tail = jnp.zeros((8, 128), jnp.float32)
    span = bias_up.shape[0]
    tail = lax.dynamic_update_slice(tail, bias_up[None, :], (0, (me % (128 // span)) * span))
    return jnp.concatenate([wide, tail], axis=0)


def small_parts(small, vectors, bias_up):
    per = 128 // vectors.shape[1]
    span = 128 // bias_up.shape[0]
    n = small.shape[0]
    vec = jnp.sum(small[:, :8].astype(jnp.float32).reshape(n // per, per, 8, 128), axis=1)
    bias = jnp.sum(small[:, 8].astype(jnp.float32).reshape(n // span, span, 128), axis=1)
    return vec.transpose(1, 0, 2).reshape(8, -1).astype(jnp.bfloat16), bias.reshape(-1).astype(jnp.bfloat16)


F32, BF16 = jnp.float32, jnp.bfloat16


def nn(a, b):
    return lax.dot_general(a, b, (((1,), (0,)), ((), ())), preferred_element_type=F32)


def nt(a, b):
    return lax.dot_general(a, b, (((1,), (1,)), ((), ())), preferred_element_type=F32)


def tn(a, b):
    return lax.dot_general(a, b, (((0,), (0,)), ((), ())), preferred_element_type=F32)


def chunks(total, size, work):
    def step(i, carry):
        work(pl.ds(pl.multiple_of(i * size, size), size))
        return carry

    lax.fori_loop(0, total // size, step, 0)


def split_colours(start, shares, orders):
    found = []
    for order, share in zip(orders, shares):
        if share:
            found.append((start, share * 128, order))
            start += share * 128
    return found


def in_thirds(columns, last):
    tiles = columns // 128
    third = tiles * last // 8
    first = (tiles - third) // 2
    return first, tiles - third - first, third


class Spread:
    def __init__(self, full, own, rows, colours, place):
        self.full, self.own, self.rows, self.colours = full, own, rows, colours
        self.sizes, self.coords, self.core = place

    def view(self, colour, fixed, core):
        where = tuple(fixed.get(dim, slice(None)) for dim in range(3))
        return self.full.at[(*where, core, pl.ds(*self.rows), pl.ds(colour[0], colour[1]))]

    def sends(self, stage):
        for colour in self.colours:
            order = colour[2]
            dim = order[stage]
            held = self.view(colour, {d: self.coords[d] for d in order[stage:]}, self.core)
            source = held
            if stage == 0:
                source = self.own.at[pl.ds(*self.rows), pl.ds(colour[0], colour[1])]
            for step in range(1, self.sizes[dim]):
                peer = swapped(self.coords, dim, (self.coords[dim] + step) % self.sizes[dim])
                yield source, held, device_at(peer, self.core, self.sizes)

    def passed(self, stage):
        for colour in self.colours:
            order = colour[2]
            dim = order[stage]
            fixed = {d: self.coords[d] for d in order[stage + 1:]}
            if stage == 0:
                yield self.view(colour, fixed, self.core)
            else:
                for step in range(1, self.sizes[dim]):
                    yield self.view(colour, {**fixed, dim: (self.coords[dim] + step) % self.sizes[dim]}, self.core)


class Group:
    def __init__(self, sem, gauge):
        self.sem, self.gauge, self.units = sem, gauge, 0

    def count(self, ref):
        self.units += math.prod(ref.shape) * jnp.dtype(ref.dtype).itemsize // 256

    def wait(self):
        whole = self.gauge.at[pl.ds(0, self.units)]
        pltpu.make_async_copy(whole, whole, self.sem).wait()


class Chunk:
    def __init__(self, wires, parts):
        self.wires, self.parts = wires, parts
        self.arriving, self.swap = {}, wires.group()

    def start(self, stage):
        self.arriving[stage] = self.wires.group()
        for part in self.parts:
            for one in part.sends(stage):
                self.wires.send(*one, self.arriving[stage])

    def land(self, stage):
        self.arriving[stage].wait()

    def share(self, stage):
        for part in self.parts:
            for view in part.passed(stage):
                self.wires.send(view, view, self.wires.partner, self.swap)

    def finish(self):
        self.swap.wait()


class Wires:
    def __init__(self, send_sem, recv_sem, gauge, partner):
        self.recv_sem, self.gauge, self.partner = recv_sem, gauge, partner
        self.used, self.sent = 0, Group(send_sem.at[0], gauge)

    def group(self):
        self.used += 1
        assert self.used <= self.recv_sem.shape[0]
        return Group(self.recv_sem.at[self.used - 1], self.gauge)

    def send(self, src, dst, target, group):
        pltpu.make_async_remote_copy(
            src_ref=src, dst_ref=dst, send_sem=self.sent.sem, recv_sem=group.sem,
            device_id=(target,), device_id_type=MESH_ID,
        ).start()
        group.count(dst)
        self.sent.count(dst)

    def swap(self, src, dst):
        group = self.group()
        self.send(src, dst, self.partner, group)
        return group

    def drain(self):
        self.sent.wait()


class Reduce:
    def __init__(self, wires, held, rows, landing, colours, place):
        self.wires, self.held, self.rows, self.landing, self.colours = wires, held, rows, landing, colours
        self.sizes, self.coords, self.core = place

    def view(self, colour, fixed):
        where = tuple(fixed.get(dim, slice(None)) for dim in range(3))
        return self.held.at[(*where, pl.ds(*self.rows), pl.ds(colour[0], colour[1]))]

    def start(self, stage):
        self.arriving = self.wires.group()
        for at, colour in enumerate(self.colours):
            order = colour[2]
            dim = order[stage]
            fixed = {d: self.coords[d] for d in order[:stage]}
            for step in range(1, self.sizes[dim]):
                theirs = (self.coords[dim] + step) % self.sizes[dim]
                peer = swapped(self.coords, dim, theirs)
                self.wires.send(
                    self.view(colour, {**fixed, dim: theirs}),
                    self.landing[at][stage].at[step - 1],
                    device_at(peer, self.core, self.sizes), self.arriving,
                )

    def land(self):
        self.arriving.wait()

    def add(self, stage, out=None):
        first, rows = self.rows
        for at, colour in enumerate(self.colours):
            order = colour[2]
            fixed = {d: self.coords[d] for d in order[:stage + 1]}
            free = [d for d in range(3) if d not in fixed]
            landing = self.landing[at][stage]
            counts = [self.sizes[d] for d in free]
            total = math.prod(counts)
            tall = min(rows, 32)

            def step(i, carry, colour=colour, fixed=fixed, free=free, landing=landing, counts=counts, tall=tall):
                where, rest, index = dict(fixed), i // (rows // tall), []
                for d, size in zip(reversed(free), reversed(counts)):
                    where[d] = rest % size
                    index.insert(0, rest % size)
                    rest = rest // size
                low = (i % (rows // tall)) * tall
                span = pl.ds(pl.multiple_of(first + low, tall), tall)
                local = pl.ds(pl.multiple_of(low, tall), tall)
                place = (where[0], where[1], where[2], span, pl.ds(colour[0], colour[1]))
                sums = self.held[place].astype(F32)
                for other in range(landing.shape[0]):
                    sums = sums + landing[(other, *index, local, slice(None))].astype(F32)
                if out is None:
                    self.held[place] = sums.astype(self.held.dtype)
                else:
                    out[span, pl.ds(colour[0], colour[1])] = sums
                return carry

            lax.fori_loop(0, total * (rows // tall), step, 0)


def landing_shapes(rows, colours, sizes, dtype):
    found = []
    for _, width, order in colours:
        stages = []
        for stage in range(3):
            free = [sizes[d] for d in range(3) if d not in order[:stage + 1]]
            stages.append(pltpu.VMEM((sizes[order[stage]] - 1, *free, rows, width), dtype))
        found.append(stages)
    return found


def stream(count, source, slots, sem, work):
    def fetch(i, slot):
        return pltpu.make_async_copy(source(i), slots(slot), sem.at[slot])

    fetch(0, 0).start()

    def step(i, carry):
        slot = lax.rem(i, 2)

        @pl.when(i + 1 < count)
        def _():
            fetch(i + 1, 1 - slot).start()

        fetch(i, slot).wait()
        work(i, slot)
        return carry

    lax.fori_loop(0, count, step, 0)


def columns_of(i, width):
    return pl.ds(pl.multiple_of(i * width, width), width)


def row_stats(values):
    mean = jnp.mean(values, axis=-1, keepdims=True)
    centred = values - mean
    rstd = lax.rsqrt(jnp.mean(centred * centred, axis=-1, keepdims=True) + ln_eps)
    return centred * rstd, rstd


SMALL, OUT, QKV, UP, DOWN = range(5)


class Box(dict):
    __getattr__ = dict.__getitem__


def leaves(tree):
    if isinstance(tree, dict):
        tree = list(tree.values())
    if isinstance(tree, list):
        return [leaf for part in tree for leaf in leaves(part)]
    return [] if tree is None else [tree]


def shape_of(tree):
    if isinstance(tree, dict):
        return {name: shape_of(part) for name, part in tree.items()}
    if isinstance(tree, list):
        return [shape_of(part) for part in tree]
    return tree is not None


def unpack(shape, refs):
    if isinstance(shape, dict):
        return {name: unpack(part, refs) for name, part in shape.items()}
    if isinstance(shape, list):
        return [unpack(part, refs) for part in shape]
    return next(refs) if shape else None


GATHER_ORDERS = ((0, 1, 2), (0, 2, 1), (2, 1, 0))
REDUCE_ORDERS = ((2, 1, 0), (1, 2, 0), (0, 1, 2))
SIZES = (4, 2, 2)
TILE = 512


def step_kernel(names, *refs):
    r = Box(unpack(names, iter(refs)))
    sizes = SIZES
    me = lax.axis_index("dp")
    coords, core = locate(me, sizes)
    place = (sizes, coords, core)
    partner = device_at(coords, 1 - core, sizes)
    rows, d = r.tokens.shape
    ff = r.own[UP].shape[1]
    heads2 = d // 128
    slots = rows // MB_ROWS

    for which in (OUT, QKV, UP, DOWN):
        r.low[which][...] = r.own[which][...].astype(BF16)
    devices = math.prod(sizes) * 2
    per = devices * 128 // d
    block, narrow = r.block, 128 // per
    block[...] = jnp.zeros_like(block)
    for k in range(per):
        here = jnp.where(me % per == k, 1.0, 0.0)
        block[0:8, k * narrow:(k + 1) * narrow] = r.vectors[...] * here
    block[8:9, :] = r.bias_up[...]
    r.low[SMALL][...] = block[...].astype(BF16)
    greet(neighbours(coords, core, sizes))
    wires = Wires(r.send_sem, r.recv_sem, r.gauge, partner)

    def part(which, row_range, start, shares):
        colours = split_colours(start, shares, GATHER_ORDERS)
        return Spread(r.full[which], r.low[which], row_range, colours, place)

    mine = []
    for which in (SMALL, OUT, QKV, UP, DOWN):
        copy = pltpu.make_async_copy(r.low[which], r.full[which].at[(*coords, core)], r.mine_sem.at[which])
        copy.start()
        mine.append(copy)
    short, tall = r.own[OUT].shape[0], r.own[DOWN].shape[0]
    all_short = (0, short)
    half, half_ff = 3 * d // 2, ff // 2
    parcels = [
        Chunk(wires, [part(SMALL, (0, 16), 0, (1,)), part(OUT, all_short, 0, in_thirds(d, 0))]),
        Chunk(wires, [part(QKV, all_short, 0, in_thirds(half, 0))]),
        Chunk(wires, [part(QKV, all_short, half, in_thirds(half, 0))]),
        Chunk(wires, [part(UP, all_short, 0, in_thirds(half_ff, 0))]),
        Chunk(wires, [part(UP, all_short, half_ff, in_thirds(half_ff, 1))]),
        Chunk(wires, [part(DOWN, (0, tall // 2), 0, in_thirds(d, 2))]),
        Chunk(wires, [part(DOWN, (tall // 2, tall // 2), 0, in_thirds(d, 2))]),
    ]

    def begin_part(t):
        parcels[t].start(0)

    def first_axis(t):
        parcels[t].land(0)
        parcels[t].start(1)
        parcels[t].share(0)

    def second_axis(t):
        parcels[t].land(1)
        parcels[t].start(2)
        parcels[t].share(1)

    def third_axis(t):
        parcels[t].land(2)
        parcels[t].share(2)

    begin_part(0)
    begin_part(1)
    for slot in range(slots):
        span = pl.ds(slot * MB_ROWS, MB_ROWS)
        live = lax.broadcasted_iota(jnp.int32, (MB_ROWS, d), 0) < r.lengths[slot]
        r.dy[span, :] = jnp.where(live, r.cotangent[span, :].astype(F32), 0.0).astype(BF16)
    dy_swap = wires.swap(r.dy, r.dy_far)

    def norm_one(span):
        normed, _ = row_stats(r.tokens[span, :].astype(F32))
        r.da[span, :] = normed

    chunks(rows, 32, norm_one)
    for copy in mine:
        copy.wait()
    first_axis(0)
    begin_part(2)
    first_axis(1)
    begin_part(3)
    second_axis(0)
    first_axis(2)
    begin_part(4)
    second_axis(1)
    third_axis(0)
    first_axis(3)
    begin_part(5)
    second_axis(2)
    third_axis(1)
    parcels[0].finish()
    copy = pltpu.make_async_copy(r.full[SMALL], r.smalls, r.mine_sem.at[0])
    copy.start()
    copy.wait()
    flat = [(z, y, x, c) for z in range(sizes[0]) for y in range(sizes[1]) for x in range(sizes[2]) for c in range(2)]
    vec, bias = r.vec, r.bias
    for j in range(d // 128):
        total = 0.0
        for k in range(per):
            total = total + r.smalls[flat[j * per + k]].astype(F32)[0:8]
        vec[:, j * 128:(j + 1) * 128] = total
    for j in range(devices):
        bias[:, j * 128:(j + 1) * 128] = r.smalls[flat[j]].astype(F32)[8:9]

    def first_in(span):
        r.a[span, :] = (r.da[span, :] * vec[0:1, :] + vec[1:2, :]).astype(BF16)

    chunks(rows, 32, first_in)
    first_axis(4)
    begin_part(6)
    second_axis(3)
    third_axis(2)
    parcels[1].finish()
    first_axis(5)
    second_axis(4)
    parcels[2].finish()

    def transpose_out(source, turned, far):
        width = source.shape[1]
        block = turned.shape[2]
        group = max(1, 256 // (2 * block))

        def step(i, carry):
            value = source[:, columns_of(i, 2 * block * group)]
            flipped = value.astype(F32).T.astype(BF16)
            turned[pl.ds(i * group, group)] = flipped.reshape(group, 2, block, rows)
            return carry

        lax.fori_loop(0, width // (2 * block * group), step, 0)
        return wires.swap(turned.at[:, 1 - core], far)

    def tile_stream(which, low, high, work):
        full, slot = r.full[which], r.wide
        stream(
            (high - low) // TILE,
            lambda i: full.at[:, :, :, :, :, columns_of(i + low // TILE, TILE)],
            lambda s: slot.at[s],
            r.tile_sem,
            lambda i, s: work(i + low // TILE, slot[s].reshape(-1, TILE)),
        )

    def qkv_tile(i, tile):
        which = i * TILE // d
        values = nn(r.a[...], tile)
        shift = jnp.where(which == 0, 1.0, 0.0) * vec[2:3, columns_of(i % (d // TILE), TILE)] + jnp.where(
            which == 2, 1.0, 0.0
        ) * vec[3:4, columns_of(i % (d // TILE), TILE)]
        r.qkv[:, columns_of(i, TILE)] = (values + shift).astype(BF16)

    tile_stream(QKV, 0, 3 * d, qkv_tile)
    one_far = transpose_out(r.a, r.one_t, r.one_far)

    low_lane = lax.broadcasted_iota(jnp.int32, (MB_ROWS, 128), 1) < HEAD_DIM
    scale = 1.0 / math.sqrt(HEAD_DIM)

    def stacked(value):
        zero = jnp.zeros_like(value)
        return jnp.concatenate([jnp.where(low_lane, value, zero), jnp.where(low_lane, zero, value)], axis=0)

    def merged(value):
        return jnp.where(low_lane, value[:MB_ROWS], value[MB_ROWS:])

    def attend(p, carry):
        row = lax.broadcasted_iota(jnp.int32, (2 * MB_ROWS, 128), 0)
        dist = (row % MB_ROWS - lax.broadcasted_iota(jnp.int32, (2 * MB_ROWS, 128), 1)).astype(F32)
        head = (2 * p + row // MB_ROWS).astype(F32)
        alibi = jnp.where(dist >= 0, -jnp.exp2((head + 1.0) * (-8.0 / HEADS)) * dist, -1e30)
        for s in range(slots):
            span = pl.ds(s * MB_ROWS, MB_ROWS)
            q = r.qkv[span, columns_of(p, 128)]
            k = r.qkv[span, columns_of(p + heads2, 128)]
            v = r.qkv[span, columns_of(p + 2 * heads2, 128)]
            scores = nt(stacked(q), k) * scale + alibi
            top = jnp.max(scores, axis=-1, keepdims=True)
            grown = jnp.exp(scores - top)
            probs = grown / jnp.sum(grown, axis=-1, keepdims=True)
            r.probs[p * slots + s] = probs
            r.attn[span, columns_of(p, 128)] = merged(nn(probs.astype(BF16), v)).astype(BF16)
        return carry

    third_axis(3)
    lax.fori_loop(0, heads2, attend, 0)
    first_axis(6)
    second_axis(5)
    attn_far = transpose_out(r.attn, r.attn_t, r.attn_far)

    def out_tile(i, tile):
        span = columns_of(i, TILE)
        r.h1[:, span] = r.tokens[:, span].astype(F32) + nn(r.attn[...], tile) + vec[4:5, span]

    tile_stream(OUT, 0, d, out_tile)
    third_axis(4)
    parcels[3].finish()

    def second_in(span):
        normed, _ = row_stats(r.h1[span, :])
        r.a[span, :] = (normed * vec[5:6, :] + vec[6:7, :]).astype(BF16)

    chunks(rows, 32, second_in)
    two_far = transpose_out(r.a, r.two_t, r.two_far)

    def up_tile(i, tile):
        pre = nn(r.a[...], tile) + bias[:, columns_of(i, TILE)]
        value, slope = gelu_pair(pre)
        r.act[:, columns_of(i, TILE)] = value.astype(BF16)
        r.slope[:, columns_of(i, TILE)] = slope.astype(BF16)

    tile_stream(UP, 0, ff // 2, up_tile)
    second_axis(6)
    third_axis(5)
    parcels[4].finish()
    tile_stream(UP, ff // 2, ff, up_tile)
    act_far = transpose_out(r.act, r.act_t, r.act_far)
    dy_swap.wait()
    act_far.wait()

    reduces = [
        Reduce(wires, r.grad[which], span, landing, colours, place)
        for (which, span, colours), landing in zip(reduce_parts(short, tall, d, ff), r.landing)
    ]

    def weight_grad(which, turned, far, near_d, far_d, low, high):
        grad = r.grad[which]
        block = turned.shape[2]
        width = 512
        total = (high - low) // width
        groups = max(1, 16 * block // 512)
        each = 16 // groups

        def step(i, carry):
            at, g = i // groups, i % groups
            left = turned[pl.ds(g * each, each), core].reshape(each * block, rows)
            other = far[pl.ds(g * each, each)].reshape(each * block, rows)
            span = columns_of(at + low // width, width)
            value = nn(left, near_d[:, span]) + nn(other, far_d[:, span])
            value = value.astype(BF16)
            if groups == 1:
                grad[:, :, :, :, span] = value.reshape(*sizes, block, width)
            else:
                grad[g, :, :, :, span] = value.reshape(*sizes[1:], block, width)
            return carry

        assert groups in (1, sizes[0])
        lax.fori_loop(0, total * groups, step, 0)

    weight_grad(DOWN, r.act_t, r.act_far, r.dy, r.dy_far, 0, d)
    reduces[0].start(0)
    reduces[1].start(0)
    third_axis(6)
    parcels[5].finish()
    parcels[6].finish()

    sums = r.sums
    sums[...] = jnp.zeros_like(sums)
    acc = r.da

    def begin(span):
        acc[span, :] = r.h1[span, :] + vec[7:8, :]
        sums[7:8, :] += jnp.sum(r.dy[span, :].astype(F32), axis=0, keepdims=True)

    chunks(rows, 32, begin)

    def down_tile(i, s):
        tile = r.deep[s].reshape(-1, d)
        wide = tile.shape[0]
        span = columns_of(i, wide)
        acc[...] += nn(r.act[:, span], tile)
        d_pre = nt(r.dy[...], tile) * r.slope[:, span].astype(F32)
        r.bias_sum[:, span] = jnp.sum(d_pre, axis=0, keepdims=True)
        r.act[:, span] = d_pre.astype(BF16)

    full_down = r.full[DOWN]
    stream(
        sizes[0] * sizes[1],
        lambda i: full_down.at[i // sizes[1], i % sizes[1]],
        lambda s: r.deep.at[s],
        r.tile_sem,
        down_tile,
    )
    pre_swap = wires.swap(r.act, r.pre_far)
    r.output[...] = acc[...].astype(BF16)

    def row_stream(which, left):
        full, slot = r.full[which], r.flat
        width = full.shape[-1]

        def work(i, s):
            tile = slot[s, :, :, :, :, pl.ds(0, width)].reshape(-1, width)
            return nt(left[...], tile)

        def run(put):
            stream(
                sizes[0],
                lambda i: full.at[i],
                lambda s: slot.at[s, :, :, :, :, pl.ds(0, width)],
                r.tile_sem,
                lambda i, s: put(i, work(i, s)),
            )

        return run

    def put_da(i, value):
        r.da[:, columns_of(i, value.shape[1])] = value

    row_stream(UP, r.act)(put_da)

    def advance(part, stage):
        reduces[part].land()
        reduces[part].add(stage - 1)
        reduces[part].start(stage)

    def complete(part, which):
        reduces[part].land()
        reduces[part].add(2, r.final[which])

    advance(0, 1)
    two_far.wait()
    pre_swap.wait()
    weight_grad(UP, r.two_t, r.two_far, r.act, r.pre_far, 0, ff // 2)
    reduces[2].start(0)
    advance(1, 1)
    weight_grad(UP, r.two_t, r.two_far, r.act, r.pre_far, ff // 2, ff)
    reduces[3].start(0)

    def norm_two_back(span):
        normed, rstd = row_stats(r.h1[span, :])
        da = r.da[span, :]
        sums[5:6, :] += jnp.sum(da * normed, axis=0, keepdims=True)
        sums[6:7, :] += jnp.sum(da, axis=0, keepdims=True)
        d_h1 = r.dy[span, :].astype(F32) + norm_back(da, normed, rstd, vec[5:6, :])
        sums[4:5, :] += jnp.sum(d_h1, axis=0, keepdims=True)
        r.d_h1[span, :] = d_h1
        r.d_mid[span, :] = d_h1.astype(BF16)

    chunks(rows, 32, norm_two_back)
    mid_swap = wires.swap(r.d_mid, r.mid_far)

    def put_attn(i, value):
        r.d_attn[:, columns_of(i, value.shape[1])] = value.astype(BF16)

    row_stream(OUT, r.d_mid)(put_attn)

    advance(0, 2)

    def attend_back(p, carry):
        span_p = columns_of(p, 128)
        d_bq = jnp.zeros((1, 128), F32)
        d_bv = jnp.zeros((1, 128), F32)
        for s in range(slots):
            span = pl.ds(s * MB_ROWS, MB_ROWS)
            q = stacked(r.qkv[span, span_p])
            k = r.qkv[span, columns_of(p + heads2, 128)]
            v = r.qkv[span, columns_of(p + 2 * heads2, 128)]
            do = r.d_attn[span, span_p]
            probs = r.probs[p * slots + s]
            both = stacked(do)
            d_v = tn(probs.astype(BF16), both)
            d_probs = nt(both, v)
            weighed = do.astype(F32) * r.attn[span, span_p].astype(F32)
            delta = jnp.sum(stacked(weighed), axis=-1, keepdims=True)
            d_scores = (probs * (d_probs - delta)).astype(BF16)
            d_q = merged(nn(d_scores, k)) * scale
            d_k = tn(d_scores, q) * scale
            d_bq += jnp.sum(d_q, axis=0, keepdims=True)
            d_bv += jnp.sum(d_v, axis=0, keepdims=True)
            r.qkv[span, span_p] = d_q.astype(BF16)
            r.qkv[span, columns_of(p + heads2, 128)] = d_k.astype(BF16)
            r.qkv[span, columns_of(p + 2 * heads2, 128)] = d_v.astype(BF16)
        sums[2:3, span_p] = d_bq
        sums[3:4, span_p] = d_bv
        return carry

    lax.fori_loop(0, heads2 // 2, attend_back, 0)
    advance(1, 2)
    lax.fori_loop(heads2 // 2, heads2, attend_back, 0)
    qkv_swap = wires.swap(r.qkv, r.qkv_far)
    advance(2, 1)
    row_stream(QKV, r.qkv)(put_da)
    one_far.wait()
    qkv_swap.wait()
    weight_grad(QKV, r.one_t, r.one_far, r.qkv, r.qkv_far, 0, 3 * d // 2)
    reduces[4].start(0)
    advance(3, 1)
    weight_grad(QKV, r.one_t, r.one_far, r.qkv, r.qkv_far, 3 * d // 2, 3 * d)
    reduces[5].start(0)
    attn_far.wait()
    mid_swap.wait()
    weight_grad(OUT, r.attn_t, r.attn_far, r.d_mid, r.mid_far, 0, d)
    reduces[6].start(0)

    def norm_one_back(span):
        normed, rstd = row_stats(r.tokens[span, :].astype(F32))
        da = r.da[span, :]
        sums[0:1, :] += jnp.sum(da * normed, axis=0, keepdims=True)
        sums[1:2, :] += jnp.sum(da, axis=0, keepdims=True)
        r.input_grad[span, :] = r.d_h1[span, :] + norm_back(da, normed, rstd, vec[0:1, :])

    chunks(rows, 32, norm_one_back)

    bundle = r.bundle
    for j in range(devices):
        at = (j // per) * 128
        bundle[flat[j]] = jnp.concatenate(
            [sums[:, at:at + 128], jnp.broadcast_to(r.bias_sum[:, j * 128:(j + 1) * 128], (8, 128))], axis=0
        )
    tiny_swap = wires.swap(bundle.at[:, :, :, 1 - core], r.tiny_far)
    tiny = reduces[7]
    advance(2, 2)
    complete(0, DOWN)
    tiny_swap.wait()
    r.grad[SMALL][...] = bundle[:, :, :, core] + r.tiny_far[...]
    tiny.start(0)
    advance(4, 1)
    advance(3, 2)
    complete(1, DOWN)
    advance(7, 1)
    advance(5, 1)
    advance(6, 1)
    complete(2, UP)
    advance(4, 2)
    advance(7, 2)
    complete(3, UP)
    advance(5, 2)
    advance(6, 2)
    complete(7, SMALL)
    complete(4, QKV)
    complete(5, QKV)
    complete(6, OUT)
    wires.drain()


def reduce_parts(short, tall, d, ff):
    rows, half, half_ff = (0, short), 3 * d // 2, ff // 2

    def colours(start, width, last):
        return split_colours(start, in_thirds(width, last), REDUCE_ORDERS)

    return [
        (DOWN, (0, tall // 2), colours(0, d, 2)),
        (DOWN, (tall // 2, tall // 2), colours(0, d, 2)),
        (UP, rows, colours(0, half_ff, 1)),
        (UP, rows, colours(half_ff, half_ff, 1)),
        (QKV, rows, colours(0, half, 0)),
        (QKV, rows, colours(half, half, 0)),
        (OUT, rows, colours(0, d, 0)),
        (SMALL, (0, 16), [(0, 128, (2, 1, 0))]),
    ]


def fused_step(tokens, cotangent, lengths, vectors, bias_up, w_qkv, w_out, w_up, w_down):
    sizes = SIZES
    rows, d = tokens.shape
    ff = w_up.shape[1]
    short, tall = w_out.shape[0], w_down.shape[0]
    heads2 = d // 128
    slots = rows // MB_ROWS
    whole = lambda s: jax.ShapeDtypeStruct((*sizes, 2, *s), BF16)
    like = jax.ShapeDtypeStruct
    wide = ((16, 128), (short, d), (short, 3 * d), (short, ff), (tall, d))
    v = pltpu.VMEM
    turned, across = v((16, 2, short, rows), BF16), v((16, short, rows), BF16)
    flat, double = v((rows, d), BF16), v((rows, d), F32)
    inputs = dict(
        tokens=tokens, cotangent=cotangent, vectors=vectors, bias_up=bias_up, own=[None, w_out, w_qkv, w_up, w_down],
    )
    in_hbm = dict(full=[whole(s) for s in wide], gauge=like((180_224, 128), BF16))
    in_vmem = dict(
        output=like((rows, d), BF16), input_grad=like((rows, d), F32), final=[like(s, F32) for s in wide]
    )
    parts = reduce_parts(short, tall, d, ff)
    scratch = dict(
        low=[v(s, BF16) for s in wide], block=v((16, 128), F32), dy=flat,
        smalls=v((*sizes, 2, 16, 128), BF16), vec=v((8, d), F32), bias=v((1, ff), F32),
        dy_far=flat, da=double, a=flat, qkv=v((rows, 3 * d), BF16), qkv_far=v((rows, 3 * d), BF16),
        probs=v((heads2 * slots, 2 * MB_ROWS, 128), F32), attn=flat, h1=double,
        act=v((rows, ff), BF16), slope=v((rows, ff), BF16), pre_far=v((rows, ff), BF16),
        d_h1=double, d_mid=flat, mid_far=flat, d_attn=flat,
        one_t=turned, one_far=across, attn_t=turned, attn_far=across, two_t=turned, two_far=across,
        act_t=v((16, 2, tall, rows), BF16), act_far=v((16, tall, rows), BF16),
        wide=v((2, *sizes, 2, short, TILE), BF16), deep=v((2, sizes[2], 2, tall, d), BF16),
        flat=v((2, *sizes[1:], 2, short, ff), BF16),
        grad=[v((*sizes, *s), BF16 if at else F32) for at, s in enumerate(wide)],
        sums=v((8, d), F32), bias_sum=v((1, ff), F32),
        bundle=v((*sizes, 2, 16, 128), F32), tiny_far=v((*sizes, 16, 128), F32),
        landing=[
            landing_shapes(span[1], colours, sizes, BF16 if which else F32) for which, span, colours in parts
        ],
        send_sem=pltpu.SemaphoreType.DMA((1,)), recv_sem=pltpu.SemaphoreType.DMA((61,)),
        mine_sem=pltpu.SemaphoreType.DMA((5,)), tile_sem=pltpu.SemaphoreType.DMA((2,)),
    )
    names = {**dict(lengths=lengths), **inputs, **in_hbm, **in_vmem, **scratch}
    found = pl.pallas_call(
        functools.partial(step_kernel, shape_of(names)),
        out_shape=[*leaves(in_hbm), *leaves(in_vmem)],
        in_specs=[pl.BlockSpec(memory_space=pltpu.SMEM)]
        + [pl.BlockSpec(memory_space=v)] * len(leaves(inputs)),
        out_specs=[pl.BlockSpec(memory_space=pltpu.HBM)] * len(leaves(in_hbm))
        + [pl.BlockSpec(memory_space=v)] * len(leaves(in_vmem)),
        scratch_shapes=leaves(scratch),
        compiler_params=pltpu.CompilerParams(
            collective_id=1, has_side_effects=True, vmem_limit_bytes=67_000_000
        ),
        name="fused_step",
    )(lengths, *leaves(inputs))
    return Box(unpack(shape_of({**in_hbm, **in_vmem}), iter(found)))


def adam_kernel(shape, *refs):
    r = Box(unpack(shape, iter(refs)))
    me = lax.axis_index("dp")
    count = float(STEP)

    def put(at, param, first, second, grad):
        update, new_first, new_second = adamw(param, (first, second), grad, count)
        r.grads[at][...] = grad
        r.updates[at][...] = update
        r.firsts[at][...] = new_first
        r.seconds[at][...] = new_second

    for at in range(2, 6):
        put(at, r.params[at][...], r.moments[at][0], r.moments[at][1], r.final[at - 1][...])
    r.output[...] = r.early_output[...]
    r.input_grad[...] = r.early_grad[...]

    @pl.when(pl.program_id(0) == 0)
    def _():
        narrow = r.params[0].shape[1]
        per = 128 // narrow
        grad = jnp.zeros((8, narrow), F32)
        for k in range(per):
            grad = grad + jnp.where(me % per == k, 1.0, 0.0) * r.final[SMALL][0:8, k * narrow:(k + 1) * narrow]
        put(0, r.params[0][...], r.moments[0][0], r.moments[0][1], grad)
        put(1, r.params[1][...], r.moments[1][0:1], r.moments[1][1:2], r.final[SMALL][8:9, :])


def adam(found, params, moments):
    steps = 4

    def whole(s):
        return pl.BlockSpec(s, lambda i: (0,) * len(s))

    def cut(s):
        return pl.BlockSpec((*s[:-1], s[-1] // steps), lambda i: (0,) * (len(s) - 1) + (i,))

    def tall(s):
        return pl.BlockSpec((s[0] // steps, s[1]), lambda i: (i, 0))

    def each(make):
        return [make(p.shape) for p in params]

    like = jax.ShapeDtypeStruct
    outs = each(lambda s: like(s, F32))
    specs = [whole(p.shape) if at < 2 else cut(p.shape) for at, p in enumerate(params)]
    moment_specs = [whole(m.shape) if at < 2 else cut(m.shape) for at, m in enumerate(moments)]
    inputs = dict(
        params=list(params), moments=list(moments), final=found.final,
        early_output=found.output, early_grad=found.input_grad,
    )
    input_specs = dict(
        params=specs, moments=moment_specs, final=[whole((16, 128)), *specs[2:]],
        early_output=tall(found.output.shape), early_grad=tall(found.input_grad.shape),
    )
    results = dict(
        grads=outs, updates=outs, firsts=outs, seconds=outs,
        output=like(found.output.shape, BF16), input_grad=like(found.input_grad.shape, F32),
    )
    result_specs = dict(
        grads=specs, updates=specs, firsts=specs, seconds=specs,
        output=tall(found.output.shape), input_grad=tall(found.input_grad.shape),
    )
    shape = shape_of({**inputs, **results})
    done = pl.pallas_call(
        functools.partial(adam_kernel, shape),
        grid=(steps,),
        out_shape=leaves(results),
        in_specs=leaves(input_specs),
        out_specs=leaves(result_specs),
        compiler_params=pltpu.CompilerParams(vmem_limit_bytes=67_000_000),
        name="adam",
    )(*leaves(inputs))
    return Box(unpack(shape_of(results), iter(done)))


def general_body(
    tokens,
    cotangent,
    lengths,
    vectors,
    bias_up,
    w_qkv,
    w_out,
    w_up,
    w_down,
    mom_vectors,
    mom_bias_up,
    mom_qkv,
    mom_out,
    mom_up,
    mom_down,
):
    params = (vectors, bias_up, w_qkv, w_out, w_up, w_down)
    moments = (mom_vectors, mom_bias_up, mom_qkv, mom_out, mom_up, mom_down)
    me = lax.axis_index("dp")
    count = lax.axis_size("dp")
    small, full_out, full_qkv, full_up, full_down = gather_all(
        [small_block(vectors, bias_up, me), w_out, w_qkv, w_up, w_down], count
    )
    vec_low, bias_low = small_parts(small, vectors, bias_up)
    weights = (
        vec_low,
        bias_low,
        full_qkv.reshape(-1, w_qkv.shape[1]),
        full_out.reshape(-1, w_out.shape[1]),
        full_up.reshape(-1, w_up.shape[1]),
        full_down.reshape(-1, w_down.shape[1]),
    )
    alibi = alibi_bias(MB_ROWS)
    place = jnp.arange(MB_ROWS)
    owned = tuple((jnp.zeros(p.shape, jnp.float32) for p in params))
    summed = None
    out_list = []
    dx_list = []
    for micro in range(MICRO):
        x_rows = tokens[micro * MB_ROWS : (micro + 1) * MB_ROWS]
        live = place < lengths[micro]
        grad_rows = jnp.where(
            live[:, None],
            cotangent[micro * MB_ROWS : (micro + 1) * MB_ROWS],
            jnp.zeros((), jnp.bfloat16),
        )
        out, saved = forward_block(x_rows, weights, alibi)
        d_x, grads = backward_block(saved, grad_rows, weights, alibi)
        out_list.append(out)
        dx_list.append(d_x)
        summed = grads if summed is None else tuple((a + b for a, b in zip(summed, grads)))
    owned = (
        lax.psum_scatter(summed[0], "dp", scatter_dimension=1, tiled=True),
        lax.psum_scatter(summed[1], "dp", scatter_dimension=0, tiled=True),
        lax.psum_scatter(summed[2], "dp", scatter_dimension=0, tiled=True),
        lax.psum_scatter(summed[3], "dp", scatter_dimension=0, tiled=True),
        lax.psum_scatter(summed[4], "dp", scatter_dimension=0, tiled=True),
        lax.psum_scatter(summed[5], "dp", scatter_dimension=0, tiled=True),
    )
    count = float(STEP)
    news = [adamw(p, m, g, count) for p, m, g in zip(params, moments, owned)]
    output = jnp.concatenate(out_list, axis=0)
    input_grad = jnp.concatenate(dx_list, axis=0)
    return (
        output,
        input_grad,
        owned[0],
        owned[1],
        owned[2],
        owned[3],
        owned[4],
        owned[5],
        news[0][0],
        news[1][0],
        news[2][0],
        news[3][0],
        news[4][0],
        news[5][0],
        news[0][1],
        news[1][1],
        news[2][1],
        news[3][1],
        news[4][1],
        news[5][1],
        news[0][2],
        news[1][2],
        news[2][2],
        news[3][2],
        news[4][2],
        news[5][2],
    )


def body(
    tokens, cotangent, lengths, vectors, bias_up, w_qkv, w_out, w_up, w_down,
    mom_vectors, mom_bias_up, mom_qkv, mom_out, mom_up, mom_down,
):
    if grid_of(lax.axis_size("dp")) != SIZES:
        return general_body(
            tokens, cotangent, lengths, vectors, bias_up, w_qkv, w_out, w_up, w_down,
            mom_vectors, mom_bias_up, mom_qkv, mom_out, mom_up, mom_down,
        )
    span = bias_up.shape[0]
    found = fused_step(tokens, cotangent, lengths, vectors, bias_up.reshape(1, span), w_qkv, w_out, w_up, w_down)
    found.final[OUT], found.final[QKV] = found.final[QKV], found.final[OUT]
    done = adam(
        found,
        (vectors, bias_up.reshape(1, span), w_qkv, w_out, w_up, w_down),
        (mom_vectors, mom_bias_up, mom_qkv, mom_out, mom_up, mom_down),
    )

    def six(arrays):
        return (arrays[0], arrays[1].reshape(span), *arrays[2:])

    return (
        done.output, done.input_grad, *six(done.grads), *six(done.updates), *six(done.firsts), *six(done.seconds),
    )


def solution(mesh):
    in_specs = (
        P("dp", None),
        P("dp", None),
        P("dp"),
        P(None, "dp"),
        P("dp"),
        P("dp", None),
        P("dp", None),
        P("dp", None),
        P("dp", None),
        P(None, None, "dp"),
        P(None, "dp"),
        P(None, "dp", None),
        P(None, "dp", None),
        P(None, "dp", None),
        P(None, "dp", None),
    )
    out_specs = (
        P("dp", None),
        P("dp", None),
        P(None, "dp"),
        P("dp"),
        P("dp", None),
        P("dp", None),
        P("dp", None),
        P("dp", None),
        P(None, "dp"),
        P("dp"),
        P("dp", None),
        P("dp", None),
        P("dp", None),
        P("dp", None),
        P(None, "dp"),
        P("dp"),
        P("dp", None),
        P("dp", None),
        P("dp", None),
        P("dp", None),
        P(None, "dp"),
        P("dp"),
        P("dp", None),
        P("dp", None),
        P("dp", None),
        P("dp", None),
    )
    return jax.shard_map(body, mesh=mesh, in_specs=in_specs, out_specs=out_specs, check_vma=False)
```

```python
import functools
import math

import jax
import jax.numpy as jnp
from jax import lax
from jax.experimental import pallas as pl
from jax.experimental.pallas import tpu as pltpu
from jax.sharding import PartitionSpec as P

D = 1024
HEADS = 16
HEAD_DIM = 64
MB_ROWS = 128
MICRO = 2
STEP = 3


ln_eps = 1e-05
gelu_c = math.sqrt(2.0 / math.pi)
beta_one = 0.9
beta_two = 0.95
decay_rate = 0.1
adam_eps = 1e-08


def product(left, right):
    return jnp.dot(left, right, preferred_element_type=jnp.float32)


def contract(form, left, right):
    return jnp.einsum(form, left, right, preferred_element_type=jnp.float32)


def layer_norm(values, gain, shift):
    centred = values - jnp.mean(values, axis=-1, keepdims=True)
    rstd = lax.rsqrt(jnp.mean(centred * centred, axis=-1, keepdims=True) + ln_eps)
    normed = centred * rstd
    return (normed * gain + shift, normed, rstd)


def norm_back(grad_in, normed, rstd, gain):
    scaled = grad_in * gain
    inner = (
        scaled
        - jnp.mean(scaled, axis=-1, keepdims=True)
        - normed * jnp.mean(scaled * normed, axis=-1, keepdims=True)
    )
    return rstd * inner


def gelu_pair(pre):
    tanh_val = jnp.tanh(gelu_c * (pre + 0.044715 * pre * pre * pre))
    value = 0.5 * pre * (1.0 + tanh_val)
    slope = 0.5 * (1.0 + tanh_val) + 0.5 * pre * (1.0 - tanh_val * tanh_val) * gelu_c * (
        1.0 + 3.0 * 0.044715 * pre * pre
    )
    return (value, slope)


def alibi_bias(rows):
    place = jnp.arange(rows)
    dist = (place[:, None] - place[None, :]).astype(jnp.float32)
    slopes = jnp.exp2(-8.0 * (jnp.arange(HEADS) + 1).astype(jnp.float32) / HEADS)
    bias = -slopes[:, None, None] * dist[None]
    return jnp.where(dist[None] >= 0, bias, -1e30)


def attention_scores(q3, k3, alibi):
    return contract("qhd,khd->hqk", q3, k3) * (1.0 / math.sqrt(HEAD_DIM)) + alibi


def forward_block(x_rows, weights, alibi):
    vec, up_bias, qkv_w, out_w, up_w, down_w = weights
    vecf = vec.astype(jnp.float32)
    rows = x_rows.shape[0]
    xf = x_rows.astype(jnp.float32)
    ln_one, normed_one, rstd_one = layer_norm(xf, vecf[0], vecf[1])
    a_one = ln_one.astype(jnp.bfloat16)
    qkv = product(a_one, qkv_w)
    query = (qkv[:, :D] + vecf[2]).astype(jnp.bfloat16).reshape(rows, HEADS, HEAD_DIM)
    keyx = qkv[:, D : 2 * D].astype(jnp.bfloat16).reshape(rows, HEADS, HEAD_DIM)
    value = (qkv[:, 2 * D :] + vecf[3]).astype(jnp.bfloat16).reshape(rows, HEADS, HEAD_DIM)
    scores = attention_scores(query, keyx, alibi)
    top = jnp.max(scores, axis=-1, keepdims=True)
    lse = top + jnp.log(jnp.sum(jnp.exp(scores - top), axis=-1, keepdims=True))
    probs = jnp.exp(scores - lse).astype(jnp.bfloat16)
    attn = contract("hqk,khd->qhd", probs, value).reshape(rows, D).astype(jnp.bfloat16)
    h_one = xf + product(attn, out_w) + vecf[4]
    ln_two, normed_two, rstd_two = layer_norm(h_one, vecf[5], vecf[6])
    a_two = ln_two.astype(jnp.bfloat16)
    pre = product(a_two, up_w) + up_bias.astype(jnp.float32)
    act, slope = gelu_pair(pre)
    act_b = act.astype(jnp.bfloat16)
    out = (h_one + product(act_b, down_w) + vecf[7]).astype(jnp.bfloat16)
    saved = (
        normed_one,
        rstd_one,
        a_one,
        query,
        keyx,
        value,
        lse,
        attn,
        normed_two,
        rstd_two,
        a_two,
        slope,
        act_b,
    )
    return (out, saved)


def backward_block(saved, grad_rows, weights, alibi):
    vec, up_bias, qkv_w, out_w, up_w, down_w = weights
    vecf = vec.astype(jnp.float32)
    (
        normed_one,
        rstd_one,
        a_one,
        query,
        keyx,
        value,
        lse,
        attn,
        normed_two,
        rstd_two,
        a_two,
        slope,
        act_b,
    ) = saved
    rows = grad_rows.shape[0]
    scale = 1.0 / math.sqrt(HEAD_DIM)
    dyf = grad_rows.astype(jnp.float32)
    g_bdown = jnp.sum(dyf, axis=0)
    g_down = product(act_b.T, grad_rows)
    d_pre = product(grad_rows, down_w.T) * slope
    g_bup = jnp.sum(d_pre, axis=0)
    d_pre_b = d_pre.astype(jnp.bfloat16)
    g_up = product(a_two.T, d_pre_b)
    d_a2 = product(d_pre_b, up_w.T)
    g_ln2g = jnp.sum(d_a2 * normed_two, axis=0)
    g_ln2b = jnp.sum(d_a2, axis=0)
    d_h1 = dyf + norm_back(d_a2, normed_two, rstd_two, vecf[5])
    g_bout = jnp.sum(d_h1, axis=0)
    d_h1_b = d_h1.astype(jnp.bfloat16)
    g_out = product(attn.T, d_h1_b)
    d_attn = product(d_h1_b, out_w.T).astype(jnp.bfloat16).reshape(rows, HEADS, HEAD_DIM)
    probs_f = jnp.exp(attention_scores(query, keyx, alibi) - lse)
    probs = probs_f.astype(jnp.bfloat16)
    d_v = contract("hqk,qhd->khd", probs, d_attn).reshape(rows, D)
    d_probs = contract("qhd,khd->hqk", d_attn, value)
    delta = jnp.sum(
        d_attn.astype(jnp.float32) * attn.reshape(rows, HEADS, HEAD_DIM).astype(jnp.float32),
        axis=-1,
    ).T[:, :, None]
    d_scores = (probs_f * (d_probs - delta)).astype(jnp.bfloat16)
    d_q = (contract("hqk,khd->qhd", d_scores, keyx) * scale).reshape(rows, D)
    d_k = (contract("hqk,qhd->khd", d_scores, query) * scale).reshape(rows, D)
    g_bq = jnp.sum(d_q, axis=0)
    g_bv = jnp.sum(d_v, axis=0)
    d_qkv = jnp.concatenate([d_q, d_k, d_v], axis=1).astype(jnp.bfloat16)
    g_qkv = product(a_one.T, d_qkv)
    d_a1 = product(d_qkv, qkv_w.T)
    g_ln1g = jnp.sum(d_a1 * normed_one, axis=0)
    g_ln1b = jnp.sum(d_a1, axis=0)
    d_x = d_h1 + norm_back(d_a1, normed_one, rstd_one, vecf[0])
    g_vec = jnp.stack([g_ln1g, g_ln1b, g_bq, g_bv, g_bout, g_ln2g, g_ln2b, g_bdown])
    return (d_x, (g_vec, g_bup, g_qkv, g_out, g_up, g_down))


def adamw(param, moments, grad, count):
    first = beta_one * moments[0] + (1.0 - beta_one) * grad
    second = beta_two * moments[1] + (1.0 - beta_two) * grad * grad
    corr_one = 1.0 - beta_one**count
    corr_two = 1.0 - beta_two**count
    update = first / corr_one / (jnp.sqrt(second / corr_two) + adam_eps) + decay_rate * param
    return (update, first, second)


MESH_ID = pl.DeviceIdType.MESH


def grid_of(count):
    known = {32: (4, 2, 2), 128: (4, 4, 4)}
    return known.get(count, (count // 2,))


def locate(me, sizes):
    rest, coords = me // 2, []
    for size in reversed(sizes):
        coords.append(rest % size)
        rest = rest // size
    return tuple(reversed(coords)), me % 2


def device_at(coords, core, sizes):
    index = 0
    for value, size in zip(coords, sizes):
        index = index * size + value
    return index * 2 + core


def swapped(coords, dim, value):
    return tuple(value if at == dim else old for at, old in enumerate(coords))


def neighbours(coords, core, sizes):
    found = [device_at(coords, 1 - core, sizes)]
    for dim, size in enumerate(sizes):
        for step in range(1, size):
            found.append(device_at(swapped(coords, dim, (coords[dim] + step) % size), core, sizes))
    return found


def greet(others):
    barrier = pltpu.get_barrier_semaphore()
    for other in others:
        pl.semaphore_signal(barrier, inc=1, device_id=(other,), device_id_type=MESH_ID)
    pl.semaphore_wait(barrier, len(others))


class Sems:
    def __init__(self, send, recv):
        self.send, self.recv, self.used = send, recv, 0

    def pair(self):
        at = self.used
        self.used += 1
        return self.send.at[at], self.recv.at[at]


def remote(sems, src, dst, target):
    send_sem, recv_sem = sems.pair()
    copy = pltpu.make_async_remote_copy(
        src_ref=src, dst_ref=dst, send_sem=send_sem, recv_sem=recv_sem,
        device_id=(target,), device_id_type=MESH_ID,
    )
    copy.start()
    return copy


class Gather:
    def __init__(self, full, colours, sizes, coords, core, sems):
        self.full, self.colours, self.sizes = full, colours, sizes
        self.coords, self.core, self.sems = coords, core, sems
        self.axis = [[] for _ in colours]
        self.swap = []
        self.sent = []

    def view(self, colour, fixed):
        start, width, _ = colour
        place = tuple(fixed.get(dim, slice(None)) for dim in range(len(self.sizes)))
        return self.full.at[(*place, self.core, slice(None), pl.ds(start, width))]

    def start(self, stage, own=None):
        for at, colour in enumerate(self.colours):
            order = colour[2]
            dim = order[stage]
            fixed = {d: self.coords[d] for d in order[stage:]}
            held = self.view(colour, fixed)
            source = held if own is None else own.at[:, pl.ds(colour[0], colour[1])]
            self.axis[at] = []
            for step in range(1, self.sizes[dim]):
                peer = swapped(self.coords, dim, (self.coords[dim] + step) % self.sizes[dim])
                self.axis[at].append(remote(self.sems, source, held, device_at(peer, self.core, self.sizes)))
            self.sent += self.axis[at]

    def land(self, stage):
        partner = device_at(self.coords, 1 - self.core, self.sizes)
        for at, colour in enumerate(self.colours):
            order = colour[2]
            dim = order[stage]
            for copy in self.axis[at]:
                copy.wait_recv()
            fixed = {d: self.coords[d] for d in order[stage + 1:]}
            if stage == 0:
                views = [self.view(colour, fixed)]
            else:
                views = [
                    self.view(colour, {**fixed, dim: (self.coords[dim] + step) % self.sizes[dim]})
                    for step in range(1, self.sizes[dim])
                ]
            for view in views:
                self.swap.append(remote(self.sems, view, view, partner))

    def finish(self):
        for copy in self.swap:
            copy.wait_recv()

    def drain(self):
        for copy in self.sent + self.swap:
            copy.wait_send()


def colours_of(columns, sizes):
    last = len(sizes) - 1
    if last < 2:
        return [(0, columns, tuple(range(len(sizes))))]
    tiles = columns // 128
    if tiles < 8:
        return [(0, columns, (0, 1, 2))]
    third = max(1, tiles // 8)
    first = (tiles - third) // 2
    second = tiles - third - first
    return [
        (0, first * 128, (0, 1, 2)),
        (first * 128, second * 128, (0, 2, 1)),
        ((first + second) * 128, third * 128, (2, 1, 0)),
    ]


def gather_kernel(sizes, count, *refs):
    shards, fulls = refs[:count], refs[count : 2 * count]
    owns = refs[2 * count : 3 * count]
    send_sem, recv_sem, local_sem = refs[3 * count :]
    coords, core = locate(lax.axis_index("dp"), sizes)
    for shard, own in zip(shards, owns):
        own[...] = shard[...].astype(own.dtype)
    greet(neighbours(coords, core, sizes))
    sems = Sems(send_sem, recv_sem)
    items = [
        Gather(full, colours_of(full.shape[-1], sizes), sizes, coords, core, sems) for full in fulls
    ]
    local = []
    for at, (own, full) in enumerate(zip(owns, fulls)):
        copy = pltpu.make_async_copy(own, full.at[(*coords, core)], local_sem.at[at])
        copy.start()
        local.append(copy)
    stages = len(sizes)
    items[0].start(0, owns[0])
    for turn in range(count + stages):
        for stage in range(stages):
            at = turn - stage
            if 0 <= at < count:
                if stage == 0:
                    if at + 1 < count:
                        items[at + 1].start(0, owns[at + 1])
                    local[at].wait()
                items[at].land(stage)
                if stage + 1 < stages:
                    items[at].start(stage + 1)
        at = turn - stages
        if 0 <= at < count:
            items[at].finish()
    for item in items:
        item.drain()


def gather_all(shards, count):
    sizes = grid_of(count)
    copies = 400
    n = len(shards)
    fulls = pl.pallas_call(
        functools.partial(gather_kernel, sizes, n),
        out_shape=[jax.ShapeDtypeStruct((*sizes, 2, *s.shape), jnp.bfloat16) for s in shards],
        in_specs=[pl.BlockSpec(memory_space=pltpu.VMEM)] * n,
        out_specs=[pl.BlockSpec(memory_space=pltpu.HBM)] * n,
        scratch_shapes=[pltpu.VMEM(s.shape, jnp.bfloat16) for s in shards]
        + [pltpu.SemaphoreType.DMA((copies,)), pltpu.SemaphoreType.DMA((copies,)), pltpu.SemaphoreType.DMA((n,))],
        compiler_params=pltpu.CompilerParams(collective_id=0, has_side_effects=True),
        name="gather_all",
    )(*shards)
    return [full.reshape(-1, *full.shape[-2:]) for full in fulls]


def small_block(vectors, bias_up, me):
    wide = jnp.zeros((8, 128), jnp.float32)
    width = vectors.shape[1]
    per = 128 // width
    wide = lax.dynamic_update_slice(wide, vectors, (0, (me % per) * width))
    tail = jnp.zeros((8, 128), jnp.float32)
    span = bias_up.shape[0]
    tail = lax.dynamic_update_slice(tail, bias_up[None, :], (0, (me % (128 // span)) * span))
    return jnp.concatenate([wide, tail], axis=0)


def small_parts(small, vectors, bias_up):
    per = 128 // vectors.shape[1]
    span = 128 // bias_up.shape[0]
    n = small.shape[0]
    vec = jnp.sum(small[:, :8].astype(jnp.float32).reshape(n // per, per, 8, 128), axis=1)
    bias = jnp.sum(small[:, 8].astype(jnp.float32).reshape(n // span, span, 128), axis=1)
    return vec.transpose(1, 0, 2).reshape(8, -1).astype(jnp.bfloat16), bias.reshape(-1).astype(jnp.bfloat16)


F32, BF16 = jnp.float32, jnp.bfloat16


def nn(a, b):
    return lax.dot_general(a, b, (((1,), (0,)), ((), ())), preferred_element_type=F32)


def nt(a, b):
    return lax.dot_general(a, b, (((1,), (1,)), ((), ())), preferred_element_type=F32)


def tn(a, b):
    return lax.dot_general(a, b, (((0,), (0,)), ((), ())), preferred_element_type=F32)


def chunks(total, size, work):
    def step(i, carry):
        work(pl.ds(pl.multiple_of(i * size, size), size))
        return carry

    lax.fori_loop(0, total // size, step, 0)


def split_colours(start, shares, orders):
    found = []
    for order, share in zip(orders, shares):
        if share:
            found.append((start, share * 128, order))
            start += share * 128
    return found


def in_thirds(columns, last):
    tiles = columns // 128
    third = tiles * last // 8
    first = (tiles - third) // 2
    return first, tiles - third - first, third


class Spread:
    def __init__(self, full, own, rows, colours, relay, place):
        self.full, self.own, self.rows, self.colours = full, own, rows, colours
        self.sizes, self.coords, self.core = place
        self.hops = []
        for colour in colours:
            hops = []
            for at, dim in enumerate(colour[2]):
                fixed = {d: self.coords[d] for d in colour[2][at + 1:]}
                hops += [(dim, kind, fixed) for kind in ((1, 2) if dim == 0 and relay else (0,))]
            self.hops.append(hops)
        self.count = len(self.hops[0])

    def view(self, colour, fixed):
        where = tuple(fixed.get(dim, slice(None)) for dim in range(3))
        return self.full.at[(*where, self.core, pl.ds(*self.rows), pl.ds(colour[0], colour[1]))]

    def peer(self, dim, value):
        return device_at(swapped(self.coords, dim, value), self.core, self.sizes)

    def mine(self, at, hop):
        colour = self.colours[at]
        dim, kind, fixed = self.hops[at][hop]
        if kind == 2:
            low = self.coords[0] // 2 * 2
            return self.view(colour, {**fixed, 0: pl.ds(low, 2)})
        return self.view(colour, {**fixed, dim: self.coords[dim]})

    def far(self, at, hop):
        colour = self.colours[at]
        _, _, fixed = self.hops[at][hop]
        return self.view(colour, {**fixed, 0: pl.ds(2 - self.coords[0] // 2 * 2, 2)})

    def inner(self):
        return (self.coords[0] + 1) // 2 == 1

    def send(self, wires, hop, group):
        for at, colour in enumerate(self.colours):
            dim, kind, _ = self.hops[at][hop]
            held = self.mine(at, hop)
            source = held if hop else self.own.at[pl.ds(*self.rows), pl.ds(colour[0], colour[1])]
            here = self.coords[dim]
            if kind == 2:
                group.count(held)
                wires.send_if(self.inner(), source, held, self.peer(0, 3 - here), group)
            elif kind == 1:
                group.count(held)
                wires.send(source, held, self.peer(0, here + 1 - 2 * (here % 2)), group)
            else:
                for step in range(1, self.sizes[dim]):
                    group.count(held)
                    wires.send(source, held, self.peer(dim, (here + step) % self.sizes[dim]), group)

    def pass_on(self, wires, hop, group):
        here = self.coords[0]
        for at in range(len(self.colours)):
            if self.hops[at][hop][1] == 2:
                far = self.far(at, hop)
                wires.put(far, far, self.peer(0, here + 1 - 2 * (here % 2)), group, wires.sent_if)

    def arrived(self, hop):
        for at, colour in enumerate(self.colours):
            dim, kind, fixed = self.hops[at][hop]
            if hop == 0:
                yield self.view(colour, {**fixed, **({0: pl.ds(self.coords[0] // 2 * 2, 2)} if kind == 1 else {})})
            elif kind == 2:
                yield self.far(at, hop)
            elif kind == 1:
                yield self.view(colour, {**fixed, 0: self.coords[0] + 1 - 2 * (self.coords[0] % 2)})
            else:
                for step in range(1, self.sizes[dim]):
                    yield self.view(colour, {**fixed, dim: (self.coords[dim] + step) % self.sizes[dim]})


class Group:
    def __init__(self, sem, gauge):
        self.sem, self.gauge, self.units = sem, gauge, 0

    def count(self, ref):
        self.units += math.prod(ref.shape) * jnp.dtype(ref.dtype).itemsize // 256

    def wait(self):
        whole = self.gauge.at[pl.ds(0, self.units)]
        pltpu.make_async_copy(whole, whole, self.sem).wait()


class Chunk:
    def __init__(self, wires, parts):
        self.wires, self.parts = wires, parts
        self.arriving, self.swap, self.relayed = {}, wires.group(), set()
        self.hops = parts[0].count

    def start(self, hop):
        self.arriving[hop] = self.wires.group()
        for part in self.parts:
            part.send(self.wires, hop, self.arriving[hop])

    def relay(self, hop):
        def forward():
            self.arriving[hop].wait()
            for part in self.parts:
                part.pass_on(self.wires, hop, self.arriving[hop])

        pl.when(self.parts[0].inner())(forward)
        self.relayed.add(hop)

    def land(self, hop):
        if hop not in self.relayed and any(h[hop][1] == 2 for part in self.parts for h in part.hops):
            self.relay(hop)
        if hop in self.relayed:
            pl.when(jnp.logical_not(self.parts[0].inner()))(self.arriving[hop].wait)
        else:
            self.arriving[hop].wait()
        if hop + 1 < self.hops:
            self.start(hop + 1)
        for part in self.parts:
            for view in part.arrived(hop):
                self.swap.count(view)
                self.wires.send(view, view, self.wires.partner, self.swap)

    def finish(self):
        self.swap.wait()


class Wires:
    def __init__(self, send_sem, recv_sem, gauge, partner):
        self.recv_sem, self.gauge, self.partner = recv_sem, gauge, partner
        self.used, self.sent, self.sent_if = 0, Group(send_sem.at[0], gauge), Group(send_sem.at[1], gauge)
        self.condition = None

    def group(self):
        self.used += 1
        assert self.used <= self.recv_sem.shape[0]
        return Group(self.recv_sem.at[self.used - 1], self.gauge)

    def put(self, src, dst, target, group, sent=None):
        pltpu.make_async_remote_copy(
            src_ref=src, dst_ref=dst, send_sem=(sent or self.sent).sem, recv_sem=group.sem,
            device_id=(target,), device_id_type=MESH_ID,
        ).start()
        if sent is not None:
            sent.count(dst)

    def send(self, src, dst, target, group):
        self.put(src, dst, target, group, self.sent)

    def send_if(self, condition, src, dst, target, group):
        self.condition = condition
        pl.when(condition)(lambda: self.put(src, dst, target, group, self.sent_if))

    def swap(self, src, dst):
        group = self.group()
        group.count(dst)
        self.send(src, dst, self.partner, group)
        return group

    def drain(self):
        self.sent.wait()
        if self.condition is not None:
            pl.when(self.condition)(self.sent_if.wait)


class Reduce:
    def __init__(self, wires, held, rows, landing, colours, place):
        self.wires, self.held, self.rows, self.landing, self.colours = wires, held, rows, landing, colours
        self.sizes, self.coords, self.core = place

    def view(self, colour, fixed):
        where = tuple(fixed.get(dim, slice(None)) for dim in range(3))
        return self.held.at[(*where, pl.ds(*self.rows), pl.ds(colour[0], colour[1]))]

    def start(self, stage):
        self.arriving = self.wires.group()
        for at, colour in enumerate(self.colours):
            order = colour[2]
            dim = order[stage]
            fixed = {d: self.coords[d] for d in order[:stage]}
            for step in range(1, self.sizes[dim]):
                theirs = (self.coords[dim] + step) % self.sizes[dim]
                self.arriving.count(self.landing[at][stage].at[step - 1])
                peer = swapped(self.coords, dim, theirs)
                self.wires.send(
                    self.view(colour, {**fixed, dim: theirs}),
                    self.landing[at][stage].at[step - 1],
                    device_at(peer, self.core, self.sizes), self.arriving,
                )

    def land(self):
        self.arriving.wait()

    def add(self, stage, out=None):
        first, rows = self.rows
        for at, colour in enumerate(self.colours):
            order = colour[2]
            fixed = {d: self.coords[d] for d in order[:stage + 1]}
            free = [d for d in range(3) if d not in fixed]
            landing = self.landing[at][stage]
            counts = [self.sizes[d] for d in free]
            total = math.prod(counts)
            tall = min(rows, 32)

            def step(i, carry, colour=colour, fixed=fixed, free=free, landing=landing, counts=counts, tall=tall):
                where, rest, index = dict(fixed), i // (rows // tall), []
                for d, size in zip(reversed(free), reversed(counts)):
                    where[d] = rest % size
                    index.insert(0, rest % size)
                    rest = rest // size
                low = (i % (rows // tall)) * tall
                span = pl.ds(pl.multiple_of(first + low, tall), tall)
                local = pl.ds(pl.multiple_of(low, tall), tall)
                place = (where[0], where[1], where[2], span, pl.ds(colour[0], colour[1]))
                sums = self.held[place].astype(F32)
                for other in range(landing.shape[0]):
                    sums = sums + landing[(other, *index, local, slice(None))].astype(F32)
                if out is None:
                    self.held[place] = sums.astype(self.held.dtype)
                else:
                    out[span, pl.ds(colour[0], colour[1])] = sums
                return carry

            lax.fori_loop(0, total * (rows // tall), step, 0)


class LineReduce:
    def __init__(self, wires, held, columns, landing, place, last):
        self.wires, self.held, self.columns, self.landing = wires, held, columns, landing
        self.sizes, (self.z, self.y, self.x), self.core = place
        self.inner = (self.z + 1) // 2 == 1
        self.own, self.beside = self.z // 2 * 2, self.z + 1 - 2 * (self.z % 2)
        self.rest = (self.y, self.x) if last else (slice(None), slice(None))
        self.spread = (self.y, self.x) if last else ((0, 2), (0, 2))
        self.groups = [wires.group() for _ in landing]
        for group, ref in zip(self.groups, landing):
            group.count(ref)

    def push(self, at, chip, *where):
        source = self.held.at[(*where, slice(None), pl.ds(*self.columns))]
        self.wires.put(source, self.landing[at], device_at(chip, self.core, self.sizes), self.groups[at])

    def add(self, landing, *where, out=None):
        counts = list(landing.shape[:-2])
        rows, tall = landing.shape[-2], 32

        def step(i, carry):
            rest, index = i // (rows // tall), []
            for size in reversed(counts):
                index.insert(0, rest % size)
                rest = rest // size
            free, place = list(index), []
            for entry in where:
                if isinstance(entry, tuple):
                    place.append(entry[0] + free.pop(0))
                else:
                    place.append(entry)
            span = pl.ds(pl.multiple_of((i % (rows // tall)) * tall, tall), tall)
            place = (*place, span, pl.ds(*self.columns))
            sums = self.held[place].astype(F32) + landing[(*index, span, slice(None))].astype(F32)
            if out is None:
                self.held[place] = sums.astype(self.held.dtype)
            else:
                out[span, pl.ds(*self.columns)] = sums
            return carry

        lax.fori_loop(0, math.prod(counts) * (rows // tall), step, 0)

    def start(self):
        def outer():
            chip = (self.beside, self.y, self.x)
            self.push(0, chip, pl.ds(2 - self.own, 2), *self.rest)
            self.push(2, chip, self.beside, *self.rest)

        pl.when(jnp.logical_not(self.inner))(outer)
        self.wires.sent.count(self.landing[0])
        self.wires.sent.count(self.landing[2])

    def across(self):
        def middle():
            self.groups[0].wait()
            self.add(self.landing[0], (2 - self.own, 2), *self.spread)
            self.push(1, (3 - self.z, self.y, self.x), pl.ds(2 - self.own, 2), *self.rest)

        pl.when(self.inner)(middle)

    def back(self):
        def middle():
            self.groups[1].wait()
            self.add(self.landing[1], (self.own, 2), *self.spread)
            self.push(2, (self.beside, self.y, self.x), self.beside, *self.rest)

        pl.when(self.inner)(middle)

    def complete(self, out):
        self.groups[2].wait()
        self.add(self.landing[2], self.z, *self.spread, out=out)

    def second(self):
        self.complete(None)
        self.push(3, (self.z, 1 - self.y, self.x), self.z, 1 - self.y, slice(None))
        self.wires.sent.count(self.landing[3])

    def third(self):
        self.groups[3].wait()
        self.add(self.landing[3], self.z, self.y, (0, 2))
        self.push(4, (self.z, self.y, 1 - self.x), self.z, self.y, 1 - self.x)
        self.wires.sent.count(self.landing[4])

    def finish(self, out):
        self.groups[4].wait()
        self.add(self.landing[4], self.z, self.y, self.x, out=out)


def line_landing(rows, width, last):
    leads = ((2,), (2,), ()) if last else ((2, 2, 2), (2, 2, 2), (2, 2), (2,), ())
    return [pltpu.VMEM((*lead, rows, width), BF16) for lead in leads]


def landing_shapes(rows, colours, sizes, dtype, count=3):
    found = []
    for _, width, order in colours:
        stages = []
        for stage in range(count):
            free = [sizes[d] for d in range(3) if d not in order[:stage + 1]]
            stages.append(pltpu.VMEM((sizes[order[stage]] - 1, *free, rows, width), dtype))
        found.append(stages)
    return found


def stream(count, source, slots, sem, work):
    def fetch(i, slot):
        return pltpu.make_async_copy(source(i), slots(slot), sem.at[slot])

    fetch(0, 0).start()

    def step(i, carry):
        slot = lax.rem(i, 2)

        @pl.when(i + 1 < count)
        def _():
            fetch(i + 1, 1 - slot).start()

        fetch(i, slot).wait()
        work(i, slot)
        return carry

    lax.fori_loop(0, count, step, 0)


def columns_of(i, width):
    return pl.ds(pl.multiple_of(i * width, width), width)


def row_stats(values):
    mean = jnp.mean(values, axis=-1, keepdims=True)
    centred = values - mean
    rstd = lax.rsqrt(jnp.mean(centred * centred, axis=-1, keepdims=True) + ln_eps)
    return centred * rstd, rstd


SMALL, OUT, QKV, UP, DOWN = range(5)


class Box(dict):
    __getattr__ = dict.__getitem__


def leaves(tree):
    if isinstance(tree, dict):
        tree = list(tree.values())
    if isinstance(tree, list):
        return [leaf for part in tree for leaf in leaves(part)]
    return [] if tree is None else [tree]


def shape_of(tree):
    if isinstance(tree, dict):
        return {name: shape_of(part) for name, part in tree.items()}
    if isinstance(tree, list):
        return [shape_of(part) for part in tree]
    return tree is not None


def unpack(shape, refs):
    if isinstance(shape, dict):
        return {name: unpack(part, refs) for name, part in shape.items()}
    if isinstance(shape, list):
        return [unpack(part, refs) for part in shape]
    return next(refs) if shape else None


GATHER_ORDERS = ((0, 1, 2), (0, 2, 1), (2, 1, 0))
REDUCE_ORDERS = ((2, 1, 0), (1, 2, 0), (0, 1, 2))
SIZES = (4, 2, 2)
EARLY_TILES = 4
LATE_TILES = 4
UP_EIGHTHS = (0, 0)
TILE = 512


def step_kernel(names, *refs):
    r = Box(unpack(names, iter(refs)))
    sizes = SIZES
    me = lax.axis_index("dp")
    coords, core = locate(me, sizes)
    place = (sizes, coords, core)
    partner = device_at(coords, 1 - core, sizes)
    rows, d = r.tokens.shape
    ff = r.low[UP].shape[1]
    heads2 = d // 128
    slots = rows // MB_ROWS

    others = neighbours(coords, core, sizes)
    barrier = pltpu.get_barrier_semaphore()
    for other in others:
        pl.semaphore_signal(barrier, inc=1, device_id=(other,), device_id_type=MESH_ID)
    loads = []
    for at, (source, target) in enumerate(
        [(r.own[which], r.fin[which]) for which in (OUT, QKV, UP, DOWN)]
        + [(r.cotangent, r.dy), (r.tokens_in, r.tokens)]
    ):
        copy = pltpu.make_async_copy(source, target, r.load_sem.at[at])
        copy.start()
        loads.append(copy)
    devices = math.prod(sizes) * 2
    per = devices * 128 // d
    block, narrow = r.block, 128 // per
    block[...] = jnp.zeros_like(block)
    for k in range(per):
        here = jnp.where(me % per == k, 1.0, 0.0)
        block[0:8, k * narrow:(k + 1) * narrow] = r.vectors[...] * here
    block[8:9, :] = r.bias_up[...]
    r.low[SMALL][...] = block[...].astype(BF16)
    for at, which in enumerate((OUT, QKV, UP, DOWN)):
        loads[at].wait()
        r.low[which][...] = r.fin[which][...].astype(BF16)
    pl.semaphore_wait(barrier, len(others))
    wires = Wires(r.send_sem, r.recv_sem, r.gauge, partner)

    def part(which, row_range, start, shares, relay, orders=GATHER_ORDERS):
        colours = split_colours(start, shares, orders)
        return Spread(r.full[which], r.low[which], row_range, colours, relay, place)

    mine = []
    for which in (SMALL, OUT, QKV, UP, DOWN):
        copy = pltpu.make_async_copy(r.low[which], r.full[which].at[(*coords, core)], r.mine_sem.at[which])
        copy.start()
        mine.append(copy)
    short, tall = r.low[OUT].shape[0], r.low[DOWN].shape[0]
    all_short = (0, short)
    half, half_ff, early = 3 * d // 2, ff // 2, EARLY_TILES * 128
    rest = in_thirds(d - early, 0)
    first = Chunk(wires, [part(SMALL, (0, 16), 0, (1,), False), part(OUT, all_short, 0, in_thirds(d, 0), False)])
    qkv0 = Chunk(wires, [part(QKV, all_short, 0, in_thirds(half, 0), True)])
    qkv1 = Chunk(wires, [part(QKV, all_short, half, in_thirds(half, 0), True)])
    up0 = Chunk(wires, [part(UP, all_short, 0, in_thirds(half_ff, UP_EIGHTHS[0]), True)])
    up1 = Chunk(wires, [part(UP, all_short, half_ff, in_thirds(half_ff, UP_EIGHTHS[1]), True)])
    ahead = Chunk(wires, [part(DOWN, (0, tall), d - early, (EARLY_TILES,), True, GATHER_ORDERS[2:])])
    down0 = Chunk(wires, [part(DOWN, (0, tall // 2), 0, rest, True)])
    down1 = Chunk(wires, [part(DOWN, (tall // 2, tall // 2), 0, rest, True)])

    first.start(0)
    ahead.start(0)
    qkv0.start(0)
    qkv1.start(0)
    loads[4].wait()
    for slot in range(slots):
        span = pl.ds(slot * MB_ROWS, MB_ROWS)
        live = lax.broadcasted_iota(jnp.int32, (MB_ROWS, d), 0) < r.lengths[slot]
        r.dy[span, :] = jnp.where(live, r.dy[span, :].astype(F32), 0.0).astype(BF16)
    dy_swap = wires.swap(r.dy, r.dy_far)

    def norm_one(span):
        normed, _ = row_stats(r.tokens[span, :].astype(F32))
        r.da[span, :] = normed

    loads[5].wait()
    chunks(rows, 32, norm_one)
    for copy in mine:
        copy.wait()
    ahead.land(0)
    first.land(0)
    qkv0.land(0)
    up0.start(0)
    qkv1.land(0)
    qkv0.relay(1)
    first.land(1)
    up0.land(0)
    qkv0.land(1)
    up1.start(0)
    qkv1.relay(1)
    first.land(2)
    qkv1.land(1)
    up0.relay(1)
    qkv0.land(2)
    ahead.land(1)
    up1.land(0)
    up0.land(1)
    down0.start(0)
    up1.relay(1)
    qkv1.land(2)
    first.finish()
    qkv0.land(3)
    copy = pltpu.make_async_copy(r.full[SMALL], r.smalls, r.mine_sem.at[0])
    copy.start()
    copy.wait()
    flat = [(z, y, x, c) for z in range(sizes[0]) for y in range(sizes[1]) for x in range(sizes[2]) for c in range(2)]
    vec, bias = r.vec, r.bias
    for j in range(d // 128):
        total = 0.0
        for k in range(per):
            total = total + r.smalls[flat[j * per + k]].astype(F32)[0:8]
        vec[:, j * 128:(j + 1) * 128] = total
    for j in range(devices):
        bias[:, j * 128:(j + 1) * 128] = r.smalls[flat[j]].astype(F32)[8:9]

    def first_in(span):
        r.a[span, :] = (r.da[span, :] * vec[0:1, :] + vec[1:2, :]).astype(BF16)

    chunks(rows, 32, first_in)
    down0.land(0)
    up1.land(1)
    up0.land(2)
    down1.start(0)
    ahead.land(2)
    down0.relay(1)
    qkv1.land(3)
    qkv0.finish()
    down1.land(0)
    down0.land(1)
    up1.land(2)
    qkv1.finish()

    def transpose_out(source, turned, far, low=0, high=16):
        block = turned.shape[2]
        group = max(1, 256 // (2 * block))

        def step(i, carry):
            value = source[:, columns_of(i, 2 * block * group)]
            flipped = value.astype(F32).T.astype(BF16)
            turned[pl.ds(i * group, group)] = flipped.reshape(group, 2, block, rows)
            return carry

        lax.fori_loop(low // group, high // group, step, 0)
        span = pl.ds(low, high - low)
        return wires.swap(turned.at[span, 1 - core], far.at[span])

    def tile_stream(which, low, high, work):
        full, slot = r.full[which], r.wide
        stream(
            (high - low) // TILE,
            lambda i: full.at[:, :, :, :, :, columns_of(i + low // TILE, TILE)],
            lambda s: slot.at[s],
            r.tile_sem,
            lambda i, s: work(i + low // TILE, slot[s].reshape(-1, TILE)),
        )

    def qkv_tile(i, tile):
        which = i * TILE // d
        values = nn(r.a[...], tile)
        shift = jnp.where(which == 0, 1.0, 0.0) * vec[2:3, columns_of(i % (d // TILE), TILE)] + jnp.where(
            which == 2, 1.0, 0.0
        ) * vec[3:4, columns_of(i % (d // TILE), TILE)]
        r.qkv[:, columns_of(i, TILE)] = (values + shift).astype(BF16)

    tile_stream(QKV, 0, 3 * d, qkv_tile)
    one_far = transpose_out(r.a, r.one_t, r.one_far)

    low_lane = lax.broadcasted_iota(jnp.int32, (MB_ROWS, 128), 1) < HEAD_DIM
    scale = 1.0 / math.sqrt(HEAD_DIM)

    def stacked(value):
        zero = jnp.zeros_like(value)
        return jnp.concatenate([jnp.where(low_lane, value, zero), jnp.where(low_lane, zero, value)], axis=0)

    def merged(value):
        return jnp.where(low_lane, value[:MB_ROWS], value[MB_ROWS:])

    def attend(p, carry):
        row = lax.broadcasted_iota(jnp.int32, (2 * MB_ROWS, 128), 0)
        dist = (row % MB_ROWS - lax.broadcasted_iota(jnp.int32, (2 * MB_ROWS, 128), 1)).astype(F32)
        head = (2 * p + row // MB_ROWS).astype(F32)
        alibi = jnp.where(dist >= 0, -jnp.exp2((head + 1.0) * (-8.0 / HEADS)) * dist, -1e30)
        for s in range(slots):
            span = pl.ds(s * MB_ROWS, MB_ROWS)
            q = r.qkv[span, columns_of(p, 128)]
            k = r.qkv[span, columns_of(p + heads2, 128)]
            v = r.qkv[span, columns_of(p + 2 * heads2, 128)]
            scores = nt(stacked(q), k) * scale + alibi
            top = jnp.max(scores, axis=-1, keepdims=True)
            grown = jnp.exp(scores - top)
            probs = grown / jnp.sum(grown, axis=-1, keepdims=True)
            r.probs[p * slots + s] = probs
            r.attn[span, columns_of(p, 128)] = merged(nn(probs.astype(BF16), v)).astype(BF16)
        return carry

    down1.relay(1)
    up0.land(3)
    lax.fori_loop(0, heads2 // 2, attend, 0)
    down1.land(1)
    down0.land(2)
    ahead.relay(3)
    lax.fori_loop(heads2 // 2, heads2, attend, 0)
    attn_far = transpose_out(r.attn, r.attn_t, r.attn_far)

    def out_tile(i, tile):
        span = columns_of(i, TILE)
        r.h1[:, span] = r.tokens[:, span].astype(F32) + nn(r.attn[...], tile) + vec[4:5, span]

    tile_stream(OUT, 0, d, out_tile)
    up1.land(3)
    up0.finish()

    def second_in(span):
        normed, _ = row_stats(r.h1[span, :])
        r.a[span, :] = (normed * vec[5:6, :] + vec[6:7, :]).astype(BF16)

    chunks(rows, 32, second_in)
    two_far = transpose_out(r.a, r.two_t, r.two_far)
    down1.land(2)

    def up_tile(i, tile):
        pre = nn(r.a[...], tile) + bias[:, columns_of(i, TILE)]
        value, slope = gelu_pair(pre)
        r.act[:, columns_of(i, TILE)] = value.astype(BF16)
        r.slope[:, columns_of(i, TILE)] = slope.astype(BF16)

    tile_stream(UP, 0, ff // 2, up_tile)
    act_far0 = transpose_out(r.act, r.act_t, r.act_far, 0, 8)
    down0.land(3)
    up1.finish()
    tile_stream(UP, ff // 2, ff, up_tile)
    act_far1 = transpose_out(r.act, r.act_t, r.act_far, 8, 16)
    dy_swap.wait()
    act_far0.wait()
    act_far1.wait()

    reduces = [
        Reduce(wires, r.grad[which], span, landing, colours, place)
        for (which, span, colours), landing in zip(reduce_parts(short, tall, d, ff), r.landing)
    ]

    def weight_grad(which, turned, far, near_d, far_d, low, high):
        grad = r.grad[which]
        block = turned.shape[2]
        width = 512 if (high - low) % 512 == 0 and low % 512 == 0 else high - low
        total = (high - low) // width
        groups = max(1, 16 * block // 512)
        each = 16 // groups

        def step(i, carry):
            at, g = i // groups, i % groups
            left = turned[pl.ds(g * each, each), core].reshape(each * block, rows)
            other = far[pl.ds(g * each, each)].reshape(each * block, rows)
            span = pl.ds(pl.multiple_of(low + at * width, 128), width)
            value = nn(left, near_d[:, span]) + nn(other, far_d[:, span])
            value = value.astype(BF16)
            if groups == 1:
                grad[:, :, :, :, span] = value.reshape(*sizes, block, width)
            else:
                grad[g, :, :, :, span] = value.reshape(*sizes[1:], block, width)
            return carry

        assert groups in (1, sizes[0])
        lax.fori_loop(0, total * groups, step, 0)

    late = LATE_TILES * 128
    weight_grad(DOWN, r.act_t, r.act_far, r.dy, r.dy_far, d - late, d)
    line = LineReduce(wires, r.grad[DOWN], (d - late, late), r.line[0], place, False)
    line.start()
    weight_grad(DOWN, r.act_t, r.act_far, r.dy, r.dy_far, 0, d - late)
    reduces[0].start(0)
    reduces[1].start(0)
    ahead.land(3)
    down1.land(3)
    down0.finish()
    down1.finish()
    ahead.finish()

    sums = r.sums
    sums[...] = jnp.zeros_like(sums)
    acc = r.da

    def begin(span):
        acc[span, :] = r.h1[span, :] + vec[7:8, :]
        sums[7:8, :] += jnp.sum(r.dy[span, :].astype(F32), axis=0, keepdims=True)

    chunks(rows, 32, begin)

    def down_tile(i, s):
        tile = r.deep[s].reshape(-1, d)
        wide = tile.shape[0]
        span = columns_of(i, wide)
        acc[...] += nn(r.act[:, span], tile)
        d_pre = nt(r.dy[...], tile) * r.slope[:, span].astype(F32)
        r.bias_sum[:, span] = jnp.sum(d_pre, axis=0, keepdims=True)
        r.act[:, span] = d_pre.astype(BF16)

    full_down = r.full[DOWN]
    tiles = sizes[0] * sizes[1]

    def down_pass(low):
        stream(
            tiles // 2,
            lambda i: full_down.at[(i + low) // sizes[1], (i + low) % sizes[1]],
            lambda s: r.deep.at[s],
            r.tile_sem,
            lambda i, s: down_tile(i + low, s),
        )
        span = pl.ds(low * (ff // tiles), ff // 2)
        return wires.swap(r.act.at[:, span], r.pre_far.at[:, span])

    def advance(part, stage):
        reduces[part].land()
        reduces[part].add(stage - 1)
        reduces[part].start(stage)

    def complete(part, which):
        reduces[part].land()
        reduces[part].add(2, r.fin[which])

    down_line = LineReduce(wires, r.grad[DOWN], (0, d - late), r.line[1], place, True)
    up_lines = [
        LineReduce(wires, r.grad[UP], (at * ff // 2, ff // 2), r.line[2 + at], place, True) for at in range(2)
    ]

    def settle(part):
        reduces[part].land()
        reduces[part].add(1)

    pre_swap0 = down_pass(0)
    advance(0, 1)
    pre_swap1 = down_pass(tiles // 2)
    advance(1, 1)
    two_far.wait()
    pre_swap0.wait()
    weight_grad(UP, r.two_t, r.two_far, r.act, r.pre_far, 0, ff // 2)
    reduces[2].start(0)
    pre_swap1.wait()
    weight_grad(UP, r.two_t, r.two_far, r.act, r.pre_far, ff // 2, ff)
    reduces[3].start(0)
    r.a[...] = acc[...].astype(BF16)

    def row_stream(which, left):
        full, slot = r.full[which], r.flat
        width = full.shape[-1]

        def work(i, s):
            tile = slot[s, :, :, :, :, pl.ds(0, width)].reshape(-1, width)
            return nt(left[...], tile)

        def run(put):
            stream(
                sizes[0],
                lambda i: full.at[i],
                lambda s: slot.at[s, :, :, :, :, pl.ds(0, width)],
                r.tile_sem,
                lambda i, s: put(i, work(i, s)),
            )

        return run

    def put_da(i, value):
        r.da[:, columns_of(i, value.shape[1])] = value

    row_stream(UP, r.act)(put_da)

    line.across()

    def norm_two_back(span):
        normed, rstd = row_stats(r.h1[span, :])
        da = r.da[span, :]
        sums[5:6, :] += jnp.sum(da * normed, axis=0, keepdims=True)
        sums[6:7, :] += jnp.sum(da, axis=0, keepdims=True)
        d_h1 = r.dy[span, :].astype(F32) + norm_back(da, normed, rstd, vec[5:6, :])
        sums[4:5, :] += jnp.sum(d_h1, axis=0, keepdims=True)
        r.h1[span, :] = d_h1
        r.d_mid[span, :] = d_h1.astype(BF16)

    chunks(rows, 32, norm_two_back)
    stores = []

    def keep(source, target):
        copy = pltpu.make_async_copy(source, target, r.store_sem.at[len(stores)])
        copy.start()
        stores.append(copy)

    keep(r.a, r.output)
    mid_swap = wires.swap(r.d_mid, r.mid_far)

    def put_attn(i, value):
        r.d_attn[:, columns_of(i, value.shape[1])] = value.astype(BF16)

    row_stream(OUT, r.d_mid)(put_attn)

    advance(2, 1)
    settle(0)
    settle(1)
    down_line.start()
    attn_far.wait()
    mid_swap.wait()
    weight_grad(OUT, r.attn_t, r.attn_far, r.d_mid, r.mid_far, 0, d)

    def attend_back(p, carry):
        span_p = columns_of(p, 128)
        d_bq = jnp.zeros((1, 128), F32)
        d_bv = jnp.zeros((1, 128), F32)
        for s in range(slots):
            span = pl.ds(s * MB_ROWS, MB_ROWS)
            q = stacked(r.qkv[span, span_p])
            k = r.qkv[span, columns_of(p + heads2, 128)]
            v = r.qkv[span, columns_of(p + 2 * heads2, 128)]
            do = r.d_attn[span, span_p]
            probs = r.probs[p * slots + s]
            both = stacked(do)
            d_v = tn(probs.astype(BF16), both)
            d_probs = nt(both, v)
            weighed = do.astype(F32) * r.attn[span, span_p].astype(F32)
            delta = jnp.sum(stacked(weighed), axis=-1, keepdims=True)
            d_scores = (probs * (d_probs - delta)).astype(BF16)
            d_q = merged(nn(d_scores, k)) * scale
            d_k = tn(d_scores, q) * scale
            d_bq += jnp.sum(d_q, axis=0, keepdims=True)
            d_bv += jnp.sum(d_v, axis=0, keepdims=True)
            r.qkv[span, span_p] = d_q.astype(BF16)
            r.qkv[span, columns_of(p + heads2, 128)] = d_k.astype(BF16)
            r.qkv[span, columns_of(p + 2 * heads2, 128)] = d_v.astype(BF16)
        sums[2:3, span_p] = d_bq
        sums[3:4, span_p] = d_bv
        return carry

    lax.fori_loop(0, heads2 // 2, attend_back, 0)
    advance(3, 1)
    reduces[4].start(0)
    lax.fori_loop(heads2 // 2, heads2, attend_back, 0)
    qkv_swap = wires.swap(r.qkv, r.qkv_far)
    down_line.across()
    row_stream(QKV, r.qkv)(put_da)
    settle(2)
    up_lines[0].start()
    one_far.wait()
    qkv_swap.wait()
    weight_grad(QKV, r.one_t, r.one_far, r.qkv, r.qkv_far, 0, d)
    reduces[5].start(0)
    weight_grad(QKV, r.one_t, r.one_far, r.qkv, r.qkv_far, d, 2 * d)
    reduces[6].start(0)
    settle(3)
    up_lines[1].start()
    weight_grad(QKV, r.one_t, r.one_far, r.qkv, r.qkv_far, 2 * d, 3 * d)
    line.back()

    def norm_one_back(span):
        normed, rstd = row_stats(r.tokens[span, :].astype(F32))
        da = r.da[span, :]
        sums[0:1, :] += jnp.sum(da * normed, axis=0, keepdims=True)
        sums[1:2, :] += jnp.sum(da, axis=0, keepdims=True)
        r.h1[span, :] = r.h1[span, :] + norm_back(da, normed, rstd, vec[0:1, :])

    chunks(rows, 32, norm_one_back)
    down_line.back()

    bundle = r.bundle
    for j in range(devices):
        at = (j // per) * 128
        bundle[flat[j]] = jnp.concatenate(
            [sums[:, at:at + 128], jnp.broadcast_to(r.bias_sum[:, j * 128:(j + 1) * 128], (8, 128))], axis=0
        )
    tiny_swap = wires.swap(bundle.at[:, :, :, 1 - core], r.tiny_far)
    tiny = reduces[8]
    keep(r.h1, r.input_grad)
    advance(4, 1)
    up_lines[0].across()
    tiny_swap.wait()
    r.grad[SMALL][...] = bundle[:, :, :, core] + r.tiny_far[...]
    tiny.start(0)
    advance(5, 1)
    reduces[7].start(0)
    up_lines[1].across()
    line.second()
    down_line.complete(r.fin[DOWN])
    advance(6, 1)
    up_lines[0].back()
    advance(4, 2)
    advance(5, 2)
    up_lines[1].back()
    advance(7, 1)
    advance(6, 2)
    line.third()
    up_lines[0].complete(r.fin[UP])
    advance(7, 2)
    advance(8, 1)
    line.finish(r.fin[DOWN])
    keep(r.fin[DOWN], r.final[DOWN])
    advance(8, 2)
    up_lines[1].complete(r.fin[UP])
    complete(4, OUT)
    keep(r.fin[UP], r.final[UP])
    complete(5, QKV)
    keep(r.fin[OUT], r.final[OUT])
    complete(6, QKV)
    complete(8, SMALL)
    keep(r.fin[SMALL], r.final[SMALL])
    complete(7, QKV)
    keep(r.fin[QKV], r.final[QKV])
    for copy in stores:
        copy.wait()
    wires.drain()


def reduce_parts(short, tall, d, ff):
    rows, half_ff = (0, short), ff // 2

    def colours(start, width, last):
        return split_colours(start, in_thirds(width, last), REDUCE_ORDERS)

    return [
        (DOWN, (0, tall // 2), colours(0, d - LATE_TILES * 128, 0)),
        (DOWN, (tall // 2, tall // 2), colours(0, d - LATE_TILES * 128, 0)),
        (UP, rows, colours(0, half_ff, 0)),
        (UP, rows, colours(half_ff, half_ff, 0)),
        (OUT, rows, colours(0, d, 0)),
        (QKV, rows, colours(0, d, 0)),
        (QKV, rows, colours(d, d, 0)),
        (QKV, rows, colours(2 * d, d, 0)),
        (SMALL, (0, 16), [(0, 128, (2, 1, 0))]),
    ]


def fused_step(tokens, cotangent, lengths, vectors, bias_up, w_qkv, w_out, w_up, w_down):
    sizes = SIZES
    rows, d = tokens.shape
    ff = w_up.shape[1]
    short, tall = w_out.shape[0], w_down.shape[0]
    heads2 = d // 128
    slots = rows // MB_ROWS
    whole = lambda s: jax.ShapeDtypeStruct((*sizes, 2, *s), BF16)
    like = jax.ShapeDtypeStruct
    wide = ((16, 128), (short, d), (short, 3 * d), (short, ff), (tall, d))
    v = pltpu.VMEM
    turned, across = v((16, 2, short, rows), BF16), v((16, short, rows), BF16)
    flat, double = v((rows, d), BF16), v((rows, d), F32)
    near = dict(vectors=vectors, bias_up=bias_up)
    distant = dict(tokens_in=tokens, cotangent=cotangent, own=[None, w_out, w_qkv, w_up, w_down])
    results = dict(
        full=[whole(s) for s in wide], gauge=like((180_224, 128), BF16),
        output=like((rows, d), BF16), input_grad=like((rows, d), F32), final=[like(s, F32) for s in wide],
    )
    parts = reduce_parts(short, tall, d, ff)
    scratch = dict(
        low=[v(s, BF16) for s in wide], block=v((16, 128), F32), dy=flat, tokens=flat,
        fin=[v(s, F32) for s in wide],
        smalls=v((*sizes, 2, 16, 128), BF16), vec=v((8, d), F32), bias=v((1, ff), F32),
        dy_far=flat, da=double, a=flat, qkv=v((rows, 3 * d), BF16), qkv_far=v((rows, 3 * d), BF16),
        probs=v((heads2 * slots, 2 * MB_ROWS, 128), F32), attn=flat, h1=double,
        act=v((rows, ff), BF16), slope=v((rows, ff), BF16), pre_far=v((rows, ff), BF16),
        d_mid=flat, mid_far=flat, d_attn=flat,
        one_t=turned, one_far=across, attn_t=turned, attn_far=across, two_t=turned, two_far=across,
        act_t=v((16, 2, tall, rows), BF16), act_far=v((16, tall, rows), BF16),
        wide=v((2, *sizes, 2, short, TILE), BF16), deep=v((2, sizes[2], 2, tall, d), BF16),
        flat=v((2, *sizes[1:], 2, short, ff), BF16),
        grad=[v((*sizes, *s), BF16 if at else F32) for at, s in enumerate(wide)],
        sums=v((8, d), F32), bias_sum=v((1, ff), F32),
        bundle=v((*sizes, 2, 16, 128), F32), tiny_far=v((*sizes, 16, 128), F32),
        landing=[
            landing_shapes(span[1], colours, sizes, BF16 if which else F32, 2 if which in (UP, DOWN) else 3)
            for which, span, colours in parts
        ],
        line=[
            line_landing(tall, LATE_TILES * 128, False), line_landing(tall, d - LATE_TILES * 128, True),
            line_landing(short, ff // 2, True), line_landing(short, ff // 2, True),
        ],
        send_sem=pltpu.SemaphoreType.DMA((2,)), recv_sem=pltpu.SemaphoreType.DMA((91,)),
        mine_sem=pltpu.SemaphoreType.DMA((5,)), tile_sem=pltpu.SemaphoreType.DMA((2,)),
        load_sem=pltpu.SemaphoreType.DMA((6,)), store_sem=pltpu.SemaphoreType.DMA((7,)),
    )
    names = {**dict(lengths=lengths), **near, **distant, **results, **scratch}
    found = pl.pallas_call(
        functools.partial(step_kernel, shape_of(names)),
        out_shape=leaves(results),
        in_specs=[pl.BlockSpec(memory_space=pltpu.SMEM)]
        + [pl.BlockSpec(memory_space=v)] * len(leaves(near))
        + [pl.BlockSpec(memory_space=pltpu.HBM)] * len(leaves(distant)),
        out_specs=[pl.BlockSpec(memory_space=pltpu.HBM)] * len(leaves(results)),
        scratch_shapes=leaves(scratch),
        compiler_params=pltpu.CompilerParams(
            collective_id=1, has_side_effects=True, vmem_limit_bytes=67_000_000
        ),
        name="fused_step",
    )(lengths, *leaves(near), *leaves(distant))
    return Box(unpack(shape_of(results), iter(found)))


def adam_kernel(shape, *refs):
    r = Box(unpack(shape, iter(refs)))
    me = lax.axis_index("dp")
    count = float(STEP)

    def put(at, param, first, second, grad):
        update, new_first, new_second = adamw(param, (first, second), grad, count)
        r.grads[at][...] = grad
        r.updates[at][...] = update
        r.firsts[at][...] = new_first
        r.seconds[at][...] = new_second

    for at in range(2, 6):
        put(at, r.params[at][...], r.moments[at][0], r.moments[at][1], r.final[at - 1][...])
    r.output[...] = r.early_output[...]
    r.input_grad[...] = r.early_grad[...]

    @pl.when(pl.program_id(0) == 0)
    def _():
        narrow = r.params[0].shape[1]
        per = 128 // narrow
        grad = jnp.zeros((8, narrow), F32)
        for k in range(per):
            grad = grad + jnp.where(me % per == k, 1.0, 0.0) * r.final[SMALL][0:8, k * narrow:(k + 1) * narrow]
        put(0, r.params[0][...], r.moments[0][0], r.moments[0][1], grad)
        put(1, r.params[1][...], r.moments[1][0:1], r.moments[1][1:2], r.final[SMALL][8:9, :])


def adam(found, params, moments):
    steps = 4

    def whole(s):
        return pl.BlockSpec(s, lambda i: (0,) * len(s))

    def cut(s):
        return pl.BlockSpec((*s[:-1], s[-1] // steps), lambda i: (0,) * (len(s) - 1) + (i,))

    def tall(s):
        return pl.BlockSpec((s[0] // steps, s[1]), lambda i: (i, 0))

    def each(make):
        return [make(p.shape) for p in params]

    like = jax.ShapeDtypeStruct
    outs = each(lambda s: like(s, F32))
    specs = [whole(p.shape) if at < 2 else cut(p.shape) for at, p in enumerate(params)]
    moment_specs = [whole(m.shape) if at < 2 else cut(m.shape) for at, m in enumerate(moments)]
    inputs = dict(
        params=list(params), moments=list(moments), final=found.final,
        early_output=found.output, early_grad=found.input_grad,
    )
    input_specs = dict(
        params=specs, moments=moment_specs, final=[whole((16, 128)), *specs[2:]],
        early_output=tall(found.output.shape), early_grad=tall(found.input_grad.shape),
    )
    results = dict(
        grads=outs, updates=outs, firsts=outs, seconds=outs,
        output=like(found.output.shape, BF16), input_grad=like(found.input_grad.shape, F32),
    )
    result_specs = dict(
        grads=specs, updates=specs, firsts=specs, seconds=specs,
        output=tall(found.output.shape), input_grad=tall(found.input_grad.shape),
    )
    shape = shape_of({**inputs, **results})
    done = pl.pallas_call(
        functools.partial(adam_kernel, shape),
        grid=(steps,),
        out_shape=leaves(results),
        in_specs=leaves(input_specs),
        out_specs=leaves(result_specs),
        compiler_params=pltpu.CompilerParams(vmem_limit_bytes=67_000_000),
        name="adam",
    )(*leaves(inputs))
    return Box(unpack(shape_of(results), iter(done)))


def general_body(
    tokens,
    cotangent,
    lengths,
    vectors,
    bias_up,
    w_qkv,
    w_out,
    w_up,
    w_down,
    mom_vectors,
    mom_bias_up,
    mom_qkv,
    mom_out,
    mom_up,
    mom_down,
):
    params = (vectors, bias_up, w_qkv, w_out, w_up, w_down)
    moments = (mom_vectors, mom_bias_up, mom_qkv, mom_out, mom_up, mom_down)
    me = lax.axis_index("dp")
    count = lax.axis_size("dp")
    small, full_out, full_qkv, full_up, full_down = gather_all(
        [small_block(vectors, bias_up, me), w_out, w_qkv, w_up, w_down], count
    )
    vec_low, bias_low = small_parts(small, vectors, bias_up)
    weights = (
        vec_low,
        bias_low,
        full_qkv.reshape(-1, w_qkv.shape[1]),
        full_out.reshape(-1, w_out.shape[1]),
        full_up.reshape(-1, w_up.shape[1]),
        full_down.reshape(-1, w_down.shape[1]),
    )
    alibi = alibi_bias(MB_ROWS)
    place = jnp.arange(MB_ROWS)
    owned = tuple((jnp.zeros(p.shape, jnp.float32) for p in params))
    summed = None
    out_list = []
    dx_list = []
    for micro in range(MICRO):
        x_rows = tokens[micro * MB_ROWS : (micro + 1) * MB_ROWS]
        live = place < lengths[micro]
        grad_rows = jnp.where(
            live[:, None],
            cotangent[micro * MB_ROWS : (micro + 1) * MB_ROWS],
            jnp.zeros((), jnp.bfloat16),
        )
        out, saved = forward_block(x_rows, weights, alibi)
        d_x, grads = backward_block(saved, grad_rows, weights, alibi)
        out_list.append(out)
        dx_list.append(d_x)
        summed = grads if summed is None else tuple((a + b for a, b in zip(summed, grads)))
    owned = (
        lax.psum_scatter(summed[0], "dp", scatter_dimension=1, tiled=True),
        lax.psum_scatter(summed[1], "dp", scatter_dimension=0, tiled=True),
        lax.psum_scatter(summed[2], "dp", scatter_dimension=0, tiled=True),
        lax.psum_scatter(summed[3], "dp", scatter_dimension=0, tiled=True),
        lax.psum_scatter(summed[4], "dp", scatter_dimension=0, tiled=True),
        lax.psum_scatter(summed[5], "dp", scatter_dimension=0, tiled=True),
    )
    count = float(STEP)
    news = [adamw(p, m, g, count) for p, m, g in zip(params, moments, owned)]
    output = jnp.concatenate(out_list, axis=0)
    input_grad = jnp.concatenate(dx_list, axis=0)
    return (
        output,
        input_grad,
        owned[0],
        owned[1],
        owned[2],
        owned[3],
        owned[4],
        owned[5],
        news[0][0],
        news[1][0],
        news[2][0],
        news[3][0],
        news[4][0],
        news[5][0],
        news[0][1],
        news[1][1],
        news[2][1],
        news[3][1],
        news[4][1],
        news[5][1],
        news[0][2],
        news[1][2],
        news[2][2],
        news[3][2],
        news[4][2],
        news[5][2],
    )


def body(
    tokens, cotangent, lengths, vectors, bias_up, w_qkv, w_out, w_up, w_down,
    mom_vectors, mom_bias_up, mom_qkv, mom_out, mom_up, mom_down,
):
    if grid_of(lax.axis_size("dp")) != SIZES:
        return general_body(
            tokens, cotangent, lengths, vectors, bias_up, w_qkv, w_out, w_up, w_down,
            mom_vectors, mom_bias_up, mom_qkv, mom_out, mom_up, mom_down,
        )
    span = bias_up.shape[0]
    found = fused_step(tokens, cotangent, lengths, vectors, bias_up.reshape(1, span), w_qkv, w_out, w_up, w_down)
    found.final[OUT], found.final[QKV] = found.final[QKV], found.final[OUT]
    done = adam(
        found,
        (vectors, bias_up.reshape(1, span), w_qkv, w_out, w_up, w_down),
        (mom_vectors, mom_bias_up, mom_qkv, mom_out, mom_up, mom_down),
    )

    def six(arrays):
        return (arrays[0], arrays[1].reshape(span), *arrays[2:])

    return (
        done.output, done.input_grad, *six(done.grads), *six(done.updates), *six(done.firsts), *six(done.seconds),
    )


def solution(mesh):
    in_specs = (
        P("dp", None),
        P("dp", None),
        P("dp"),
        P(None, "dp"),
        P("dp"),
        P("dp", None),
        P("dp", None),
        P("dp", None),
        P("dp", None),
        P(None, None, "dp"),
        P(None, "dp"),
        P(None, "dp", None),
        P(None, "dp", None),
        P(None, "dp", None),
        P(None, "dp", None),
    )
    out_specs = (
        P("dp", None),
        P("dp", None),
        P(None, "dp"),
        P("dp"),
        P("dp", None),
        P("dp", None),
        P("dp", None),
        P("dp", None),
        P(None, "dp"),
        P("dp"),
        P("dp", None),
        P("dp", None),
        P("dp", None),
        P("dp", None),
        P(None, "dp"),
        P("dp"),
        P("dp", None),
        P("dp", None),
        P("dp", None),
        P("dp", None),
        P(None, "dp"),
        P("dp"),
        P("dp", None),
        P("dp", None),
        P("dp", None),
        P("dp", None),
    )
    return jax.shard_map(body, mesh=mesh, in_specs=in_specs, out_specs=out_specs, check_vma=False)
```

```python
import functools
import math

import jax
import jax.numpy as jnp
from jax import lax
from jax.experimental import pallas as pl
from jax.experimental.pallas import tpu as pltpu
from jax.sharding import PartitionSpec as P

D = 1024
HEADS = 16
HEAD_DIM = 64
MB_ROWS = 128
MICRO = 2
STEP = 3


ln_eps = 1e-05
gelu_c = math.sqrt(2.0 / math.pi)
beta_one = 0.9
beta_two = 0.95
decay_rate = 0.1
adam_eps = 1e-08


def product(left, right):
    return jnp.dot(left, right, preferred_element_type=jnp.float32)


def contract(form, left, right):
    return jnp.einsum(form, left, right, preferred_element_type=jnp.float32)


def layer_norm(values, gain, shift):
    centred = values - jnp.mean(values, axis=-1, keepdims=True)
    rstd = lax.rsqrt(jnp.mean(centred * centred, axis=-1, keepdims=True) + ln_eps)
    normed = centred * rstd
    return (normed * gain + shift, normed, rstd)


def norm_back(grad_in, normed, rstd, gain):
    scaled = grad_in * gain
    inner = (
        scaled
        - jnp.mean(scaled, axis=-1, keepdims=True)
        - normed * jnp.mean(scaled * normed, axis=-1, keepdims=True)
    )
    return rstd * inner


def gelu_pair(pre):
    tanh_val = jnp.tanh(gelu_c * (pre + 0.044715 * pre * pre * pre))
    value = 0.5 * pre * (1.0 + tanh_val)
    slope = 0.5 * (1.0 + tanh_val) + 0.5 * pre * (1.0 - tanh_val * tanh_val) * gelu_c * (
        1.0 + 3.0 * 0.044715 * pre * pre
    )
    return (value, slope)


def alibi_bias(rows):
    place = jnp.arange(rows)
    dist = (place[:, None] - place[None, :]).astype(jnp.float32)
    slopes = jnp.exp2(-8.0 * (jnp.arange(HEADS) + 1).astype(jnp.float32) / HEADS)
    bias = -slopes[:, None, None] * dist[None]
    return jnp.where(dist[None] >= 0, bias, -1e30)


def attention_scores(q3, k3, alibi):
    return contract("qhd,khd->hqk", q3, k3) * (1.0 / math.sqrt(HEAD_DIM)) + alibi


def forward_block(x_rows, weights, alibi):
    vec, up_bias, qkv_w, out_w, up_w, down_w = weights
    vecf = vec.astype(jnp.float32)
    rows = x_rows.shape[0]
    xf = x_rows.astype(jnp.float32)
    ln_one, normed_one, rstd_one = layer_norm(xf, vecf[0], vecf[1])
    a_one = ln_one.astype(jnp.bfloat16)
    qkv = product(a_one, qkv_w)
    query = (qkv[:, :D] + vecf[2]).astype(jnp.bfloat16).reshape(rows, HEADS, HEAD_DIM)
    keyx = qkv[:, D : 2 * D].astype(jnp.bfloat16).reshape(rows, HEADS, HEAD_DIM)
    value = (qkv[:, 2 * D :] + vecf[3]).astype(jnp.bfloat16).reshape(rows, HEADS, HEAD_DIM)
    scores = attention_scores(query, keyx, alibi)
    top = jnp.max(scores, axis=-1, keepdims=True)
    lse = top + jnp.log(jnp.sum(jnp.exp(scores - top), axis=-1, keepdims=True))
    probs = jnp.exp(scores - lse).astype(jnp.bfloat16)
    attn = contract("hqk,khd->qhd", probs, value).reshape(rows, D).astype(jnp.bfloat16)
    h_one = xf + product(attn, out_w) + vecf[4]
    ln_two, normed_two, rstd_two = layer_norm(h_one, vecf[5], vecf[6])
    a_two = ln_two.astype(jnp.bfloat16)
    pre = product(a_two, up_w) + up_bias.astype(jnp.float32)
    act, slope = gelu_pair(pre)
    act_b = act.astype(jnp.bfloat16)
    out = (h_one + product(act_b, down_w) + vecf[7]).astype(jnp.bfloat16)
    saved = (
        normed_one,
        rstd_one,
        a_one,
        query,
        keyx,
        value,
        lse,
        attn,
        normed_two,
        rstd_two,
        a_two,
        slope,
        act_b,
    )
    return (out, saved)


def backward_block(saved, grad_rows, weights, alibi):
    vec, up_bias, qkv_w, out_w, up_w, down_w = weights
    vecf = vec.astype(jnp.float32)
    (
        normed_one,
        rstd_one,
        a_one,
        query,
        keyx,
        value,
        lse,
        attn,
        normed_two,
        rstd_two,
        a_two,
        slope,
        act_b,
    ) = saved
    rows = grad_rows.shape[0]
    scale = 1.0 / math.sqrt(HEAD_DIM)
    dyf = grad_rows.astype(jnp.float32)
    g_bdown = jnp.sum(dyf, axis=0)
    g_down = product(act_b.T, grad_rows)
    d_pre = product(grad_rows, down_w.T) * slope
    g_bup = jnp.sum(d_pre, axis=0)
    d_pre_b = d_pre.astype(jnp.bfloat16)
    g_up = product(a_two.T, d_pre_b)
    d_a2 = product(d_pre_b, up_w.T)
    g_ln2g = jnp.sum(d_a2 * normed_two, axis=0)
    g_ln2b = jnp.sum(d_a2, axis=0)
    d_h1 = dyf + norm_back(d_a2, normed_two, rstd_two, vecf[5])
    g_bout = jnp.sum(d_h1, axis=0)
    d_h1_b = d_h1.astype(jnp.bfloat16)
    g_out = product(attn.T, d_h1_b)
    d_attn = product(d_h1_b, out_w.T).astype(jnp.bfloat16).reshape(rows, HEADS, HEAD_DIM)
    probs_f = jnp.exp(attention_scores(query, keyx, alibi) - lse)
    probs = probs_f.astype(jnp.bfloat16)
    d_v = contract("hqk,qhd->khd", probs, d_attn).reshape(rows, D)
    d_probs = contract("qhd,khd->hqk", d_attn, value)
    delta = jnp.sum(
        d_attn.astype(jnp.float32) * attn.reshape(rows, HEADS, HEAD_DIM).astype(jnp.float32),
        axis=-1,
    ).T[:, :, None]
    d_scores = (probs_f * (d_probs - delta)).astype(jnp.bfloat16)
    d_q = (contract("hqk,khd->qhd", d_scores, keyx) * scale).reshape(rows, D)
    d_k = (contract("hqk,qhd->khd", d_scores, query) * scale).reshape(rows, D)
    g_bq = jnp.sum(d_q, axis=0)
    g_bv = jnp.sum(d_v, axis=0)
    d_qkv = jnp.concatenate([d_q, d_k, d_v], axis=1).astype(jnp.bfloat16)
    g_qkv = product(a_one.T, d_qkv)
    d_a1 = product(d_qkv, qkv_w.T)
    g_ln1g = jnp.sum(d_a1 * normed_one, axis=0)
    g_ln1b = jnp.sum(d_a1, axis=0)
    d_x = d_h1 + norm_back(d_a1, normed_one, rstd_one, vecf[0])
    g_vec = jnp.stack([g_ln1g, g_ln1b, g_bq, g_bv, g_bout, g_ln2g, g_ln2b, g_bdown])
    return (d_x, (g_vec, g_bup, g_qkv, g_out, g_up, g_down))


def adamw(param, moments, grad, count):
    first = beta_one * moments[0] + (1.0 - beta_one) * grad
    second = beta_two * moments[1] + (1.0 - beta_two) * grad * grad
    corr_one = 1.0 - beta_one**count
    corr_two = 1.0 - beta_two**count
    update = first / corr_one / (jnp.sqrt(second / corr_two) + adam_eps) + decay_rate * param
    return (update, first, second)


MESH_ID = pl.DeviceIdType.MESH


def grid_of(count):
    known = {32: (4, 2, 2), 128: (4, 4, 4)}
    return known.get(count, (count // 2,))


def locate(me, sizes):
    rest, coords = me // 2, []
    for size in reversed(sizes):
        coords.append(rest % size)
        rest = rest // size
    return tuple(reversed(coords)), me % 2


def device_at(coords, core, sizes):
    index = 0
    for value, size in zip(coords, sizes):
        index = index * size + value
    return index * 2 + core


def swapped(coords, dim, value):
    return tuple(value if at == dim else old for at, old in enumerate(coords))


def neighbours(coords, core, sizes):
    found = [device_at(coords, 1 - core, sizes)]
    for dim, size in enumerate(sizes):
        for step in range(1, size):
            found.append(device_at(swapped(coords, dim, (coords[dim] + step) % size), core, sizes))
    return found


def greet(others):
    barrier = pltpu.get_barrier_semaphore()
    for other in others:
        pl.semaphore_signal(barrier, inc=1, device_id=(other,), device_id_type=MESH_ID)
    pl.semaphore_wait(barrier, len(others))


class Sems:
    def __init__(self, send, recv):
        self.send, self.recv, self.used = send, recv, 0

    def pair(self):
        at = self.used
        self.used += 1
        return self.send.at[at], self.recv.at[at]


def remote(sems, src, dst, target):
    send_sem, recv_sem = sems.pair()
    copy = pltpu.make_async_remote_copy(
        src_ref=src, dst_ref=dst, send_sem=send_sem, recv_sem=recv_sem,
        device_id=(target,), device_id_type=MESH_ID,
    )
    copy.start()
    return copy


class Gather:
    def __init__(self, full, colours, sizes, coords, core, sems):
        self.full, self.colours, self.sizes = full, colours, sizes
        self.coords, self.core, self.sems = coords, core, sems
        self.axis = [[] for _ in colours]
        self.swap = []
        self.sent = []

    def view(self, colour, fixed):
        start, width, _ = colour
        place = tuple(fixed.get(dim, slice(None)) for dim in range(len(self.sizes)))
        return self.full.at[(*place, self.core, slice(None), pl.ds(start, width))]

    def start(self, stage, own=None):
        for at, colour in enumerate(self.colours):
            order = colour[2]
            dim = order[stage]
            fixed = {d: self.coords[d] for d in order[stage:]}
            held = self.view(colour, fixed)
            source = held if own is None else own.at[:, pl.ds(colour[0], colour[1])]
            self.axis[at] = []
            for step in range(1, self.sizes[dim]):
                peer = swapped(self.coords, dim, (self.coords[dim] + step) % self.sizes[dim])
                self.axis[at].append(remote(self.sems, source, held, device_at(peer, self.core, self.sizes)))
            self.sent += self.axis[at]

    def land(self, stage):
        partner = device_at(self.coords, 1 - self.core, self.sizes)
        for at, colour in enumerate(self.colours):
            order = colour[2]
            dim = order[stage]
            for copy in self.axis[at]:
                copy.wait_recv()
            fixed = {d: self.coords[d] for d in order[stage + 1:]}
            if stage == 0:
                views = [self.view(colour, fixed)]
            else:
                views = [
                    self.view(colour, {**fixed, dim: (self.coords[dim] + step) % self.sizes[dim]})
                    for step in range(1, self.sizes[dim])
                ]
            for view in views:
                self.swap.append(remote(self.sems, view, view, partner))

    def finish(self):
        for copy in self.swap:
            copy.wait_recv()

    def drain(self):
        for copy in self.sent + self.swap:
            copy.wait_send()


def colours_of(columns, sizes):
    last = len(sizes) - 1
    if last < 2:
        return [(0, columns, tuple(range(len(sizes))))]
    tiles = columns // 128
    if tiles < 8:
        return [(0, columns, (0, 1, 2))]
    third = max(1, tiles // 8)
    first = (tiles - third) // 2
    second = tiles - third - first
    return [
        (0, first * 128, (0, 1, 2)),
        (first * 128, second * 128, (0, 2, 1)),
        ((first + second) * 128, third * 128, (2, 1, 0)),
    ]


def gather_kernel(sizes, count, *refs):
    shards, fulls = refs[:count], refs[count : 2 * count]
    owns = refs[2 * count : 3 * count]
    send_sem, recv_sem, local_sem = refs[3 * count :]
    coords, core = locate(lax.axis_index("dp"), sizes)
    for shard, own in zip(shards, owns):
        own[...] = shard[...].astype(own.dtype)
    greet(neighbours(coords, core, sizes))
    sems = Sems(send_sem, recv_sem)
    items = [
        Gather(full, colours_of(full.shape[-1], sizes), sizes, coords, core, sems) for full in fulls
    ]
    local = []
    for at, (own, full) in enumerate(zip(owns, fulls)):
        copy = pltpu.make_async_copy(own, full.at[(*coords, core)], local_sem.at[at])
        copy.start()
        local.append(copy)
    stages = len(sizes)
    items[0].start(0, owns[0])
    for turn in range(count + stages):
        for stage in range(stages):
            at = turn - stage
            if 0 <= at < count:
                if stage == 0:
                    if at + 1 < count:
                        items[at + 1].start(0, owns[at + 1])
                    local[at].wait()
                items[at].land(stage)
                if stage + 1 < stages:
                    items[at].start(stage + 1)
        at = turn - stages
        if 0 <= at < count:
            items[at].finish()
    for item in items:
        item.drain()


def gather_all(shards, count):
    sizes = grid_of(count)
    copies = 400
    n = len(shards)
    fulls = pl.pallas_call(
        functools.partial(gather_kernel, sizes, n),
        out_shape=[jax.ShapeDtypeStruct((*sizes, 2, *s.shape), jnp.bfloat16) for s in shards],
        in_specs=[pl.BlockSpec(memory_space=pltpu.VMEM)] * n,
        out_specs=[pl.BlockSpec(memory_space=pltpu.HBM)] * n,
        scratch_shapes=[pltpu.VMEM(s.shape, jnp.bfloat16) for s in shards]
        + [pltpu.SemaphoreType.DMA((copies,)), pltpu.SemaphoreType.DMA((copies,)), pltpu.SemaphoreType.DMA((n,))],
        compiler_params=pltpu.CompilerParams(collective_id=0, has_side_effects=True),
        name="gather_all",
    )(*shards)
    return [full.reshape(-1, *full.shape[-2:]) for full in fulls]


def small_block(vectors, bias_up, me):
    wide = jnp.zeros((8, 128), jnp.float32)
    width = vectors.shape[1]
    per = 128 // width
    wide = lax.dynamic_update_slice(wide, vectors, (0, (me % per) * width))
    tail = jnp.zeros((8, 128), jnp.float32)
    span = bias_up.shape[0]
    tail = lax.dynamic_update_slice(tail, bias_up[None, :], (0, (me % (128 // span)) * span))
    return jnp.concatenate([wide, tail], axis=0)


def small_parts(small, vectors, bias_up):
    per = 128 // vectors.shape[1]
    span = 128 // bias_up.shape[0]
    n = small.shape[0]
    vec = jnp.sum(small[:, :8].astype(jnp.float32).reshape(n // per, per, 8, 128), axis=1)
    bias = jnp.sum(small[:, 8].astype(jnp.float32).reshape(n // span, span, 128), axis=1)
    return vec.transpose(1, 0, 2).reshape(8, -1).astype(jnp.bfloat16), bias.reshape(-1).astype(jnp.bfloat16)


F32, BF16 = jnp.float32, jnp.bfloat16


def nn(a, b):
    return lax.dot_general(a, b, (((1,), (0,)), ((), ())), preferred_element_type=F32)


def nt(a, b):
    return lax.dot_general(a, b, (((1,), (1,)), ((), ())), preferred_element_type=F32)


def tn(a, b):
    return lax.dot_general(a, b, (((0,), (0,)), ((), ())), preferred_element_type=F32)


def chunks(total, size, work):
    def step(i, carry):
        work(pl.ds(pl.multiple_of(i * size, size), size))
        return carry

    lax.fori_loop(0, total // size, step, 0)


def split_colours(start, shares, orders):
    found = []
    for order, share in zip(orders, shares):
        if share:
            found.append((start, share * 128, order))
            start += share * 128
    return found


def in_thirds(columns, last):
    tiles = columns // 128
    third = tiles * last // 8
    first = (tiles - third) // 2
    return first, tiles - third - first, third


class Spread:
    def __init__(self, full, own, rows, colours, relay, place):
        self.full, self.own, self.rows, self.colours = full, own, rows, colours
        self.sizes, self.coords, self.core = place
        self.hops = []
        for colour in colours:
            hops = []
            for at, dim in enumerate(colour[2]):
                fixed = {d: self.coords[d] for d in colour[2][at + 1:]}
                hops += [(dim, kind, fixed) for kind in ((1, 2) if dim == 0 and relay else (0,))]
            self.hops.append(hops)
        self.count = len(self.hops[0])

    def view(self, colour, fixed):
        where = tuple(fixed.get(dim, slice(None)) for dim in range(3))
        return self.full.at[(*where, self.core, pl.ds(*self.rows), pl.ds(colour[0], colour[1]))]

    def peer(self, dim, value):
        return device_at(swapped(self.coords, dim, value), self.core, self.sizes)

    def mine(self, at, hop):
        colour = self.colours[at]
        dim, kind, fixed = self.hops[at][hop]
        if kind == 2:
            low = self.coords[0] // 2 * 2
            return self.view(colour, {**fixed, 0: pl.ds(low, 2)})
        return self.view(colour, {**fixed, dim: self.coords[dim]})

    def far(self, at, hop):
        colour = self.colours[at]
        _, _, fixed = self.hops[at][hop]
        return self.view(colour, {**fixed, 0: pl.ds(2 - self.coords[0] // 2 * 2, 2)})

    def inner(self):
        return (self.coords[0] + 1) // 2 == 1

    def send(self, wires, hop, group):
        for at, colour in enumerate(self.colours):
            dim, kind, _ = self.hops[at][hop]
            held = self.mine(at, hop)
            source = held if hop else self.own.at[pl.ds(*self.rows), pl.ds(colour[0], colour[1])]
            here = self.coords[dim]
            if kind == 2:
                group.count(held)
                wires.send_if(self.inner(), source, held, self.peer(0, 3 - here), group)
            elif kind == 1:
                group.count(held)
                wires.send(source, held, self.peer(0, here + 1 - 2 * (here % 2)), group)
            else:
                for step in range(1, self.sizes[dim]):
                    group.count(held)
                    wires.send(source, held, self.peer(dim, (here + step) % self.sizes[dim]), group)

    def pass_on(self, wires, hop, group):
        here = self.coords[0]
        for at in range(len(self.colours)):
            if self.hops[at][hop][1] == 2:
                far = self.far(at, hop)
                wires.put(far, far, self.peer(0, here + 1 - 2 * (here % 2)), group, wires.sent_if)

    def arrived(self, hop):
        for at, colour in enumerate(self.colours):
            dim, kind, fixed = self.hops[at][hop]
            if hop == 0:
                yield self.view(colour, {**fixed, **({0: pl.ds(self.coords[0] // 2 * 2, 2)} if kind == 1 else {})})
            elif kind == 2:
                yield self.far(at, hop)
            elif kind == 1:
                yield self.view(colour, {**fixed, 0: self.coords[0] + 1 - 2 * (self.coords[0] % 2)})
            else:
                for step in range(1, self.sizes[dim]):
                    yield self.view(colour, {**fixed, dim: (self.coords[dim] + step) % self.sizes[dim]})


class Group:
    def __init__(self, sem, gauge):
        self.sem, self.gauge, self.units = sem, gauge, 0

    def count(self, ref):
        self.units += math.prod(ref.shape) * jnp.dtype(ref.dtype).itemsize // 256

    def wait(self):
        whole = self.gauge.at[pl.ds(0, self.units)]
        pltpu.make_async_copy(whole, whole, self.sem).wait()


class Chunk:
    def __init__(self, wires, parts):
        self.wires, self.parts = wires, parts
        self.arriving, self.swap, self.relayed = {}, wires.group(), set()
        self.hops = parts[0].count

    def start(self, hop):
        self.arriving[hop] = self.wires.group()
        for part in self.parts:
            part.send(self.wires, hop, self.arriving[hop])

    def relay(self, hop):
        def forward():
            self.arriving[hop].wait()
            for part in self.parts:
                part.pass_on(self.wires, hop, self.arriving[hop])

        pl.when(self.parts[0].inner())(forward)
        self.relayed.add(hop)

    def land(self, hop):
        if hop not in self.relayed and any(h[hop][1] == 2 for part in self.parts for h in part.hops):
            self.relay(hop)
        if hop in self.relayed:
            pl.when(jnp.logical_not(self.parts[0].inner()))(self.arriving[hop].wait)
        else:
            self.arriving[hop].wait()
        if hop + 1 < self.hops:
            self.start(hop + 1)
        for part in self.parts:
            for view in part.arrived(hop):
                self.swap.count(view)
                self.wires.send(view, view, self.wires.partner, self.swap)

    def finish(self):
        self.swap.wait()


class Wires:
    def __init__(self, send_sem, recv_sem, gauge, partner):
        self.recv_sem, self.gauge, self.partner = recv_sem, gauge, partner
        self.used, self.sent, self.sent_if = 0, Group(send_sem.at[0], gauge), Group(send_sem.at[1], gauge)
        self.condition = None

    def group(self):
        self.used += 1
        assert self.used <= self.recv_sem.shape[0]
        return Group(self.recv_sem.at[self.used - 1], self.gauge)

    def put(self, src, dst, target, group, sent=None):
        pltpu.make_async_remote_copy(
            src_ref=src, dst_ref=dst, send_sem=(sent or self.sent).sem, recv_sem=group.sem,
            device_id=(target,), device_id_type=MESH_ID,
        ).start()
        if sent is not None:
            sent.count(dst)

    def send(self, src, dst, target, group):
        self.put(src, dst, target, group, self.sent)

    def send_if(self, condition, src, dst, target, group):
        self.condition = condition
        pl.when(condition)(lambda: self.put(src, dst, target, group, self.sent_if))

    def swap(self, src, dst):
        group = self.group()
        group.count(dst)
        self.send(src, dst, self.partner, group)
        return group

    def drain(self):
        self.sent.wait()
        if self.condition is not None:
            pl.when(self.condition)(self.sent_if.wait)


class Reduce:
    def __init__(self, wires, held, rows, landing, colours, place):
        self.wires, self.held, self.rows, self.landing, self.colours = wires, held, rows, landing, colours
        self.sizes, self.coords, self.core = place

    def view(self, colour, fixed):
        where = tuple(fixed.get(dim, slice(None)) for dim in range(3))
        return self.held.at[(*where, pl.ds(*self.rows), pl.ds(colour[0], colour[1]))]

    def start(self, stage):
        self.arriving = self.wires.group()
        for at, colour in enumerate(self.colours):
            order = colour[2]
            dim = order[stage]
            fixed = {d: self.coords[d] for d in order[:stage]}
            for step in range(1, self.sizes[dim]):
                theirs = (self.coords[dim] + step) % self.sizes[dim]
                self.arriving.count(self.landing[at][stage].at[step - 1])
                peer = swapped(self.coords, dim, theirs)
                self.wires.send(
                    self.view(colour, {**fixed, dim: theirs}),
                    self.landing[at][stage].at[step - 1],
                    device_at(peer, self.core, self.sizes), self.arriving,
                )

    def land(self):
        self.arriving.wait()

    def add(self, stage, out=None):
        first, rows = self.rows
        for at, colour in enumerate(self.colours):
            order = colour[2]
            fixed = {d: self.coords[d] for d in order[:stage + 1]}
            free = [d for d in range(3) if d not in fixed]
            landing = self.landing[at][stage]
            counts = [self.sizes[d] for d in free]
            total = math.prod(counts)
            tall = min(rows, 32)

            def step(i, carry, colour=colour, fixed=fixed, free=free, landing=landing, counts=counts, tall=tall):
                where, rest, index = dict(fixed), i // (rows // tall), []
                for d, size in zip(reversed(free), reversed(counts)):
                    where[d] = rest % size
                    index.insert(0, rest % size)
                    rest = rest // size
                low = (i % (rows // tall)) * tall
                span = pl.ds(pl.multiple_of(first + low, tall), tall)
                local = pl.ds(pl.multiple_of(low, tall), tall)
                place = (where[0], where[1], where[2], span, pl.ds(colour[0], colour[1]))
                sums = self.held[place].astype(F32)
                for other in range(landing.shape[0]):
                    sums = sums + landing[(other, *index, local, slice(None))].astype(F32)
                if out is None:
                    self.held[place] = sums.astype(self.held.dtype)
                else:
                    out[span, pl.ds(colour[0], colour[1])] = sums
                return carry

            lax.fori_loop(0, total * (rows // tall), step, 0)


class LineReduce:
    def __init__(self, wires, held, columns, landing, place, last):
        self.wires, self.held, self.columns, self.landing = wires, held, columns, landing
        self.sizes, (self.z, self.y, self.x), self.core = place
        self.inner = (self.z + 1) // 2 == 1
        self.own, self.beside = self.z // 2 * 2, self.z + 1 - 2 * (self.z % 2)
        self.rest = (self.y, self.x) if last else (slice(None), slice(None))
        self.spread = (self.y, self.x) if last else ((0, 2), (0, 2))
        self.groups = [wires.group() for _ in landing]
        for group, ref in zip(self.groups, landing):
            group.count(ref)

    def push(self, at, chip, *where):
        source = self.held.at[(*where, slice(None), pl.ds(*self.columns))]
        self.wires.put(source, self.landing[at], device_at(chip, self.core, self.sizes), self.groups[at])

    def add(self, landing, *where, out=None):
        counts = list(landing.shape[:-2])
        rows, tall = landing.shape[-2], 32

        def step(i, carry):
            rest, index = i // (rows // tall), []
            for size in reversed(counts):
                index.insert(0, rest % size)
                rest = rest // size
            free, place = list(index), []
            for entry in where:
                if isinstance(entry, tuple):
                    place.append(entry[0] + free.pop(0))
                else:
                    place.append(entry)
            span = pl.ds(pl.multiple_of((i % (rows // tall)) * tall, tall), tall)
            place = (*place, span, pl.ds(*self.columns))
            sums = self.held[place].astype(F32) + landing[(*index, span, slice(None))].astype(F32)
            if out is None:
                self.held[place] = sums.astype(self.held.dtype)
            else:
                out[span, pl.ds(*self.columns)] = sums
            return carry

        lax.fori_loop(0, math.prod(counts) * (rows // tall), step, 0)

    def start(self):
        def outer():
            chip = (self.beside, self.y, self.x)
            self.push(0, chip, pl.ds(2 - self.own, 2), *self.rest)
            self.push(2, chip, self.beside, *self.rest)

        pl.when(jnp.logical_not(self.inner))(outer)
        self.wires.sent.count(self.landing[0])
        self.wires.sent.count(self.landing[2])

    def across(self):
        def middle():
            self.groups[0].wait()
            self.add(self.landing[0], (2 - self.own, 2), *self.spread)
            self.push(1, (3 - self.z, self.y, self.x), pl.ds(2 - self.own, 2), *self.rest)

        pl.when(self.inner)(middle)

    def back(self):
        def middle():
            self.groups[1].wait()
            self.add(self.landing[1], (self.own, 2), *self.spread)
            self.push(2, (self.beside, self.y, self.x), self.beside, *self.rest)

        pl.when(self.inner)(middle)

    def complete(self, out):
        self.groups[2].wait()
        self.add(self.landing[2], self.z, *self.spread, out=out)

    def second(self):
        self.complete(None)
        self.push(3, (self.z, 1 - self.y, self.x), self.z, 1 - self.y, slice(None))
        self.wires.sent.count(self.landing[3])

    def third(self):
        self.groups[3].wait()
        self.add(self.landing[3], self.z, self.y, (0, 2))
        self.push(4, (self.z, self.y, 1 - self.x), self.z, self.y, 1 - self.x)
        self.wires.sent.count(self.landing[4])

    def finish(self, out):
        self.groups[4].wait()
        self.add(self.landing[4], self.z, self.y, self.x, out=out)


def line_landing(rows, width, last):
    leads = ((2,), (2,), ()) if last else ((2, 2, 2), (2, 2, 2), (2, 2), (2,), ())
    return [pltpu.VMEM((*lead, rows, width), BF16) for lead in leads]


def landing_shapes(rows, colours, sizes, dtype, count=3):
    found = []
    for _, width, order in colours:
        stages = []
        for stage in range(count):
            free = [sizes[d] for d in range(3) if d not in order[:stage + 1]]
            stages.append(pltpu.VMEM((sizes[order[stage]] - 1, *free, rows, width), dtype))
        found.append(stages)
    return found


def stream(count, source, slots, sem, work):
    def fetch(i, slot):
        return pltpu.make_async_copy(source(i), slots(slot), sem.at[slot])

    fetch(0, 0).start()

    def step(i, carry):
        slot = lax.rem(i, 2)

        @pl.when(i + 1 < count)
        def _():
            fetch(i + 1, 1 - slot).start()

        fetch(i, slot).wait()
        work(i, slot)
        return carry

    lax.fori_loop(0, count, step, 0)


def columns_of(i, width):
    return pl.ds(pl.multiple_of(i * width, width), width)


def row_stats(values):
    mean = jnp.mean(values, axis=-1, keepdims=True)
    centred = values - mean
    rstd = lax.rsqrt(jnp.mean(centred * centred, axis=-1, keepdims=True) + ln_eps)
    return centred * rstd, rstd


SMALL, OUT, QKV, UP, DOWN = range(5)


class Box(dict):
    __getattr__ = dict.__getitem__


def leaves(tree):
    if isinstance(tree, dict):
        tree = list(tree.values())
    if isinstance(tree, list):
        return [leaf for part in tree for leaf in leaves(part)]
    return [] if tree is None else [tree]


def shape_of(tree):
    if isinstance(tree, dict):
        return {name: shape_of(part) for name, part in tree.items()}
    if isinstance(tree, list):
        return [shape_of(part) for part in tree]
    return tree is not None


def unpack(shape, refs):
    if isinstance(shape, dict):
        return {name: unpack(part, refs) for name, part in shape.items()}
    if isinstance(shape, list):
        return [unpack(part, refs) for part in shape]
    return next(refs) if shape else None


GATHER_ORDERS = ((0, 1, 2), (0, 2, 1), (2, 1, 0))
REDUCE_ORDERS = ((2, 1, 0), (1, 2, 0), (0, 1, 2))
SIZES = (4, 2, 2)
EARLY_TILES = 2
EARLY_UP = 8
LATE_TILES = 4
TILE = 512


def step_kernel(names, *refs):
    r = Box(unpack(names, iter(refs)))
    sizes = SIZES
    me = lax.axis_index("dp")
    coords, core = locate(me, sizes)
    place = (sizes, coords, core)
    partner = device_at(coords, 1 - core, sizes)
    rows, d = r.tokens.shape
    ff = r.low[UP].shape[1]
    heads2 = d // 128
    slots = rows // MB_ROWS

    others = neighbours(coords, core, sizes)
    barrier = pltpu.get_barrier_semaphore()
    for other in others:
        pl.semaphore_signal(barrier, inc=1, device_id=(other,), device_id_type=MESH_ID)
    loads = []
    for at, (source, target) in enumerate(
        [(r.own[which], r.fin[which]) for which in (OUT, QKV, UP, DOWN)]
        + [(r.cotangent, r.dy), (r.tokens_in, r.tokens)]
    ):
        copy = pltpu.make_async_copy(source, target, r.load_sem.at[at])
        copy.start()
        loads.append(copy)
    devices = math.prod(sizes) * 2
    per = devices * 128 // d
    block, narrow = r.block, 128 // per
    block[...] = jnp.zeros_like(block)
    for k in range(per):
        here = jnp.where(me % per == k, 1.0, 0.0)
        block[0:8, k * narrow:(k + 1) * narrow] = r.vectors[...] * here
    block[8:9, :] = r.bias_up[...]
    r.low[SMALL][...] = block[...].astype(BF16)
    for at, which in enumerate((OUT, QKV, UP, DOWN)):
        loads[at].wait()
        r.low[which][...] = r.fin[which][...].astype(BF16)
    pl.semaphore_wait(barrier, len(others))
    wires = Wires(r.send_sem, r.recv_sem, r.gauge, partner)

    def part(which, row_range, start, shares, relay, orders=GATHER_ORDERS):
        colours = split_colours(start, shares, orders)
        return Spread(r.full[which], r.low[which], row_range, colours, relay, place)

    mine = []
    for which in (SMALL, OUT, QKV, UP, DOWN):
        copy = pltpu.make_async_copy(r.low[which], r.full[which].at[(*coords, core)], r.mine_sem.at[which])
        copy.start()
        mine.append(copy)
    short, tall = r.low[OUT].shape[0], r.low[DOWN].shape[0]
    all_short = (0, short)
    half, early, early_up = 3 * d // 2, EARLY_TILES * 128, EARLY_UP * 128
    mid_ff, end_ff = (ff - early_up) // 2, ff - early_up
    rest = in_thirds(d - early, 0)
    first = Chunk(wires, [part(SMALL, (0, 16), 0, (1,), False), part(OUT, all_short, 0, in_thirds(d, 0), False)])
    qkv0 = Chunk(wires, [part(QKV, all_short, 0, in_thirds(half, 0), True)])
    qkv1 = Chunk(wires, [part(QKV, all_short, half, in_thirds(half, 0), True)])
    up0 = Chunk(wires, [part(UP, all_short, 0, in_thirds(mid_ff, 0), True)])
    up1 = Chunk(wires, [part(UP, all_short, mid_ff, in_thirds(mid_ff, 0), True)])
    ahead_up = Chunk(wires, [part(UP, all_short, end_ff, (EARLY_UP,), True, GATHER_ORDERS[2:])])
    ahead = Chunk(wires, [part(DOWN, (0, tall), d - early, (EARLY_TILES,), True, GATHER_ORDERS[2:])])
    down0 = Chunk(wires, [part(DOWN, (0, tall // 2), 0, rest, True)])
    down1 = Chunk(wires, [part(DOWN, (tall // 2, tall // 2), 0, rest, True)])

    first.start(0)
    ahead_up.start(0)
    ahead.start(0)
    qkv0.start(0)
    qkv1.start(0)
    loads[4].wait()
    for slot in range(slots):
        span = pl.ds(slot * MB_ROWS, MB_ROWS)
        live = lax.broadcasted_iota(jnp.int32, (MB_ROWS, d), 0) < r.lengths[slot]
        r.dy[span, :] = jnp.where(live, r.dy[span, :].astype(F32), 0.0).astype(BF16)
    dy_swap = wires.swap(r.dy, r.dy_far)

    def norm_one(span):
        normed, _ = row_stats(r.tokens[span, :].astype(F32))
        r.da[span, :] = normed

    loads[5].wait()
    chunks(rows, 32, norm_one)
    for copy in mine:
        copy.wait()
    ahead_up.land(0)
    first.land(0)
    qkv0.land(0)
    up0.start(0)
    qkv1.land(0)
    qkv0.relay(1)
    first.land(1)
    up0.land(0)
    qkv0.land(1)
    up1.start(0)
    ahead.land(0)
    qkv1.relay(1)
    first.land(2)
    qkv1.land(1)
    up0.relay(1)
    qkv0.land(2)
    ahead_up.land(1)
    up1.land(0)
    up0.land(1)
    down0.start(0)
    up1.relay(1)
    qkv1.land(2)
    first.finish()
    ahead_up.land(2)
    qkv0.land(3)
    copy = pltpu.make_async_copy(r.full[SMALL], r.smalls, r.mine_sem.at[0])
    copy.start()
    copy.wait()
    flat = [(z, y, x, c) for z in range(sizes[0]) for y in range(sizes[1]) for x in range(sizes[2]) for c in range(2)]
    vec, bias = r.vec, r.bias
    for j in range(d // 128):
        total = 0.0
        for k in range(per):
            total = total + r.smalls[flat[j * per + k]].astype(F32)[0:8]
        vec[:, j * 128:(j + 1) * 128] = total
    for j in range(devices):
        bias[:, j * 128:(j + 1) * 128] = r.smalls[flat[j]].astype(F32)[8:9]

    def first_in(span):
        r.a[span, :] = (r.da[span, :] * vec[0:1, :] + vec[1:2, :]).astype(BF16)

    chunks(rows, 32, first_in)
    down0.land(0)
    up1.land(1)
    up0.land(2)
    down1.start(0)
    ahead.land(1)
    ahead_up.relay(3)
    down0.relay(1)
    qkv1.land(3)
    qkv0.finish()
    down1.land(0)
    down0.land(1)
    up1.land(2)
    qkv1.finish()

    def transpose_out(source, turned, far, low=0, high=16):
        block = turned.shape[2]
        group = max(1, 256 // (2 * block))

        def step(i, carry):
            value = source[:, columns_of(i, 2 * block * group)]
            flipped = value.astype(F32).T.astype(BF16)
            turned[pl.ds(i * group, group)] = flipped.reshape(group, 2, block, rows)
            return carry

        lax.fori_loop(low // group, high // group, step, 0)
        span = pl.ds(low, high - low)
        return wires.swap(turned.at[span, 1 - core], far.at[span])

    def tile_stream(which, low, high, work):
        full, slot = r.full[which], r.wide
        stream(
            (high - low) // TILE,
            lambda i: full.at[:, :, :, :, :, columns_of(i + low // TILE, TILE)],
            lambda s: slot.at[s],
            r.tile_sem,
            lambda i, s: work(i + low // TILE, slot[s].reshape(-1, TILE)),
        )

    def qkv_tile(i, tile):
        which = i * TILE // d
        values = nn(r.a[...], tile)
        shift = jnp.where(which == 0, 1.0, 0.0) * vec[2:3, columns_of(i % (d // TILE), TILE)] + jnp.where(
            which == 2, 1.0, 0.0
        ) * vec[3:4, columns_of(i % (d // TILE), TILE)]
        r.qkv[:, columns_of(i, TILE)] = (values + shift).astype(BF16)

    tile_stream(QKV, 0, 3 * d, qkv_tile)
    one_far = transpose_out(r.a, r.one_t, r.one_far)

    low_lane = lax.broadcasted_iota(jnp.int32, (MB_ROWS, 128), 1) < HEAD_DIM
    scale = 1.0 / math.sqrt(HEAD_DIM)

    def stacked(value):
        zero = jnp.zeros_like(value)
        return jnp.concatenate([jnp.where(low_lane, value, zero), jnp.where(low_lane, zero, value)], axis=0)

    def merged(value):
        return jnp.where(low_lane, value[:MB_ROWS], value[MB_ROWS:])

    def attend(p, carry):
        row = lax.broadcasted_iota(jnp.int32, (2 * MB_ROWS, 128), 0)
        dist = (row % MB_ROWS - lax.broadcasted_iota(jnp.int32, (2 * MB_ROWS, 128), 1)).astype(F32)
        head = (2 * p + row // MB_ROWS).astype(F32)
        alibi = jnp.where(dist >= 0, -jnp.exp2((head + 1.0) * (-8.0 / HEADS)) * dist, -1e30)
        for s in range(slots):
            span = pl.ds(s * MB_ROWS, MB_ROWS)
            q = r.qkv[span, columns_of(p, 128)]
            k = r.qkv[span, columns_of(p + heads2, 128)]
            v = r.qkv[span, columns_of(p + 2 * heads2, 128)]
            scores = nt(stacked(q), k) * scale + alibi
            top = jnp.max(scores, axis=-1, keepdims=True)
            grown = jnp.exp(scores - top)
            probs = grown / jnp.sum(grown, axis=-1, keepdims=True)
            r.probs[p * slots + s] = probs
            r.attn[span, columns_of(p, 128)] = merged(nn(probs.astype(BF16), v)).astype(BF16)
        return carry

    down1.relay(1)
    up0.land(3)
    ahead.land(2)
    ahead_up.land(3)
    lax.fori_loop(0, heads2 // 2, attend, 0)
    down1.land(1)
    down0.land(2)
    lax.fori_loop(heads2 // 2, heads2, attend, 0)
    attn_far = transpose_out(r.attn, r.attn_t, r.attn_far)

    def out_tile(i, tile):
        span = columns_of(i, TILE)
        r.h1[:, span] = r.tokens[:, span].astype(F32) + nn(r.attn[...], tile) + vec[4:5, span]

    tile_stream(OUT, 0, d, out_tile)
    ahead.relay(3)

    def second_in(span):
        normed, _ = row_stats(r.h1[span, :])
        r.a[span, :] = (normed * vec[5:6, :] + vec[6:7, :]).astype(BF16)

    chunks(rows, 32, second_in)
    two_far = transpose_out(r.a, r.two_t, r.two_far)

    def up_tile(i, tile):
        pre = nn(r.a[...], tile) + bias[:, columns_of(i, TILE)]
        value, slope = gelu_pair(pre)
        r.act[:, columns_of(i, TILE)] = value.astype(BF16)
        r.slope[:, columns_of(i, TILE)] = slope.astype(BF16)

    ahead_up.finish()
    tile_stream(UP, end_ff, ff, up_tile)
    up0.finish()
    down1.land(2)
    up1.land(3)
    tile_stream(UP, 0, mid_ff, up_tile)
    act_far0 = transpose_out(r.act, r.act_t, r.act_far, 0, mid_ff // 256)
    act_far2 = transpose_out(r.act, r.act_t, r.act_far, end_ff // 256, 16)
    up1.finish()
    tile_stream(UP, mid_ff, end_ff, up_tile)
    act_far1 = transpose_out(r.act, r.act_t, r.act_far, mid_ff // 256, end_ff // 256)
    down0.land(3)
    dy_swap.wait()
    act_far2.wait()
    act_far0.wait()
    act_far1.wait()

    reduces = [
        Reduce(wires, r.grad[which], span, landing, colours, place)
        for (which, span, colours), landing in zip(reduce_parts(short, tall, d, ff), r.landing)
    ]

    def weight_grad(which, turned, far, near_d, far_d, low, high):
        grad = r.grad[which]
        block = turned.shape[2]
        width = 512 if (high - low) % 512 == 0 and low % 512 == 0 else high - low
        total = (high - low) // width
        groups = max(1, 16 * block // 512)
        each = 16 // groups

        def step(i, carry):
            at, g = i // groups, i % groups
            left = turned[pl.ds(g * each, each), core].reshape(each * block, rows)
            other = far[pl.ds(g * each, each)].reshape(each * block, rows)
            span = pl.ds(pl.multiple_of(low + at * width, 128), width)
            value = nn(left, near_d[:, span]) + nn(other, far_d[:, span])
            value = value.astype(BF16)
            if groups == 1:
                grad[:, :, :, :, span] = value.reshape(*sizes, block, width)
            else:
                grad[g, :, :, :, span] = value.reshape(*sizes[1:], block, width)
            return carry

        assert groups in (1, sizes[0])
        lax.fori_loop(0, total * groups, step, 0)

    late = LATE_TILES * 128
    weight_grad(DOWN, r.act_t, r.act_far, r.dy, r.dy_far, d - late, d)
    line = LineReduce(wires, r.grad[DOWN], (d - late, late), r.line[0], place, False)
    line.start()
    weight_grad(DOWN, r.act_t, r.act_far, r.dy, r.dy_far, 0, d - late)
    reduces[0].start(0)
    reduces[1].start(0)
    ahead.land(3)
    down1.land(3)
    down0.finish()
    down1.finish()
    ahead.finish()

    sums = r.sums
    sums[...] = jnp.zeros_like(sums)
    acc = r.da

    def begin(span):
        acc[span, :] = r.h1[span, :] + vec[7:8, :]
        sums[7:8, :] += jnp.sum(r.dy[span, :].astype(F32), axis=0, keepdims=True)

    chunks(rows, 32, begin)

    def down_tile(i, s):
        tile = r.deep[s].reshape(-1, d)
        wide = tile.shape[0]
        span = columns_of(i, wide)
        acc[...] += nn(r.act[:, span], tile)
        d_pre = nt(r.dy[...], tile) * r.slope[:, span].astype(F32)
        r.bias_sum[:, span] = jnp.sum(d_pre, axis=0, keepdims=True)
        r.act[:, span] = d_pre.astype(BF16)

    full_down = r.full[DOWN]
    tiles = sizes[0] * sizes[1]

    def down_pass(low):
        stream(
            tiles // 2,
            lambda i: full_down.at[(i + low) // sizes[1], (i + low) % sizes[1]],
            lambda s: r.deep.at[s],
            r.tile_sem,
            lambda i, s: down_tile(i + low, s),
        )
        span = pl.ds(low * (ff // tiles), ff // 2)
        return wires.swap(r.act.at[:, span], r.pre_far.at[:, span])

    def advance(part, stage):
        reduces[part].land()
        reduces[part].add(stage - 1)
        reduces[part].start(stage)

    def complete(part, which):
        reduces[part].land()
        reduces[part].add(2, r.fin[which])

    down_line = LineReduce(wires, r.grad[DOWN], (0, d - late), r.line[1], place, True)
    up_lines = [
        LineReduce(wires, r.grad[UP], (at * ff // 2, ff // 2), r.line[2 + at], place, True) for at in range(2)
    ]

    def settle(part):
        reduces[part].land()
        reduces[part].add(1)

    pre_swap0 = down_pass(0)
    advance(0, 1)
    pre_swap1 = down_pass(tiles // 2)
    advance(1, 1)
    two_far.wait()
    pre_swap0.wait()
    weight_grad(UP, r.two_t, r.two_far, r.act, r.pre_far, 0, ff // 2)
    reduces[2].start(0)
    pre_swap1.wait()
    weight_grad(UP, r.two_t, r.two_far, r.act, r.pre_far, ff // 2, ff)
    reduces[3].start(0)
    r.a[...] = acc[...].astype(BF16)

    def row_stream(which, left):
        full, slot = r.full[which], r.flat
        width = full.shape[-1]

        def work(i, s):
            tile = slot[s, :, :, :, :, pl.ds(0, width)].reshape(-1, width)
            return nt(left[...], tile)

        def run(put):
            stream(
                sizes[0],
                lambda i: full.at[i],
                lambda s: slot.at[s, :, :, :, :, pl.ds(0, width)],
                r.tile_sem,
                lambda i, s: put(i, work(i, s)),
            )

        return run

    def put_da(i, value):
        r.da[:, columns_of(i, value.shape[1])] = value

    row_stream(UP, r.act)(put_da)

    line.across()

    def norm_two_back(span):
        normed, rstd = row_stats(r.h1[span, :])
        da = r.da[span, :]
        sums[5:6, :] += jnp.sum(da * normed, axis=0, keepdims=True)
        sums[6:7, :] += jnp.sum(da, axis=0, keepdims=True)
        d_h1 = r.dy[span, :].astype(F32) + norm_back(da, normed, rstd, vec[5:6, :])
        sums[4:5, :] += jnp.sum(d_h1, axis=0, keepdims=True)
        r.h1[span, :] = d_h1
        r.d_mid[span, :] = d_h1.astype(BF16)

    chunks(rows, 32, norm_two_back)
    stores = []

    def keep(source, target):
        copy = pltpu.make_async_copy(source, target, r.store_sem.at[len(stores)])
        copy.start()
        stores.append(copy)

    keep(r.a, r.output)
    mid_swap = wires.swap(r.d_mid, r.mid_far)

    def put_attn(i, value):
        r.d_attn[:, columns_of(i, value.shape[1])] = value.astype(BF16)

    row_stream(OUT, r.d_mid)(put_attn)

    advance(2, 1)
    settle(0)
    settle(1)
    down_line.start()
    attn_far.wait()
    mid_swap.wait()
    weight_grad(OUT, r.attn_t, r.attn_far, r.d_mid, r.mid_far, 0, d)

    def attend_back(p, carry):
        span_p = columns_of(p, 128)
        d_bq = jnp.zeros((1, 128), F32)
        d_bv = jnp.zeros((1, 128), F32)
        for s in range(slots):
            span = pl.ds(s * MB_ROWS, MB_ROWS)
            q = stacked(r.qkv[span, span_p])
            k = r.qkv[span, columns_of(p + heads2, 128)]
            v = r.qkv[span, columns_of(p + 2 * heads2, 128)]
            do = r.d_attn[span, span_p]
            probs = r.probs[p * slots + s]
            both = stacked(do)
            d_v = tn(probs.astype(BF16), both)
            d_probs = nt(both, v)
            weighed = do.astype(F32) * r.attn[span, span_p].astype(F32)
            delta = jnp.sum(stacked(weighed), axis=-1, keepdims=True)
            d_scores = (probs * (d_probs - delta)).astype(BF16)
            d_q = merged(nn(d_scores, k)) * scale
            d_k = tn(d_scores, q) * scale
            d_bq += jnp.sum(d_q, axis=0, keepdims=True)
            d_bv += jnp.sum(d_v, axis=0, keepdims=True)
            r.qkv[span, span_p] = d_q.astype(BF16)
            r.qkv[span, columns_of(p + heads2, 128)] = d_k.astype(BF16)
            r.qkv[span, columns_of(p + 2 * heads2, 128)] = d_v.astype(BF16)
        sums[2:3, span_p] = d_bq
        sums[3:4, span_p] = d_bv
        return carry

    lax.fori_loop(0, heads2 // 2, attend_back, 0)
    advance(3, 1)
    reduces[4].start(0)
    lax.fori_loop(heads2 // 2, heads2, attend_back, 0)
    qkv_swap = wires.swap(r.qkv, r.qkv_far)
    down_line.across()
    row_stream(QKV, r.qkv)(put_da)
    settle(2)
    up_lines[0].start()
    one_far.wait()
    qkv_swap.wait()
    weight_grad(QKV, r.one_t, r.one_far, r.qkv, r.qkv_far, 0, d)
    reduces[5].start(0)
    weight_grad(QKV, r.one_t, r.one_far, r.qkv, r.qkv_far, d, 2 * d)
    reduces[6].start(0)
    settle(3)
    up_lines[1].start()
    weight_grad(QKV, r.one_t, r.one_far, r.qkv, r.qkv_far, 2 * d, 3 * d)
    line.back()

    def norm_one_back(span):
        normed, rstd = row_stats(r.tokens[span, :].astype(F32))
        da = r.da[span, :]
        sums[0:1, :] += jnp.sum(da * normed, axis=0, keepdims=True)
        sums[1:2, :] += jnp.sum(da, axis=0, keepdims=True)
        r.h1[span, :] = r.h1[span, :] + norm_back(da, normed, rstd, vec[0:1, :])

    chunks(rows, 32, norm_one_back)
    down_line.back()

    bundle = r.bundle
    for j in range(devices):
        at = (j // per) * 128
        bundle[flat[j]] = jnp.concatenate(
            [sums[:, at:at + 128], jnp.broadcast_to(r.bias_sum[:, j * 128:(j + 1) * 128], (8, 128))], axis=0
        )
    tiny_swap = wires.swap(bundle.at[:, :, :, 1 - core], r.tiny_far)
    tiny = reduces[8]
    keep(r.h1, r.input_grad)
    advance(4, 1)
    up_lines[0].across()
    tiny_swap.wait()
    r.grad[SMALL][...] = bundle[:, :, :, core] + r.tiny_far[...]
    tiny.start(0)
    advance(5, 1)
    reduces[7].start(0)
    up_lines[1].across()
    down_line.complete(r.fin[DOWN])
    advance(6, 1)
    up_lines[0].back()
    advance(4, 2)
    advance(5, 2)
    up_lines[1].back()
    advance(7, 1)
    line.second()
    advance(6, 2)
    up_lines[0].complete(r.fin[UP])
    advance(7, 2)
    advance(8, 1)
    line.third()
    advance(8, 2)
    up_lines[1].complete(r.fin[UP])
    complete(4, OUT)
    keep(r.fin[UP], r.final[UP])
    complete(5, QKV)
    keep(r.fin[OUT], r.final[OUT])
    complete(6, QKV)
    line.finish(r.fin[DOWN])
    keep(r.fin[DOWN], r.final[DOWN])
    complete(8, SMALL)
    keep(r.fin[SMALL], r.final[SMALL])
    complete(7, QKV)
    keep(r.fin[QKV], r.final[QKV])
    for copy in stores:
        copy.wait()
    wires.drain()


def reduce_parts(short, tall, d, ff):
    rows, half_ff = (0, short), ff // 2

    def colours(start, width, last):
        return split_colours(start, in_thirds(width, last), REDUCE_ORDERS)

    return [
        (DOWN, (0, tall // 2), colours(0, d - LATE_TILES * 128, 0)),
        (DOWN, (tall // 2, tall // 2), colours(0, d - LATE_TILES * 128, 0)),
        (UP, rows, colours(0, half_ff, 0)),
        (UP, rows, colours(half_ff, half_ff, 0)),
        (OUT, rows, colours(0, d, 0)),
        (QKV, rows, colours(0, d, 0)),
        (QKV, rows, colours(d, d, 0)),
        (QKV, rows, colours(2 * d, d, 0)),
        (SMALL, (0, 16), [(0, 128, (2, 1, 0))]),
    ]


def fused_step(tokens, cotangent, lengths, vectors, bias_up, w_qkv, w_out, w_up, w_down):
    sizes = SIZES
    rows, d = tokens.shape
    ff = w_up.shape[1]
    short, tall = w_out.shape[0], w_down.shape[0]
    heads2 = d // 128
    slots = rows // MB_ROWS
    whole = lambda s: jax.ShapeDtypeStruct((*sizes, 2, *s), BF16)
    like = jax.ShapeDtypeStruct
    wide = ((16, 128), (short, d), (short, 3 * d), (short, ff), (tall, d))
    v = pltpu.VMEM
    turned, across = v((16, 2, short, rows), BF16), v((16, short, rows), BF16)
    flat, double = v((rows, d), BF16), v((rows, d), F32)
    near = dict(vectors=vectors, bias_up=bias_up)
    distant = dict(tokens_in=tokens, cotangent=cotangent, own=[None, w_out, w_qkv, w_up, w_down])
    results = dict(
        full=[whole(s) for s in wide], gauge=like((180_224, 128), BF16),
        output=like((rows, d), BF16), input_grad=like((rows, d), F32), final=[like(s, F32) for s in wide],
    )
    parts = reduce_parts(short, tall, d, ff)
    scratch = dict(
        low=[v(s, BF16) for s in wide], block=v((16, 128), F32), dy=flat, tokens=flat,
        fin=[v(s, F32) for s in wide],
        smalls=v((*sizes, 2, 16, 128), BF16), vec=v((8, d), F32), bias=v((1, ff), F32),
        dy_far=flat, da=double, a=flat, qkv=v((rows, 3 * d), BF16), qkv_far=v((rows, 3 * d), BF16),
        probs=v((heads2 * slots, 2 * MB_ROWS, 128), F32), attn=flat, h1=double,
        act=v((rows, ff), BF16), slope=v((rows, ff), BF16), pre_far=v((rows, ff), BF16),
        d_mid=flat, mid_far=flat, d_attn=flat,
        one_t=turned, one_far=across, attn_t=turned, attn_far=across, two_t=turned, two_far=across,
        act_t=v((16, 2, tall, rows), BF16), act_far=v((16, tall, rows), BF16),
        wide=v((2, *sizes, 2, short, TILE), BF16), deep=v((2, sizes[2], 2, tall, d), BF16),
        flat=v((2, *sizes[1:], 2, short, ff), BF16),
        grad=[v((*sizes, *s), BF16 if at else F32) for at, s in enumerate(wide)],
        sums=v((8, d), F32), bias_sum=v((1, ff), F32),
        bundle=v((*sizes, 2, 16, 128), F32), tiny_far=v((*sizes, 16, 128), F32),
        landing=[
            landing_shapes(span[1], colours, sizes, BF16 if which else F32, 2 if which in (UP, DOWN) else 3)
            for which, span, colours in parts
        ],
        line=[
            line_landing(tall, LATE_TILES * 128, False), line_landing(tall, d - LATE_TILES * 128, True),
            line_landing(short, ff // 2, True), line_landing(short, ff // 2, True),
        ],
        send_sem=pltpu.SemaphoreType.DMA((2,)), recv_sem=pltpu.SemaphoreType.DMA((97,)),
        mine_sem=pltpu.SemaphoreType.DMA((5,)), tile_sem=pltpu.SemaphoreType.DMA((2,)),
        load_sem=pltpu.SemaphoreType.DMA((6,)), store_sem=pltpu.SemaphoreType.DMA((7,)),
    )
    names = {**dict(lengths=lengths), **near, **distant, **results, **scratch}
    found = pl.pallas_call(
        functools.partial(step_kernel, shape_of(names)),
        out_shape=leaves(results),
        in_specs=[pl.BlockSpec(memory_space=pltpu.SMEM)]
        + [pl.BlockSpec(memory_space=v)] * len(leaves(near))
        + [pl.BlockSpec(memory_space=pltpu.HBM)] * len(leaves(distant)),
        out_specs=[pl.BlockSpec(memory_space=pltpu.HBM)] * len(leaves(results)),
        scratch_shapes=leaves(scratch),
        compiler_params=pltpu.CompilerParams(
            collective_id=1, has_side_effects=True, vmem_limit_bytes=67_000_000
        ),
        name="fused_step",
    )(lengths, *leaves(near), *leaves(distant))
    return Box(unpack(shape_of(results), iter(found)))


def adam_kernel(shape, *refs):
    r = Box(unpack(shape, iter(refs)))
    me = lax.axis_index("dp")
    count = float(STEP)

    def put(at, param, first, second, grad):
        update, new_first, new_second = adamw(param, (first, second), grad, count)
        r.grads[at][...] = grad
        r.updates[at][...] = update
        r.firsts[at][...] = new_first
        r.seconds[at][...] = new_second

    for at in range(2, 6):
        put(at, r.params[at][...], r.moments[at][0], r.moments[at][1], r.final[at - 1][...])
    r.output[...] = r.early_output[...]
    r.input_grad[...] = r.early_grad[...]

    @pl.when(pl.program_id(0) == 0)
    def _():
        narrow = r.params[0].shape[1]
        per = 128 // narrow
        grad = jnp.zeros((8, narrow), F32)
        for k in range(per):
            grad = grad + jnp.where(me % per == k, 1.0, 0.0) * r.final[SMALL][0:8, k * narrow:(k + 1) * narrow]
        put(0, r.params[0][...], r.moments[0][0], r.moments[0][1], grad)
        put(1, r.params[1][...], r.moments[1][0:1], r.moments[1][1:2], r.final[SMALL][8:9, :])


def adam(found, params, moments):
    steps = 4

    def whole(s):
        return pl.BlockSpec(s, lambda i: (0,) * len(s))

    def cut(s):
        return pl.BlockSpec((*s[:-1], s[-1] // steps), lambda i: (0,) * (len(s) - 1) + (i,))

    def tall(s):
        return pl.BlockSpec((s[0] // steps, s[1]), lambda i: (i, 0))

    def each(make):
        return [make(p.shape) for p in params]

    like = jax.ShapeDtypeStruct
    outs = each(lambda s: like(s, F32))
    specs = [whole(p.shape) if at < 2 else cut(p.shape) for at, p in enumerate(params)]
    moment_specs = [whole(m.shape) if at < 2 else cut(m.shape) for at, m in enumerate(moments)]
    inputs = dict(
        params=list(params), moments=list(moments), final=found.final,
        early_output=found.output, early_grad=found.input_grad,
    )
    input_specs = dict(
        params=specs, moments=moment_specs, final=[whole((16, 128)), *specs[2:]],
        early_output=tall(found.output.shape), early_grad=tall(found.input_grad.shape),
    )
    results = dict(
        grads=outs, updates=outs, firsts=outs, seconds=outs,
        output=like(found.output.shape, BF16), input_grad=like(found.input_grad.shape, F32),
    )
    result_specs = dict(
        grads=specs, updates=specs, firsts=specs, seconds=specs,
        output=tall(found.output.shape), input_grad=tall(found.input_grad.shape),
    )
    shape = shape_of({**inputs, **results})
    done = pl.pallas_call(
        functools.partial(adam_kernel, shape),
        grid=(steps,),
        out_shape=leaves(results),
        in_specs=leaves(input_specs),
        out_specs=leaves(result_specs),
        compiler_params=pltpu.CompilerParams(vmem_limit_bytes=67_000_000),
        name="adam",
    )(*leaves(inputs))
    return Box(unpack(shape_of(results), iter(done)))


def general_body(
    tokens,
    cotangent,
    lengths,
    vectors,
    bias_up,
    w_qkv,
    w_out,
    w_up,
    w_down,
    mom_vectors,
    mom_bias_up,
    mom_qkv,
    mom_out,
    mom_up,
    mom_down,
):
    params = (vectors, bias_up, w_qkv, w_out, w_up, w_down)
    moments = (mom_vectors, mom_bias_up, mom_qkv, mom_out, mom_up, mom_down)
    me = lax.axis_index("dp")
    count = lax.axis_size("dp")
    small, full_out, full_qkv, full_up, full_down = gather_all(
        [small_block(vectors, bias_up, me), w_out, w_qkv, w_up, w_down], count
    )
    vec_low, bias_low = small_parts(small, vectors, bias_up)
    weights = (
        vec_low,
        bias_low,
        full_qkv.reshape(-1, w_qkv.shape[1]),
        full_out.reshape(-1, w_out.shape[1]),
        full_up.reshape(-1, w_up.shape[1]),
        full_down.reshape(-1, w_down.shape[1]),
    )
    alibi = alibi_bias(MB_ROWS)
    place = jnp.arange(MB_ROWS)
    owned = tuple((jnp.zeros(p.shape, jnp.float32) for p in params))
    summed = None
    out_list = []
    dx_list = []
    for micro in range(MICRO):
        x_rows = tokens[micro * MB_ROWS : (micro + 1) * MB_ROWS]
        live = place < lengths[micro]
        grad_rows = jnp.where(
            live[:, None],
            cotangent[micro * MB_ROWS : (micro + 1) * MB_ROWS],
            jnp.zeros((), jnp.bfloat16),
        )
        out, saved = forward_block(x_rows, weights, alibi)
        d_x, grads = backward_block(saved, grad_rows, weights, alibi)
        out_list.append(out)
        dx_list.append(d_x)
        summed = grads if summed is None else tuple((a + b for a, b in zip(summed, grads)))
    owned = (
        lax.psum_scatter(summed[0], "dp", scatter_dimension=1, tiled=True),
        lax.psum_scatter(summed[1], "dp", scatter_dimension=0, tiled=True),
        lax.psum_scatter(summed[2], "dp", scatter_dimension=0, tiled=True),
        lax.psum_scatter(summed[3], "dp", scatter_dimension=0, tiled=True),
        lax.psum_scatter(summed[4], "dp", scatter_dimension=0, tiled=True),
        lax.psum_scatter(summed[5], "dp", scatter_dimension=0, tiled=True),
    )
    count = float(STEP)
    news = [adamw(p, m, g, count) for p, m, g in zip(params, moments, owned)]
    output = jnp.concatenate(out_list, axis=0)
    input_grad = jnp.concatenate(dx_list, axis=0)
    return (
        output,
        input_grad,
        owned[0],
        owned[1],
        owned[2],
        owned[3],
        owned[4],
        owned[5],
        news[0][0],
        news[1][0],
        news[2][0],
        news[3][0],
        news[4][0],
        news[5][0],
        news[0][1],
        news[1][1],
        news[2][1],
        news[3][1],
        news[4][1],
        news[5][1],
        news[0][2],
        news[1][2],
        news[2][2],
        news[3][2],
        news[4][2],
        news[5][2],
    )


def body(
    tokens, cotangent, lengths, vectors, bias_up, w_qkv, w_out, w_up, w_down,
    mom_vectors, mom_bias_up, mom_qkv, mom_out, mom_up, mom_down,
):
    if grid_of(lax.axis_size("dp")) != SIZES:
        return general_body(
            tokens, cotangent, lengths, vectors, bias_up, w_qkv, w_out, w_up, w_down,
            mom_vectors, mom_bias_up, mom_qkv, mom_out, mom_up, mom_down,
        )
    span = bias_up.shape[0]
    found = fused_step(tokens, cotangent, lengths, vectors, bias_up.reshape(1, span), w_qkv, w_out, w_up, w_down)
    found.final[OUT], found.final[QKV] = found.final[QKV], found.final[OUT]
    done = adam(
        found,
        (vectors, bias_up.reshape(1, span), w_qkv, w_out, w_up, w_down),
        (mom_vectors, mom_bias_up, mom_qkv, mom_out, mom_up, mom_down),
    )

    def six(arrays):
        return (arrays[0], arrays[1].reshape(span), *arrays[2:])

    return (
        done.output, done.input_grad, *six(done.grads), *six(done.updates), *six(done.firsts), *six(done.seconds),
    )


def solution(mesh):
    in_specs = (
        P("dp", None),
        P("dp", None),
        P("dp"),
        P(None, "dp"),
        P("dp"),
        P("dp", None),
        P("dp", None),
        P("dp", None),
        P("dp", None),
        P(None, None, "dp"),
        P(None, "dp"),
        P(None, "dp", None),
        P(None, "dp", None),
        P(None, "dp", None),
        P(None, "dp", None),
    )
    out_specs = (
        P("dp", None),
        P("dp", None),
        P(None, "dp"),
        P("dp"),
        P("dp", None),
        P("dp", None),
        P("dp", None),
        P("dp", None),
        P(None, "dp"),
        P("dp"),
        P("dp", None),
        P("dp", None),
        P("dp", None),
        P("dp", None),
        P(None, "dp"),
        P("dp"),
        P("dp", None),
        P("dp", None),
        P("dp", None),
        P("dp", None),
        P(None, "dp"),
        P("dp"),
        P("dp", None),
        P("dp", None),
        P("dp", None),
        P("dp", None),
    )
    return jax.shard_map(body, mesh=mesh, in_specs=in_specs, out_specs=out_specs, check_vma=False)
```

```python
import functools
import math

import jax
import jax.numpy as jnp
from jax import lax
from jax.experimental import pallas as pl
from jax.experimental.pallas import tpu as pltpu
from jax.sharding import PartitionSpec as P

D = 1024
HEADS = 16
HEAD_DIM = 64
MB_ROWS = 128
MICRO = 2
STEP = 3


ln_eps = 1e-05
gelu_c = math.sqrt(2.0 / math.pi)
beta_one = 0.9
beta_two = 0.95
decay_rate = 0.1
adam_eps = 1e-08


def product(left, right):
    return jnp.dot(left, right, preferred_element_type=jnp.float32)


def contract(form, left, right):
    return jnp.einsum(form, left, right, preferred_element_type=jnp.float32)


def layer_norm(values, gain, shift):
    centred = values - jnp.mean(values, axis=-1, keepdims=True)
    rstd = lax.rsqrt(jnp.mean(centred * centred, axis=-1, keepdims=True) + ln_eps)
    normed = centred * rstd
    return (normed * gain + shift, normed, rstd)


def norm_back(grad_in, normed, rstd, gain):
    scaled = grad_in * gain
    inner = (
        scaled
        - jnp.mean(scaled, axis=-1, keepdims=True)
        - normed * jnp.mean(scaled * normed, axis=-1, keepdims=True)
    )
    return rstd * inner


def gelu_pair(pre):
    tanh_val = jnp.tanh(gelu_c * (pre + 0.044715 * pre * pre * pre))
    value = 0.5 * pre * (1.0 + tanh_val)
    slope = 0.5 * (1.0 + tanh_val) + 0.5 * pre * (1.0 - tanh_val * tanh_val) * gelu_c * (
        1.0 + 3.0 * 0.044715 * pre * pre
    )
    return (value, slope)


def alibi_bias(rows):
    place = jnp.arange(rows)
    dist = (place[:, None] - place[None, :]).astype(jnp.float32)
    slopes = jnp.exp2(-8.0 * (jnp.arange(HEADS) + 1).astype(jnp.float32) / HEADS)
    bias = -slopes[:, None, None] * dist[None]
    return jnp.where(dist[None] >= 0, bias, -1e30)


def attention_scores(q3, k3, alibi):
    return contract("qhd,khd->hqk", q3, k3) * (1.0 / math.sqrt(HEAD_DIM)) + alibi


def forward_block(x_rows, weights, alibi):
    vec, up_bias, qkv_w, out_w, up_w, down_w = weights
    vecf = vec.astype(jnp.float32)
    rows = x_rows.shape[0]
    xf = x_rows.astype(jnp.float32)
    ln_one, normed_one, rstd_one = layer_norm(xf, vecf[0], vecf[1])
    a_one = ln_one.astype(jnp.bfloat16)
    qkv = product(a_one, qkv_w)
    query = (qkv[:, :D] + vecf[2]).astype(jnp.bfloat16).reshape(rows, HEADS, HEAD_DIM)
    keyx = qkv[:, D : 2 * D].astype(jnp.bfloat16).reshape(rows, HEADS, HEAD_DIM)
    value = (qkv[:, 2 * D :] + vecf[3]).astype(jnp.bfloat16).reshape(rows, HEADS, HEAD_DIM)
    scores = attention_scores(query, keyx, alibi)
    top = jnp.max(scores, axis=-1, keepdims=True)
    lse = top + jnp.log(jnp.sum(jnp.exp(scores - top), axis=-1, keepdims=True))
    probs = jnp.exp(scores - lse).astype(jnp.bfloat16)
    attn = contract("hqk,khd->qhd", probs, value).reshape(rows, D).astype(jnp.bfloat16)
    h_one = xf + product(attn, out_w) + vecf[4]
    ln_two, normed_two, rstd_two = layer_norm(h_one, vecf[5], vecf[6])
    a_two = ln_two.astype(jnp.bfloat16)
    pre = product(a_two, up_w) + up_bias.astype(jnp.float32)
    act, slope = gelu_pair(pre)
    act_b = act.astype(jnp.bfloat16)
    out = (h_one + product(act_b, down_w) + vecf[7]).astype(jnp.bfloat16)
    saved = (
        normed_one,
        rstd_one,
        a_one,
        query,
        keyx,
        value,
        lse,
        attn,
        normed_two,
        rstd_two,
        a_two,
        slope,
        act_b,
    )
    return (out, saved)


def backward_block(saved, grad_rows, weights, alibi):
    vec, up_bias, qkv_w, out_w, up_w, down_w = weights
    vecf = vec.astype(jnp.float32)
    (
        normed_one,
        rstd_one,
        a_one,
        query,
        keyx,
        value,
        lse,
        attn,
        normed_two,
        rstd_two,
        a_two,
        slope,
        act_b,
    ) = saved
    rows = grad_rows.shape[0]
    scale = 1.0 / math.sqrt(HEAD_DIM)
    dyf = grad_rows.astype(jnp.float32)
    g_bdown = jnp.sum(dyf, axis=0)
    g_down = product(act_b.T, grad_rows)
    d_pre = product(grad_rows, down_w.T) * slope
    g_bup = jnp.sum(d_pre, axis=0)
    d_pre_b = d_pre.astype(jnp.bfloat16)
    g_up = product(a_two.T, d_pre_b)
    d_a2 = product(d_pre_b, up_w.T)
    g_ln2g = jnp.sum(d_a2 * normed_two, axis=0)
    g_ln2b = jnp.sum(d_a2, axis=0)
    d_h1 = dyf + norm_back(d_a2, normed_two, rstd_two, vecf[5])
    g_bout = jnp.sum(d_h1, axis=0)
    d_h1_b = d_h1.astype(jnp.bfloat16)
    g_out = product(attn.T, d_h1_b)
    d_attn = product(d_h1_b, out_w.T).astype(jnp.bfloat16).reshape(rows, HEADS, HEAD_DIM)
    probs_f = jnp.exp(attention_scores(query, keyx, alibi) - lse)
    probs = probs_f.astype(jnp.bfloat16)
    d_v = contract("hqk,qhd->khd", probs, d_attn).reshape(rows, D)
    d_probs = contract("qhd,khd->hqk", d_attn, value)
    delta = jnp.sum(
        d_attn.astype(jnp.float32) * attn.reshape(rows, HEADS, HEAD_DIM).astype(jnp.float32),
        axis=-1,
    ).T[:, :, None]
    d_scores = (probs_f * (d_probs - delta)).astype(jnp.bfloat16)
    d_q = (contract("hqk,khd->qhd", d_scores, keyx) * scale).reshape(rows, D)
    d_k = (contract("hqk,qhd->khd", d_scores, query) * scale).reshape(rows, D)
    g_bq = jnp.sum(d_q, axis=0)
    g_bv = jnp.sum(d_v, axis=0)
    d_qkv = jnp.concatenate([d_q, d_k, d_v], axis=1).astype(jnp.bfloat16)
    g_qkv = product(a_one.T, d_qkv)
    d_a1 = product(d_qkv, qkv_w.T)
    g_ln1g = jnp.sum(d_a1 * normed_one, axis=0)
    g_ln1b = jnp.sum(d_a1, axis=0)
    d_x = d_h1 + norm_back(d_a1, normed_one, rstd_one, vecf[0])
    g_vec = jnp.stack([g_ln1g, g_ln1b, g_bq, g_bv, g_bout, g_ln2g, g_ln2b, g_bdown])
    return (d_x, (g_vec, g_bup, g_qkv, g_out, g_up, g_down))


def adamw(param, moments, grad, count):
    first = beta_one * moments[0] + (1.0 - beta_one) * grad
    second = beta_two * moments[1] + (1.0 - beta_two) * grad * grad
    corr_one = 1.0 - beta_one**count
    corr_two = 1.0 - beta_two**count
    update = first / corr_one / (jnp.sqrt(second / corr_two) + adam_eps) + decay_rate * param
    return (update, first, second)


MESH_ID = pl.DeviceIdType.MESH


def grid_of(count):
    known = {32: (4, 2, 2), 128: (4, 4, 4)}
    return known.get(count, (count // 2,))


def locate(me, sizes):
    rest, coords = me // 2, []
    for size in reversed(sizes):
        coords.append(rest % size)
        rest = rest // size
    return tuple(reversed(coords)), me % 2


def device_at(coords, core, sizes):
    index = 0
    for value, size in zip(coords, sizes):
        index = index * size + value
    return index * 2 + core


def swapped(coords, dim, value):
    return tuple(value if at == dim else old for at, old in enumerate(coords))


def neighbours(coords, core, sizes):
    found = [device_at(coords, 1 - core, sizes)]
    for dim, size in enumerate(sizes):
        for step in range(1, size):
            found.append(device_at(swapped(coords, dim, (coords[dim] + step) % size), core, sizes))
    return found


def greet(others):
    barrier = pltpu.get_barrier_semaphore()
    for other in others:
        pl.semaphore_signal(barrier, inc=1, device_id=(other,), device_id_type=MESH_ID)
    pl.semaphore_wait(barrier, len(others))


class Sems:
    def __init__(self, send, recv):
        self.send, self.recv, self.used = send, recv, 0

    def pair(self):
        at = self.used
        self.used += 1
        return self.send.at[at], self.recv.at[at]


def remote(sems, src, dst, target):
    send_sem, recv_sem = sems.pair()
    copy = pltpu.make_async_remote_copy(
        src_ref=src, dst_ref=dst, send_sem=send_sem, recv_sem=recv_sem,
        device_id=(target,), device_id_type=MESH_ID,
    )
    copy.start()
    return copy


class Gather:
    def __init__(self, full, colours, sizes, coords, core, sems):
        self.full, self.colours, self.sizes = full, colours, sizes
        self.coords, self.core, self.sems = coords, core, sems
        self.axis = [[] for _ in colours]
        self.swap = []
        self.sent = []

    def view(self, colour, fixed):
        start, width, _ = colour
        place = tuple(fixed.get(dim, slice(None)) for dim in range(len(self.sizes)))
        return self.full.at[(*place, self.core, slice(None), pl.ds(start, width))]

    def start(self, stage, own=None):
        for at, colour in enumerate(self.colours):
            order = colour[2]
            dim = order[stage]
            fixed = {d: self.coords[d] for d in order[stage:]}
            held = self.view(colour, fixed)
            source = held if own is None else own.at[:, pl.ds(colour[0], colour[1])]
            self.axis[at] = []
            for step in range(1, self.sizes[dim]):
                peer = swapped(self.coords, dim, (self.coords[dim] + step) % self.sizes[dim])
                self.axis[at].append(remote(self.sems, source, held, device_at(peer, self.core, self.sizes)))
            self.sent += self.axis[at]

    def land(self, stage):
        partner = device_at(self.coords, 1 - self.core, self.sizes)
        for at, colour in enumerate(self.colours):
            order = colour[2]
            dim = order[stage]
            for copy in self.axis[at]:
                copy.wait_recv()
            fixed = {d: self.coords[d] for d in order[stage + 1:]}
            if stage == 0:
                views = [self.view(colour, fixed)]
            else:
                views = [
                    self.view(colour, {**fixed, dim: (self.coords[dim] + step) % self.sizes[dim]})
                    for step in range(1, self.sizes[dim])
                ]
            for view in views:
                self.swap.append(remote(self.sems, view, view, partner))

    def finish(self):
        for copy in self.swap:
            copy.wait_recv()

    def drain(self):
        for copy in self.sent + self.swap:
            copy.wait_send()


def colours_of(columns, sizes):
    last = len(sizes) - 1
    if last < 2:
        return [(0, columns, tuple(range(len(sizes))))]
    tiles = columns // 128
    if tiles < 8:
        return [(0, columns, (0, 1, 2))]
    third = max(1, tiles // 8)
    first = (tiles - third) // 2
    second = tiles - third - first
    return [
        (0, first * 128, (0, 1, 2)),
        (first * 128, second * 128, (0, 2, 1)),
        ((first + second) * 128, third * 128, (2, 1, 0)),
    ]


def gather_kernel(sizes, count, *refs):
    shards, fulls = refs[:count], refs[count : 2 * count]
    owns = refs[2 * count : 3 * count]
    send_sem, recv_sem, local_sem = refs[3 * count :]
    coords, core = locate(lax.axis_index("dp"), sizes)
    for shard, own in zip(shards, owns):
        own[...] = shard[...].astype(own.dtype)
    greet(neighbours(coords, core, sizes))
    sems = Sems(send_sem, recv_sem)
    items = [
        Gather(full, colours_of(full.shape[-1], sizes), sizes, coords, core, sems) for full in fulls
    ]
    local = []
    for at, (own, full) in enumerate(zip(owns, fulls)):
        copy = pltpu.make_async_copy(own, full.at[(*coords, core)], local_sem.at[at])
        copy.start()
        local.append(copy)
    stages = len(sizes)
    items[0].start(0, owns[0])
    for turn in range(count + stages):
        for stage in range(stages):
            at = turn - stage
            if 0 <= at < count:
                if stage == 0:
                    if at + 1 < count:
                        items[at + 1].start(0, owns[at + 1])
                    local[at].wait()
                items[at].land(stage)
                if stage + 1 < stages:
                    items[at].start(stage + 1)
        at = turn - stages
        if 0 <= at < count:
            items[at].finish()
    for item in items:
        item.drain()


def gather_all(shards, count):
    sizes = grid_of(count)
    copies = 400
    n = len(shards)
    fulls = pl.pallas_call(
        functools.partial(gather_kernel, sizes, n),
        out_shape=[jax.ShapeDtypeStruct((*sizes, 2, *s.shape), jnp.bfloat16) for s in shards],
        in_specs=[pl.BlockSpec(memory_space=pltpu.VMEM)] * n,
        out_specs=[pl.BlockSpec(memory_space=pltpu.HBM)] * n,
        scratch_shapes=[pltpu.VMEM(s.shape, jnp.bfloat16) for s in shards]
        + [pltpu.SemaphoreType.DMA((copies,)), pltpu.SemaphoreType.DMA((copies,)), pltpu.SemaphoreType.DMA((n,))],
        compiler_params=pltpu.CompilerParams(collective_id=0, has_side_effects=True),
        name="gather_all",
    )(*shards)
    return [full.reshape(-1, *full.shape[-2:]) for full in fulls]


def small_block(vectors, bias_up, me):
    wide = jnp.zeros((8, 128), jnp.float32)
    width = vectors.shape[1]
    per = 128 // width
    wide = lax.dynamic_update_slice(wide, vectors, (0, (me % per) * width))
    tail = jnp.zeros((8, 128), jnp.float32)
    span = bias_up.shape[0]
    tail = lax.dynamic_update_slice(tail, bias_up[None, :], (0, (me % (128 // span)) * span))
    return jnp.concatenate([wide, tail], axis=0)


def small_parts(small, vectors, bias_up):
    per = 128 // vectors.shape[1]
    span = 128 // bias_up.shape[0]
    n = small.shape[0]
    vec = jnp.sum(small[:, :8].astype(jnp.float32).reshape(n // per, per, 8, 128), axis=1)
    bias = jnp.sum(small[:, 8].astype(jnp.float32).reshape(n // span, span, 128), axis=1)
    return vec.transpose(1, 0, 2).reshape(8, -1).astype(jnp.bfloat16), bias.reshape(-1).astype(jnp.bfloat16)


F32, BF16 = jnp.float32, jnp.bfloat16


def nn(a, b):
    return lax.dot_general(a, b, (((1,), (0,)), ((), ())), preferred_element_type=F32)


def nt(a, b):
    return lax.dot_general(a, b, (((1,), (1,)), ((), ())), preferred_element_type=F32)


def tn(a, b):
    return lax.dot_general(a, b, (((0,), (0,)), ((), ())), preferred_element_type=F32)


def chunks(total, size, work):
    def step(i, carry):
        work(pl.ds(pl.multiple_of(i * size, size), size))
        return carry

    lax.fori_loop(0, total // size, step, 0)


def split_colours(start, shares, orders):
    found = []
    for order, share in zip(orders, shares):
        if share:
            found.append((start, share * 128, order))
            start += share * 128
    return found


def in_thirds(columns, last):
    tiles = columns // 128
    third = tiles * last // 8
    first = (tiles - third) // 2
    return first, tiles - third - first, third


class Spread:
    def __init__(self, full, own, rows, colours, relay, place):
        self.full, self.own, self.rows, self.colours = full, own, rows, colours
        self.sizes, self.coords, self.core = place
        self.hops = []
        for colour in colours:
            hops = []
            for at, dim in enumerate(colour[2]):
                fixed = {d: self.coords[d] for d in colour[2][at + 1:]}
                hops += [(dim, kind, fixed) for kind in ((1, 2) if dim == 0 and relay else (0,))]
            self.hops.append(hops)
        self.count = len(self.hops[0])

    def view(self, colour, fixed):
        where = tuple(fixed.get(dim, slice(None)) for dim in range(3))
        return self.full.at[(*where, self.core, pl.ds(*self.rows), pl.ds(colour[0], colour[1]))]

    def peer(self, dim, value):
        return device_at(swapped(self.coords, dim, value), self.core, self.sizes)

    def mine(self, at, hop):
        colour = self.colours[at]
        dim, kind, fixed = self.hops[at][hop]
        if kind == 2:
            low = self.coords[0] // 2 * 2
            return self.view(colour, {**fixed, 0: pl.ds(low, 2)})
        return self.view(colour, {**fixed, dim: self.coords[dim]})

    def far(self, at, hop):
        colour = self.colours[at]
        _, _, fixed = self.hops[at][hop]
        return self.view(colour, {**fixed, 0: pl.ds(2 - self.coords[0] // 2 * 2, 2)})

    def inner(self):
        return (self.coords[0] + 1) // 2 == 1

    def send(self, wires, hop, group):
        for at, colour in enumerate(self.colours):
            dim, kind, _ = self.hops[at][hop]
            held = self.mine(at, hop)
            source = held if hop else self.own.at[pl.ds(*self.rows), pl.ds(colour[0], colour[1])]
            here = self.coords[dim]
            if kind == 2:
                group.count(held)
                wires.send_if(self.inner(), source, held, self.peer(0, 3 - here), group)
            elif kind == 1:
                group.count(held)
                wires.send(source, held, self.peer(0, here + 1 - 2 * (here % 2)), group)
            else:
                for step in range(1, self.sizes[dim]):
                    group.count(held)
                    wires.send(source, held, self.peer(dim, (here + step) % self.sizes[dim]), group)

    def pass_on(self, wires, hop, group):
        here = self.coords[0]
        for at in range(len(self.colours)):
            if self.hops[at][hop][1] == 2:
                far = self.far(at, hop)
                wires.put(far, far, self.peer(0, here + 1 - 2 * (here % 2)), group, wires.sent_if)

    def arrived(self, hop):
        for at, colour in enumerate(self.colours):
            dim, kind, fixed = self.hops[at][hop]
            if hop == 0:
                yield self.view(colour, {**fixed, **({0: pl.ds(self.coords[0] // 2 * 2, 2)} if kind == 1 else {})})
            elif kind == 2:
                yield self.far(at, hop)
            elif kind == 1:
                yield self.view(colour, {**fixed, 0: self.coords[0] + 1 - 2 * (self.coords[0] % 2)})
            else:
                for step in range(1, self.sizes[dim]):
                    yield self.view(colour, {**fixed, dim: (self.coords[dim] + step) % self.sizes[dim]})


class Group:
    def __init__(self, sem, gauge):
        self.sem, self.gauge, self.units = sem, gauge, 0

    def count(self, ref):
        self.units += math.prod(ref.shape) * jnp.dtype(ref.dtype).itemsize // 256

    def wait(self):
        whole = self.gauge.at[pl.ds(0, self.units)]
        pltpu.make_async_copy(whole, whole, self.sem).wait()


class Chunk:
    def __init__(self, wires, parts):
        self.wires, self.parts = wires, parts
        self.arriving, self.swap, self.relayed = {}, wires.group(), set()
        self.hops = parts[0].count

    def start(self, hop):
        self.arriving[hop] = self.wires.group()
        for part in self.parts:
            part.send(self.wires, hop, self.arriving[hop])

    def relay(self, hop):
        def forward():
            self.arriving[hop].wait()
            for part in self.parts:
                part.pass_on(self.wires, hop, self.arriving[hop])

        pl.when(self.parts[0].inner())(forward)
        self.relayed.add(hop)

    def land(self, hop):
        if hop not in self.relayed and any(h[hop][1] == 2 for part in self.parts for h in part.hops):
            self.relay(hop)
        if hop in self.relayed:
            pl.when(jnp.logical_not(self.parts[0].inner()))(self.arriving[hop].wait)
        else:
            self.arriving[hop].wait()
        if hop + 1 < self.hops:
            self.start(hop + 1)
        for part in self.parts:
            for view in part.arrived(hop):
                self.swap.count(view)
                self.wires.send(view, view, self.wires.partner, self.swap)

    def finish(self):
        self.swap.wait()


class Wires:
    def __init__(self, send_sem, recv_sem, gauge, partner):
        self.recv_sem, self.gauge, self.partner = recv_sem, gauge, partner
        self.used, self.sent, self.sent_if = 0, Group(send_sem.at[0], gauge), Group(send_sem.at[1], gauge)
        self.condition = None

    def group(self):
        self.used += 1
        assert self.used <= self.recv_sem.shape[0]
        return Group(self.recv_sem.at[self.used - 1], self.gauge)

    def put(self, src, dst, target, group, sent=None):
        pltpu.make_async_remote_copy(
            src_ref=src, dst_ref=dst, send_sem=(sent or self.sent).sem, recv_sem=group.sem,
            device_id=(target,), device_id_type=MESH_ID,
        ).start()
        if sent is not None:
            sent.count(dst)

    def send(self, src, dst, target, group):
        self.put(src, dst, target, group, self.sent)

    def send_if(self, condition, src, dst, target, group):
        self.condition = condition
        pl.when(condition)(lambda: self.put(src, dst, target, group, self.sent_if))

    def swap(self, src, dst):
        group = self.group()
        group.count(dst)
        self.send(src, dst, self.partner, group)
        return group

    def drain(self):
        self.sent.wait()
        if self.condition is not None:
            pl.when(self.condition)(self.sent_if.wait)


class Reduce:
    def __init__(self, wires, held, rows, landing, colours, place):
        self.wires, self.held, self.rows, self.landing, self.colours = wires, held, rows, landing, colours
        self.sizes, self.coords, self.core = place

    def view(self, colour, fixed):
        where = tuple(fixed.get(dim, slice(None)) for dim in range(3))
        return self.held.at[(*where, pl.ds(*self.rows), pl.ds(colour[0], colour[1]))]

    def start(self, stage):
        self.arriving = self.wires.group()
        for at, colour in enumerate(self.colours):
            order = colour[2]
            dim = order[stage]
            fixed = {d: self.coords[d] for d in order[:stage]}
            for step in range(1, self.sizes[dim]):
                theirs = (self.coords[dim] + step) % self.sizes[dim]
                self.arriving.count(self.landing[at][stage].at[step - 1])
                peer = swapped(self.coords, dim, theirs)
                self.wires.send(
                    self.view(colour, {**fixed, dim: theirs}),
                    self.landing[at][stage].at[step - 1],
                    device_at(peer, self.core, self.sizes), self.arriving,
                )

    def land(self):
        self.arriving.wait()

    def add(self, stage, out=None):
        first, rows = self.rows
        for at, colour in enumerate(self.colours):
            order = colour[2]
            fixed = {d: self.coords[d] for d in order[:stage + 1]}
            free = [d for d in range(3) if d not in fixed]
            landing = self.landing[at][stage]
            counts = [self.sizes[d] for d in free]
            total = math.prod(counts)
            tall = min(rows, 32)

            def step(i, carry, colour=colour, fixed=fixed, free=free, landing=landing, counts=counts, tall=tall):
                where, rest, index = dict(fixed), i // (rows // tall), []
                for d, size in zip(reversed(free), reversed(counts)):
                    where[d] = rest % size
                    index.insert(0, rest % size)
                    rest = rest // size
                low = (i % (rows // tall)) * tall
                span = pl.ds(pl.multiple_of(first + low, tall), tall)
                local = pl.ds(pl.multiple_of(low, tall), tall)
                place = (where[0], where[1], where[2], span, pl.ds(colour[0], colour[1]))
                sums = self.held[place].astype(F32)
                for other in range(landing.shape[0]):
                    sums = sums + landing[(other, *index, local, slice(None))].astype(F32)
                if out is None:
                    self.held[place] = sums.astype(self.held.dtype)
                else:
                    out[span, pl.ds(colour[0], colour[1])] = sums
                return carry

            lax.fori_loop(0, total * (rows // tall), step, 0)


class LineReduce:
    def __init__(self, wires, held, columns, landing, place, last):
        self.wires, self.held, self.columns, self.landing = wires, held, columns, landing
        self.sizes, (self.z, self.y, self.x), self.core = place
        self.inner = (self.z + 1) // 2 == 1
        self.own, self.beside = self.z // 2 * 2, self.z + 1 - 2 * (self.z % 2)
        self.rest = (self.y, self.x) if last else (slice(None), slice(None))
        self.spread = (self.y, self.x) if last else ((0, 2), (0, 2))
        self.groups = [wires.group() for _ in landing]
        for group, ref in zip(self.groups, landing):
            group.count(ref)

    def push(self, at, chip, *where):
        source = self.held.at[(*where, slice(None), pl.ds(*self.columns))]
        self.wires.put(source, self.landing[at], device_at(chip, self.core, self.sizes), self.groups[at])

    def add(self, landing, *where, out=None):
        counts = list(landing.shape[:-2])
        rows, tall = landing.shape[-2], 32

        def step(i, carry):
            rest, index = i // (rows // tall), []
            for size in reversed(counts):
                index.insert(0, rest % size)
                rest = rest // size
            free, place = list(index), []
            for entry in where:
                if isinstance(entry, tuple):
                    place.append(entry[0] + free.pop(0))
                else:
                    place.append(entry)
            span = pl.ds(pl.multiple_of((i % (rows // tall)) * tall, tall), tall)
            place = (*place, span, pl.ds(*self.columns))
            sums = self.held[place].astype(F32) + landing[(*index, span, slice(None))].astype(F32)
            if out is None:
                self.held[place] = sums.astype(self.held.dtype)
            else:
                out[span, pl.ds(*self.columns)] = sums
            return carry

        lax.fori_loop(0, math.prod(counts) * (rows // tall), step, 0)

    def start(self):
        def outer():
            chip = (self.beside, self.y, self.x)
            self.push(0, chip, pl.ds(2 - self.own, 2), *self.rest)
            self.push(2, chip, self.beside, *self.rest)

        pl.when(jnp.logical_not(self.inner))(outer)
        self.wires.sent.count(self.landing[0])
        self.wires.sent.count(self.landing[2])

    def across(self):
        def middle():
            self.groups[0].wait()
            self.add(self.landing[0], (2 - self.own, 2), *self.spread)
            self.push(1, (3 - self.z, self.y, self.x), pl.ds(2 - self.own, 2), *self.rest)

        pl.when(self.inner)(middle)

    def back(self):
        def middle():
            self.groups[1].wait()
            self.add(self.landing[1], (self.own, 2), *self.spread)
            self.push(2, (self.beside, self.y, self.x), self.beside, *self.rest)

        pl.when(self.inner)(middle)

    def complete(self, out):
        self.groups[2].wait()
        self.add(self.landing[2], self.z, *self.spread, out=out)

    def second(self):
        self.complete(None)
        self.push(3, (self.z, 1 - self.y, self.x), self.z, 1 - self.y, slice(None))
        self.wires.sent.count(self.landing[3])

    def third(self):
        self.groups[3].wait()
        self.add(self.landing[3], self.z, self.y, (0, 2))
        self.push(4, (self.z, self.y, 1 - self.x), self.z, self.y, 1 - self.x)
        self.wires.sent.count(self.landing[4])

    def finish(self, out):
        self.groups[4].wait()
        self.add(self.landing[4], self.z, self.y, self.x, out=out)


def line_landing(rows, width, last):
    leads = ((2,), (2,), ()) if last else ((2, 2, 2), (2, 2, 2), (2, 2), (2,), ())
    return [pltpu.VMEM((*lead, rows, width), BF16) for lead in leads]


def landing_shapes(rows, colours, sizes, dtype, count=3):
    found = []
    for _, width, order in colours:
        stages = []
        for stage in range(count):
            free = [sizes[d] for d in range(3) if d not in order[:stage + 1]]
            stages.append(pltpu.VMEM((sizes[order[stage]] - 1, *free, rows, width), dtype))
        found.append(stages)
    return found


def stream(count, source, slots, sem, work):
    def fetch(i, slot):
        return pltpu.make_async_copy(source(i), slots(slot), sem.at[slot])

    fetch(0, 0).start()

    def step(i, carry):
        slot = lax.rem(i, 2)

        @pl.when(i + 1 < count)
        def _():
            fetch(i + 1, 1 - slot).start()

        fetch(i, slot).wait()
        work(i, slot)
        return carry

    lax.fori_loop(0, count, step, 0)


def columns_of(i, width):
    return pl.ds(pl.multiple_of(i * width, width), width)


def row_stats(values):
    mean = jnp.mean(values, axis=-1, keepdims=True)
    centred = values - mean
    rstd = lax.rsqrt(jnp.mean(centred * centred, axis=-1, keepdims=True) + ln_eps)
    return centred * rstd, rstd


SMALL, OUT, QKV, UP, DOWN = range(5)


class Box(dict):
    __getattr__ = dict.__getitem__


def leaves(tree):
    if isinstance(tree, dict):
        tree = list(tree.values())
    if isinstance(tree, list):
        return [leaf for part in tree for leaf in leaves(part)]
    return [] if tree is None else [tree]


def shape_of(tree):
    if isinstance(tree, dict):
        return {name: shape_of(part) for name, part in tree.items()}
    if isinstance(tree, list):
        return [shape_of(part) for part in tree]
    return tree is not None


def unpack(shape, refs):
    if isinstance(shape, dict):
        return {name: unpack(part, refs) for name, part in shape.items()}
    if isinstance(shape, list):
        return [unpack(part, refs) for part in shape]
    return next(refs) if shape else None


GATHER_ORDERS = ((0, 1, 2), (0, 2, 1), (2, 1, 0))
REDUCE_ORDERS = ((2, 1, 0), (1, 2, 0), (0, 1, 2))
SIZES = (4, 2, 2)
EARLY_TILES = 2
EARLY_UP = 8
LATE_TILES = 4
TILE = 512


def step_kernel(names, *refs):
    r = Box(unpack(names, iter(refs)))
    sizes = SIZES
    me = lax.axis_index("dp")
    coords, core = locate(me, sizes)
    place = (sizes, coords, core)
    partner = device_at(coords, 1 - core, sizes)
    rows, d = r.tokens.shape
    ff = r.low[UP].shape[1]
    heads2 = d // 128
    slots = rows // MB_ROWS

    others = neighbours(coords, core, sizes)
    barrier = pltpu.get_barrier_semaphore()
    for other in others:
        pl.semaphore_signal(barrier, inc=1, device_id=(other,), device_id_type=MESH_ID)
    loads = []
    for at, (source, target) in enumerate(
        [(r.own[which], r.fin[which]) for which in (OUT, QKV, UP, DOWN)]
        + [(r.cotangent, r.dy), (r.tokens_in, r.tokens)]
    ):
        copy = pltpu.make_async_copy(source, target, r.load_sem.at[at])
        copy.start()
        loads.append(copy)
    devices = math.prod(sizes) * 2
    per = devices * 128 // d
    block, narrow = r.block, 128 // per
    block[...] = jnp.zeros_like(block)
    for k in range(per):
        here = jnp.where(me % per == k, 1.0, 0.0)
        block[0:8, k * narrow:(k + 1) * narrow] = r.vectors[...] * here
    block[8:9, :] = r.bias_up[...]
    r.low[SMALL][...] = block[...].astype(BF16)

    def lower(at, which):
        loads[at].wait()
        r.low[which][...] = r.fin[which][...].astype(BF16)

    lower(0, OUT)
    pl.semaphore_wait(barrier, len(others))
    wires = Wires(r.send_sem, r.recv_sem, r.gauge, partner)

    def part(which, row_range, start, shares, relay, orders=GATHER_ORDERS):
        colours = split_colours(start, shares, orders)
        return Spread(r.full[which], r.low[which], row_range, colours, relay, place)

    short, tall = r.low[OUT].shape[0], r.low[DOWN].shape[0]
    all_short = (0, short)
    half, early, early_up = 3 * d // 2, EARLY_TILES * 128, EARLY_UP * 128
    mid_ff, end_ff = (ff - early_up) // 2, ff - early_up
    rest = in_thirds(d - early, 0)
    first = Chunk(wires, [part(SMALL, (0, 16), 0, (1,), False), part(OUT, all_short, 0, in_thirds(d, 0), False)])
    qkv0 = Chunk(wires, [part(QKV, all_short, 0, in_thirds(half, 0), True)])
    qkv1 = Chunk(wires, [part(QKV, all_short, half, in_thirds(half, 0), True)])
    up0 = Chunk(wires, [part(UP, all_short, 0, in_thirds(mid_ff, 0), True)])
    up1 = Chunk(wires, [part(UP, all_short, mid_ff, in_thirds(mid_ff, 0), True)])
    ahead_up = Chunk(wires, [part(UP, all_short, end_ff, (EARLY_UP,), True, GATHER_ORDERS[2:])])
    ahead = Chunk(wires, [part(DOWN, (0, tall), d - early, (EARLY_TILES,), True, GATHER_ORDERS[2:])])
    down0 = Chunk(wires, [part(DOWN, (0, tall // 2), 0, rest, True)])
    down1 = Chunk(wires, [part(DOWN, (tall // 2, tall // 2), 0, rest, True)])

    first.start(0)
    lower(2, UP)
    ahead_up.start(0)
    lower(1, QKV)
    qkv0.start(0)
    qkv1.start(0)
    lower(3, DOWN)
    ahead.start(0)
    mine = []
    for which in (SMALL, OUT, QKV, UP, DOWN):
        copy = pltpu.make_async_copy(r.low[which], r.full[which].at[(*coords, core)], r.mine_sem.at[which])
        copy.start()
        mine.append(copy)
    loads[4].wait()
    for slot in range(slots):
        span = pl.ds(slot * MB_ROWS, MB_ROWS)
        live = lax.broadcasted_iota(jnp.int32, (MB_ROWS, d), 0) < r.lengths[slot]
        r.dy[span, :] = jnp.where(live, r.dy[span, :].astype(F32), 0.0).astype(BF16)
    dy_swap = wires.swap(r.dy, r.dy_far)

    def norm_one(span):
        normed, _ = row_stats(r.tokens[span, :].astype(F32))
        r.da[span, :] = normed

    loads[5].wait()
    chunks(rows, 32, norm_one)
    for copy in mine:
        copy.wait()
    ahead_up.land(0)
    first.land(0)
    qkv0.land(0)
    up0.start(0)
    qkv1.land(0)
    qkv0.relay(1)
    first.land(1)
    up0.land(0)
    qkv0.land(1)
    up1.start(0)
    ahead.land(0)
    qkv1.relay(1)
    first.land(2)
    qkv1.land(1)
    up0.relay(1)
    qkv0.land(2)
    ahead_up.land(1)
    up1.land(0)
    up0.land(1)
    down0.start(0)
    up1.relay(1)
    qkv1.land(2)
    first.finish()
    ahead_up.land(2)
    qkv0.land(3)
    copy = pltpu.make_async_copy(r.full[SMALL], r.smalls, r.mine_sem.at[0])
    copy.start()
    copy.wait()
    flat = [(z, y, x, c) for z in range(sizes[0]) for y in range(sizes[1]) for x in range(sizes[2]) for c in range(2)]
    vec, bias = r.vec, r.bias
    for j in range(d // 128):
        total = 0.0
        for k in range(per):
            total = total + r.smalls[flat[j * per + k]].astype(F32)[0:8]
        vec[:, j * 128:(j + 1) * 128] = total
    for j in range(devices):
        bias[:, j * 128:(j + 1) * 128] = r.smalls[flat[j]].astype(F32)[8:9]

    def first_in(span):
        r.a[span, :] = (r.da[span, :] * vec[0:1, :] + vec[1:2, :]).astype(BF16)

    chunks(rows, 32, first_in)
    down0.land(0)
    up1.land(1)
    up0.land(2)
    down1.start(0)
    ahead.land(1)
    ahead_up.relay(3)
    down0.relay(1)
    qkv1.land(3)
    qkv0.finish()
    down1.land(0)
    down0.land(1)
    up1.land(2)
    qkv1.finish()

    def transpose_out(source, turned, far, low=0, high=16):
        block = turned.shape[2]
        group = max(1, 256 // (2 * block))

        def step(i, carry):
            value = source[:, columns_of(i, 2 * block * group)]
            flipped = value.astype(F32).T.astype(BF16)
            turned[pl.ds(i * group, group)] = flipped.reshape(group, 2, block, rows)
            return carry

        lax.fori_loop(low // group, high // group, step, 0)
        span = pl.ds(low, high - low)
        return wires.swap(turned.at[span, 1 - core], far.at[span])

    def tile_stream(which, low, high, work):
        full, slot = r.full[which], r.wide
        stream(
            (high - low) // TILE,
            lambda i: full.at[:, :, :, :, :, columns_of(i + low // TILE, TILE)],
            lambda s: slot.at[s],
            r.tile_sem,
            lambda i, s: work(i + low // TILE, slot[s].reshape(-1, TILE)),
        )

    def qkv_tile(i, tile):
        which = i * TILE // d
        values = nn(r.a[...], tile)
        shift = jnp.where(which == 0, 1.0, 0.0) * vec[2:3, columns_of(i % (d // TILE), TILE)] + jnp.where(
            which == 2, 1.0, 0.0
        ) * vec[3:4, columns_of(i % (d // TILE), TILE)]
        r.qkv[:, columns_of(i, TILE)] = (values + shift).astype(BF16)

    tile_stream(QKV, 0, 3 * d, qkv_tile)
    one_far = transpose_out(r.a, r.one_t, r.one_far)

    low_lane = lax.broadcasted_iota(jnp.int32, (MB_ROWS, 128), 1) < HEAD_DIM
    scale = 1.0 / math.sqrt(HEAD_DIM)

    def stacked(value):
        zero = jnp.zeros_like(value)
        return jnp.concatenate([jnp.where(low_lane, value, zero), jnp.where(low_lane, zero, value)], axis=0)

    def merged(value):
        return jnp.where(low_lane, value[:MB_ROWS], value[MB_ROWS:])

    def attend(p, carry):
        row = lax.broadcasted_iota(jnp.int32, (2 * MB_ROWS, 128), 0)
        dist = (row % MB_ROWS - lax.broadcasted_iota(jnp.int32, (2 * MB_ROWS, 128), 1)).astype(F32)
        head = (2 * p + row // MB_ROWS).astype(F32)
        alibi = jnp.where(dist >= 0, -jnp.exp2((head + 1.0) * (-8.0 / HEADS)) * dist, -1e30)
        for s in range(slots):
            span = pl.ds(s * MB_ROWS, MB_ROWS)
            q = r.qkv[span, columns_of(p, 128)]
            k = r.qkv[span, columns_of(p + heads2, 128)]
            v = r.qkv[span, columns_of(p + 2 * heads2, 128)]
            scores = nt(stacked(q), k) * scale + alibi
            top = jnp.max(scores, axis=-1, keepdims=True)
            grown = jnp.exp(scores - top)
            probs = grown / jnp.sum(grown, axis=-1, keepdims=True)
            r.probs[p * slots + s] = probs
            r.attn[span, columns_of(p, 128)] = merged(nn(probs.astype(BF16), v)).astype(BF16)
        return carry

    down1.relay(1)
    up0.land(3)
    ahead.land(2)
    ahead_up.land(3)
    lax.fori_loop(0, heads2 // 2, attend, 0)
    down1.land(1)
    down0.land(2)
    lax.fori_loop(heads2 // 2, heads2, attend, 0)
    attn_far = transpose_out(r.attn, r.attn_t, r.attn_far)

    def out_tile(i, tile):
        span = columns_of(i, TILE)
        r.h1[:, span] = r.tokens[:, span].astype(F32) + nn(r.attn[...], tile) + vec[4:5, span]

    tile_stream(OUT, 0, d, out_tile)
    ahead.relay(3)

    def second_in(span):
        normed, _ = row_stats(r.h1[span, :])
        r.a[span, :] = (normed * vec[5:6, :] + vec[6:7, :]).astype(BF16)

    chunks(rows, 32, second_in)
    two_far = transpose_out(r.a, r.two_t, r.two_far)

    def up_tile(i, tile):
        pre = nn(r.a[...], tile) + bias[:, columns_of(i, TILE)]
        value, slope = gelu_pair(pre)
        r.act[:, columns_of(i, TILE)] = value.astype(BF16)
        r.slope[:, columns_of(i, TILE)] = slope.astype(BF16)

    ahead_up.finish()
    tile_stream(UP, end_ff, ff, up_tile)
    up0.finish()
    down1.land(2)
    up1.land(3)
    tile_stream(UP, 0, mid_ff, up_tile)
    act_far0 = transpose_out(r.act, r.act_t, r.act_far, 0, mid_ff // 256)
    act_far2 = transpose_out(r.act, r.act_t, r.act_far, end_ff // 256, 16)
    up1.finish()
    tile_stream(UP, mid_ff, end_ff, up_tile)
    act_far1 = transpose_out(r.act, r.act_t, r.act_far, mid_ff // 256, end_ff // 256)
    down0.land(3)
    dy_swap.wait()
    act_far2.wait()
    act_far0.wait()
    act_far1.wait()

    reduces = [
        Reduce(wires, r.grad[which], span, landing, colours, place)
        for (which, span, colours), landing in zip(reduce_parts(short, tall, d, ff), r.landing)
    ]

    def weight_grad(which, turned, far, near_d, far_d, low, high):
        grad = r.grad[which]
        block = turned.shape[2]
        width = 512 if (high - low) % 512 == 0 and low % 512 == 0 else high - low
        total = (high - low) // width
        groups = max(1, 16 * block // 512)
        each = 16 // groups

        def step(i, carry):
            at, g = i // groups, i % groups
            left = turned[pl.ds(g * each, each), core].reshape(each * block, rows)
            other = far[pl.ds(g * each, each)].reshape(each * block, rows)
            span = pl.ds(pl.multiple_of(low + at * width, 128), width)
            value = nn(left, near_d[:, span]) + nn(other, far_d[:, span])
            value = value.astype(BF16)
            if groups == 1:
                grad[:, :, :, :, span] = value.reshape(*sizes, block, width)
            else:
                grad[g, :, :, :, span] = value.reshape(*sizes[1:], block, width)
            return carry

        assert groups in (1, sizes[0])
        lax.fori_loop(0, total * groups, step, 0)

    late = LATE_TILES * 128
    weight_grad(DOWN, r.act_t, r.act_far, r.dy, r.dy_far, d - late, d)
    line = LineReduce(wires, r.grad[DOWN], (d - late, late), r.line[0], place, False)
    line.start()
    weight_grad(DOWN, r.act_t, r.act_far, r.dy, r.dy_far, 0, d - late)
    reduces[0].start(0)
    reduces[1].start(0)
    ahead.land(3)
    down1.land(3)
    down0.finish()
    down1.finish()
    ahead.finish()

    sums = r.sums
    sums[...] = jnp.zeros_like(sums)
    acc = r.da

    def begin(span):
        acc[span, :] = r.h1[span, :] + vec[7:8, :]
        sums[7:8, :] += jnp.sum(r.dy[span, :].astype(F32), axis=0, keepdims=True)

    chunks(rows, 32, begin)

    def down_tile(i, s):
        tile = r.deep[s].reshape(-1, d)
        wide = tile.shape[0]
        span = columns_of(i, wide)
        acc[...] += nn(r.act[:, span], tile)
        d_pre = nt(r.dy[...], tile) * r.slope[:, span].astype(F32)
        r.bias_sum[:, span] = jnp.sum(d_pre, axis=0, keepdims=True)
        r.act[:, span] = d_pre.astype(BF16)

    full_down = r.full[DOWN]
    tiles = sizes[0] * sizes[1]

    def down_pass(low):
        stream(
            tiles // 2,
            lambda i: full_down.at[(i + low) // sizes[1], (i + low) % sizes[1]],
            lambda s: r.deep.at[s],
            r.tile_sem,
            lambda i, s: down_tile(i + low, s),
        )
        span = pl.ds(low * (ff // tiles), ff // 2)
        return wires.swap(r.act.at[:, span], r.pre_far.at[:, span])

    def advance(part, stage):
        reduces[part].land()
        reduces[part].add(stage - 1)
        reduces[part].start(stage)

    def complete(part, which):
        reduces[part].land()
        reduces[part].add(2, r.fin[which])

    down_line = LineReduce(wires, r.grad[DOWN], (0, d - late), r.line[1], place, True)
    up_lines = [
        LineReduce(wires, r.grad[UP], (at * ff // 2, ff // 2), r.line[2 + at], place, True) for at in range(2)
    ]

    def settle(part):
        reduces[part].land()
        reduces[part].add(1)

    pre_swap0 = down_pass(0)
    advance(0, 1)
    pre_swap1 = down_pass(tiles // 2)
    advance(1, 1)
    two_far.wait()
    pre_swap0.wait()
    weight_grad(UP, r.two_t, r.two_far, r.act, r.pre_far, 0, ff // 2)
    reduces[2].start(0)
    pre_swap1.wait()
    weight_grad(UP, r.two_t, r.two_far, r.act, r.pre_far, ff // 2, ff)
    reduces[3].start(0)
    r.a[...] = acc[...].astype(BF16)

    def row_stream(which, left):
        full, slot = r.full[which], r.flat
        width = full.shape[-1]

        def work(i, s):
            tile = slot[s, :, :, :, :, pl.ds(0, width)].reshape(-1, width)
            return nt(left[...], tile)

        def run(put):
            stream(
                sizes[0],
                lambda i: full.at[i],
                lambda s: slot.at[s, :, :, :, :, pl.ds(0, width)],
                r.tile_sem,
                lambda i, s: put(i, work(i, s)),
            )

        return run

    def put_da(i, value):
        r.da[:, columns_of(i, value.shape[1])] = value

    row_stream(UP, r.act)(put_da)

    line.across()

    def norm_two_back(span):
        normed, rstd = row_stats(r.h1[span, :])
        da = r.da[span, :]
        sums[5:6, :] += jnp.sum(da * normed, axis=0, keepdims=True)
        sums[6:7, :] += jnp.sum(da, axis=0, keepdims=True)
        d_h1 = r.dy[span, :].astype(F32) + norm_back(da, normed, rstd, vec[5:6, :])
        sums[4:5, :] += jnp.sum(d_h1, axis=0, keepdims=True)
        r.h1[span, :] = d_h1
        r.d_mid[span, :] = d_h1.astype(BF16)

    chunks(rows, 32, norm_two_back)
    stores = []

    def keep(source, target):
        copy = pltpu.make_async_copy(source, target, r.store_sem.at[len(stores)])
        copy.start()
        stores.append(copy)

    keep(r.a, r.output)
    mid_swap = wires.swap(r.d_mid, r.mid_far)

    def put_attn(i, value):
        r.d_attn[:, columns_of(i, value.shape[1])] = value.astype(BF16)

    row_stream(OUT, r.d_mid)(put_attn)

    advance(2, 1)
    settle(0)
    settle(1)
    down_line.start()
    attn_far.wait()
    mid_swap.wait()
    weight_grad(OUT, r.attn_t, r.attn_far, r.d_mid, r.mid_far, 0, d)

    def attend_back(p, carry):
        span_p = columns_of(p, 128)
        d_bq = jnp.zeros((1, 128), F32)
        d_bv = jnp.zeros((1, 128), F32)
        for s in range(slots):
            span = pl.ds(s * MB_ROWS, MB_ROWS)
            q = stacked(r.qkv[span, span_p])
            k = r.qkv[span, columns_of(p + heads2, 128)]
            v = r.qkv[span, columns_of(p + 2 * heads2, 128)]
            do = r.d_attn[span, span_p]
            probs = r.probs[p * slots + s]
            both = stacked(do)
            d_v = tn(probs.astype(BF16), both)
            d_probs = nt(both, v)
            weighed = do.astype(F32) * r.attn[span, span_p].astype(F32)
            delta = jnp.sum(stacked(weighed), axis=-1, keepdims=True)
            d_scores = (probs * (d_probs - delta)).astype(BF16)
            d_q = merged(nn(d_scores, k)) * scale
            d_k = tn(d_scores, q) * scale
            d_bq += jnp.sum(d_q, axis=0, keepdims=True)
            d_bv += jnp.sum(d_v, axis=0, keepdims=True)
            r.qkv[span, span_p] = d_q.astype(BF16)
            r.qkv[span, columns_of(p + heads2, 128)] = d_k.astype(BF16)
            r.qkv[span, columns_of(p + 2 * heads2, 128)] = d_v.astype(BF16)
        sums[2:3, span_p] = d_bq
        sums[3:4, span_p] = d_bv
        return carry

    lax.fori_loop(0, heads2 // 2, attend_back, 0)
    advance(3, 1)
    reduces[4].start(0)
    lax.fori_loop(heads2 // 2, heads2, attend_back, 0)
    qkv_swap = wires.swap(r.qkv, r.qkv_far)
    down_line.across()
    row_stream(QKV, r.qkv)(put_da)
    settle(2)
    up_lines[0].start()
    one_far.wait()
    qkv_swap.wait()
    weight_grad(QKV, r.one_t, r.one_far, r.qkv, r.qkv_far, 0, d)
    reduces[5].start(0)
    weight_grad(QKV, r.one_t, r.one_far, r.qkv, r.qkv_far, d, 2 * d)
    reduces[6].start(0)
    settle(3)
    up_lines[1].start()
    weight_grad(QKV, r.one_t, r.one_far, r.qkv, r.qkv_far, 2 * d, 3 * d)
    line.back()

    def norm_one_back(span):
        normed, rstd = row_stats(r.tokens[span, :].astype(F32))
        da = r.da[span, :]
        sums[0:1, :] += jnp.sum(da * normed, axis=0, keepdims=True)
        sums[1:2, :] += jnp.sum(da, axis=0, keepdims=True)
        r.h1[span, :] = r.h1[span, :] + norm_back(da, normed, rstd, vec[0:1, :])

    chunks(rows, 32, norm_one_back)
    down_line.back()

    bundle = r.bundle
    for j in range(devices):
        at = (j // per) * 128
        bundle[flat[j]] = jnp.concatenate(
            [sums[:, at:at + 128], jnp.broadcast_to(r.bias_sum[:, j * 128:(j + 1) * 128], (8, 128))], axis=0
        )
    tiny_swap = wires.swap(bundle.at[:, :, :, 1 - core], r.tiny_far)
    tiny = reduces[8]
    keep(r.h1, r.input_grad)
    advance(4, 1)
    up_lines[0].across()
    tiny_swap.wait()
    r.grad[SMALL][...] = bundle[:, :, :, core] + r.tiny_far[...]
    tiny.start(0)
    advance(5, 1)
    reduces[7].start(0)
    up_lines[1].across()
    down_line.complete(r.fin[DOWN])
    advance(6, 1)
    up_lines[0].back()
    advance(4, 2)
    advance(5, 2)
    up_lines[1].back()
    advance(7, 1)
    line.second()
    advance(6, 2)
    up_lines[0].complete(r.fin[UP])
    advance(7, 2)
    advance(8, 1)
    line.third()
    advance(8, 2)
    up_lines[1].complete(r.fin[UP])
    complete(4, OUT)
    keep(r.fin[UP], r.final[UP])
    complete(5, QKV)
    keep(r.fin[OUT], r.final[OUT])
    complete(6, QKV)
    line.finish(r.fin[DOWN])
    keep(r.fin[DOWN], r.final[DOWN])
    complete(8, SMALL)
    keep(r.fin[SMALL], r.final[SMALL])
    complete(7, QKV)
    keep(r.fin[QKV], r.final[QKV])
    for copy in stores:
        copy.wait()
    wires.drain()


def reduce_parts(short, tall, d, ff):
    rows, half_ff = (0, short), ff // 2

    def colours(start, width, last):
        return split_colours(start, in_thirds(width, last), REDUCE_ORDERS)

    return [
        (DOWN, (0, tall // 2), colours(0, d - LATE_TILES * 128, 0)),
        (DOWN, (tall // 2, tall // 2), colours(0, d - LATE_TILES * 128, 0)),
        (UP, rows, colours(0, half_ff, 0)),
        (UP, rows, colours(half_ff, half_ff, 0)),
        (OUT, rows, colours(0, d, 0)),
        (QKV, rows, colours(0, d, 0)),
        (QKV, rows, colours(d, d, 0)),
        (QKV, rows, colours(2 * d, d, 0)),
        (SMALL, (0, 16), [(0, 128, (2, 1, 0))]),
    ]


def fused_step(tokens, cotangent, lengths, vectors, bias_up, w_qkv, w_out, w_up, w_down):
    sizes = SIZES
    rows, d = tokens.shape
    ff = w_up.shape[1]
    short, tall = w_out.shape[0], w_down.shape[0]
    heads2 = d // 128
    slots = rows // MB_ROWS
    whole = lambda s: jax.ShapeDtypeStruct((*sizes, 2, *s), BF16)
    like = jax.ShapeDtypeStruct
    wide = ((16, 128), (short, d), (short, 3 * d), (short, ff), (tall, d))
    v = pltpu.VMEM
    turned, across = v((16, 2, short, rows), BF16), v((16, short, rows), BF16)
    flat, double = v((rows, d), BF16), v((rows, d), F32)
    near = dict(vectors=vectors, bias_up=bias_up)
    distant = dict(tokens_in=tokens, cotangent=cotangent, own=[None, w_out, w_qkv, w_up, w_down])
    results = dict(
        full=[whole(s) for s in wide], gauge=like((180_224, 128), BF16),
        output=like((rows, d), BF16), input_grad=like((rows, d), F32), final=[like(s, F32) for s in wide],
    )
    parts = reduce_parts(short, tall, d, ff)
    scratch = dict(
        low=[v(s, BF16) for s in wide], block=v((16, 128), F32), dy=flat, tokens=flat,
        fin=[v(s, F32) for s in wide],
        smalls=v((*sizes, 2, 16, 128), BF16), vec=v((8, d), F32), bias=v((1, ff), F32),
        dy_far=flat, da=double, a=flat, qkv=v((rows, 3 * d), BF16), qkv_far=v((rows, 3 * d), BF16),
        probs=v((heads2 * slots, 2 * MB_ROWS, 128), F32), attn=flat, h1=double,
        act=v((rows, ff), BF16), slope=v((rows, ff), BF16), pre_far=v((rows, ff), BF16),
        d_mid=flat, mid_far=flat, d_attn=flat,
        one_t=turned, one_far=across, attn_t=turned, attn_far=across, two_t=turned, two_far=across,
        act_t=v((16, 2, tall, rows), BF16), act_far=v((16, tall, rows), BF16),
        wide=v((2, *sizes, 2, short, TILE), BF16), deep=v((2, sizes[2], 2, tall, d), BF16),
        flat=v((2, *sizes[1:], 2, short, ff), BF16),
        grad=[v((*sizes, *s), BF16 if at else F32) for at, s in enumerate(wide)],
        sums=v((8, d), F32), bias_sum=v((1, ff), F32),
        bundle=v((*sizes, 2, 16, 128), F32), tiny_far=v((*sizes, 16, 128), F32),
        landing=[
            landing_shapes(span[1], colours, sizes, BF16 if which else F32, 2 if which in (UP, DOWN) else 3)
            for which, span, colours in parts
        ],
        line=[
            line_landing(tall, LATE_TILES * 128, False), line_landing(tall, d - LATE_TILES * 128, True),
            line_landing(short, ff // 2, True), line_landing(short, ff // 2, True),
        ],
        send_sem=pltpu.SemaphoreType.DMA((2,)), recv_sem=pltpu.SemaphoreType.DMA((97,)),
        mine_sem=pltpu.SemaphoreType.DMA((5,)), tile_sem=pltpu.SemaphoreType.DMA((2,)),
        load_sem=pltpu.SemaphoreType.DMA((6,)), store_sem=pltpu.SemaphoreType.DMA((7,)),
    )
    names = {**dict(lengths=lengths), **near, **distant, **results, **scratch}
    found = pl.pallas_call(
        functools.partial(step_kernel, shape_of(names)),
        out_shape=leaves(results),
        in_specs=[pl.BlockSpec(memory_space=pltpu.SMEM)]
        + [pl.BlockSpec(memory_space=v)] * len(leaves(near))
        + [pl.BlockSpec(memory_space=pltpu.HBM)] * len(leaves(distant)),
        out_specs=[pl.BlockSpec(memory_space=pltpu.HBM)] * len(leaves(results)),
        scratch_shapes=leaves(scratch),
        compiler_params=pltpu.CompilerParams(
            collective_id=1, has_side_effects=True, vmem_limit_bytes=67_000_000
        ),
        name="fused_step",
    )(lengths, *leaves(near), *leaves(distant))
    return Box(unpack(shape_of(results), iter(found)))


def adam_kernel(shape, *refs):
    r = Box(unpack(shape, iter(refs)))
    me = lax.axis_index("dp")
    count = float(STEP)

    def put(at, param, first, second, grad):
        update, new_first, new_second = adamw(param, (first, second), grad, count)
        r.grads[at][...] = grad
        r.updates[at][...] = update
        r.firsts[at][...] = new_first
        r.seconds[at][...] = new_second

    for at in range(2, 6):
        put(at, r.params[at][...], r.moments[at][0], r.moments[at][1], r.final[at - 1][...])
    r.output[...] = r.early_output[...]
    r.input_grad[...] = r.early_grad[...]

    @pl.when(pl.program_id(0) == 0)
    def _():
        narrow = r.params[0].shape[1]
        per = 128 // narrow
        grad = jnp.zeros((8, narrow), F32)
        for k in range(per):
            grad = grad + jnp.where(me % per == k, 1.0, 0.0) * r.final[SMALL][0:8, k * narrow:(k + 1) * narrow]
        put(0, r.params[0][...], r.moments[0][0], r.moments[0][1], grad)
        put(1, r.params[1][...], r.moments[1][0:1], r.moments[1][1:2], r.final[SMALL][8:9, :])


def adam(found, params, moments):
    steps = 2

    def whole(s):
        return pl.BlockSpec(s, lambda i: (0,) * len(s))

    def cut(s):
        return pl.BlockSpec((*s[:-1], s[-1] // steps), lambda i: (0,) * (len(s) - 1) + (i,))

    def tall(s):
        return pl.BlockSpec((s[0] // steps, s[1]), lambda i: (i, 0))

    def each(make):
        return [make(p.shape) for p in params]

    like = jax.ShapeDtypeStruct
    outs = each(lambda s: like(s, F32))
    specs = [whole(p.shape) if at < 2 else cut(p.shape) for at, p in enumerate(params)]
    moment_specs = [whole(m.shape) if at < 2 else cut(m.shape) for at, m in enumerate(moments)]
    inputs = dict(
        params=list(params), moments=list(moments), final=found.final,
        early_output=found.output, early_grad=found.input_grad,
    )
    input_specs = dict(
        params=specs, moments=moment_specs, final=[whole((16, 128)), *specs[2:]],
        early_output=tall(found.output.shape), early_grad=tall(found.input_grad.shape),
    )
    results = dict(
        grads=outs, updates=outs, firsts=outs, seconds=outs,
        output=like(found.output.shape, BF16), input_grad=like(found.input_grad.shape, F32),
    )
    result_specs = dict(
        grads=specs, updates=specs, firsts=specs, seconds=specs,
        output=tall(found.output.shape), input_grad=tall(found.input_grad.shape),
    )
    shape = shape_of({**inputs, **results})
    done = pl.pallas_call(
        functools.partial(adam_kernel, shape),
        grid=(steps,),
        out_shape=leaves(results),
        in_specs=leaves(input_specs),
        out_specs=leaves(result_specs),
        compiler_params=pltpu.CompilerParams(vmem_limit_bytes=67_000_000),
        name="adam",
    )(*leaves(inputs))
    return Box(unpack(shape_of(results), iter(done)))


def general_body(
    tokens,
    cotangent,
    lengths,
    vectors,
    bias_up,
    w_qkv,
    w_out,
    w_up,
    w_down,
    mom_vectors,
    mom_bias_up,
    mom_qkv,
    mom_out,
    mom_up,
    mom_down,
):
    params = (vectors, bias_up, w_qkv, w_out, w_up, w_down)
    moments = (mom_vectors, mom_bias_up, mom_qkv, mom_out, mom_up, mom_down)
    me = lax.axis_index("dp")
    count = lax.axis_size("dp")
    small, full_out, full_qkv, full_up, full_down = gather_all(
        [small_block(vectors, bias_up, me), w_out, w_qkv, w_up, w_down], count
    )
    vec_low, bias_low = small_parts(small, vectors, bias_up)
    weights = (
        vec_low,
        bias_low,
        full_qkv.reshape(-1, w_qkv.shape[1]),
        full_out.reshape(-1, w_out.shape[1]),
        full_up.reshape(-1, w_up.shape[1]),
        full_down.reshape(-1, w_down.shape[1]),
    )
    alibi = alibi_bias(MB_ROWS)
    place = jnp.arange(MB_ROWS)
    owned = tuple((jnp.zeros(p.shape, jnp.float32) for p in params))
    summed = None
    out_list = []
    dx_list = []
    for micro in range(MICRO):
        x_rows = tokens[micro * MB_ROWS : (micro + 1) * MB_ROWS]
        live = place < lengths[micro]
        grad_rows = jnp.where(
            live[:, None],
            cotangent[micro * MB_ROWS : (micro + 1) * MB_ROWS],
            jnp.zeros((), jnp.bfloat16),
        )
        out, saved = forward_block(x_rows, weights, alibi)
        d_x, grads = backward_block(saved, grad_rows, weights, alibi)
        out_list.append(out)
        dx_list.append(d_x)
        summed = grads if summed is None else tuple((a + b for a, b in zip(summed, grads)))
    owned = (
        lax.psum_scatter(summed[0], "dp", scatter_dimension=1, tiled=True),
        lax.psum_scatter(summed[1], "dp", scatter_dimension=0, tiled=True),
        lax.psum_scatter(summed[2], "dp", scatter_dimension=0, tiled=True),
        lax.psum_scatter(summed[3], "dp", scatter_dimension=0, tiled=True),
        lax.psum_scatter(summed[4], "dp", scatter_dimension=0, tiled=True),
        lax.psum_scatter(summed[5], "dp", scatter_dimension=0, tiled=True),
    )
    count = float(STEP)
    news = [adamw(p, m, g, count) for p, m, g in zip(params, moments, owned)]
    output = jnp.concatenate(out_list, axis=0)
    input_grad = jnp.concatenate(dx_list, axis=0)
    return (
        output,
        input_grad,
        owned[0],
        owned[1],
        owned[2],
        owned[3],
        owned[4],
        owned[5],
        news[0][0],
        news[1][0],
        news[2][0],
        news[3][0],
        news[4][0],
        news[5][0],
        news[0][1],
        news[1][1],
        news[2][1],
        news[3][1],
        news[4][1],
        news[5][1],
        news[0][2],
        news[1][2],
        news[2][2],
        news[3][2],
        news[4][2],
        news[5][2],
    )


def body(
    tokens, cotangent, lengths, vectors, bias_up, w_qkv, w_out, w_up, w_down,
    mom_vectors, mom_bias_up, mom_qkv, mom_out, mom_up, mom_down,
):
    if grid_of(lax.axis_size("dp")) != SIZES:
        return general_body(
            tokens, cotangent, lengths, vectors, bias_up, w_qkv, w_out, w_up, w_down,
            mom_vectors, mom_bias_up, mom_qkv, mom_out, mom_up, mom_down,
        )
    span = bias_up.shape[0]
    found = fused_step(tokens, cotangent, lengths, vectors, bias_up.reshape(1, span), w_qkv, w_out, w_up, w_down)
    found.final[OUT], found.final[QKV] = found.final[QKV], found.final[OUT]
    done = adam(
        found,
        (vectors, bias_up.reshape(1, span), w_qkv, w_out, w_up, w_down),
        (mom_vectors, mom_bias_up, mom_qkv, mom_out, mom_up, mom_down),
    )

    def six(arrays):
        return (arrays[0], arrays[1].reshape(span), *arrays[2:])

    return (
        done.output, done.input_grad, *six(done.grads), *six(done.updates), *six(done.firsts), *six(done.seconds),
    )


def solution(mesh):
    in_specs = (
        P("dp", None),
        P("dp", None),
        P("dp"),
        P(None, "dp"),
        P("dp"),
        P("dp", None),
        P("dp", None),
        P("dp", None),
        P("dp", None),
        P(None, None, "dp"),
        P(None, "dp"),
        P(None, "dp", None),
        P(None, "dp", None),
        P(None, "dp", None),
        P(None, "dp", None),
    )
    out_specs = (
        P("dp", None),
        P("dp", None),
        P(None, "dp"),
        P("dp"),
        P("dp", None),
        P("dp", None),
        P("dp", None),
        P("dp", None),
        P(None, "dp"),
        P("dp"),
        P("dp", None),
        P("dp", None),
        P("dp", None),
        P("dp", None),
        P(None, "dp"),
        P("dp"),
        P("dp", None),
        P("dp", None),
        P("dp", None),
        P("dp", None),
        P(None, "dp"),
        P("dp"),
        P("dp", None),
        P("dp", None),
        P("dp", None),
        P("dp", None),
    )
    return jax.shard_map(body, mesh=mesh, in_specs=in_specs, out_specs=out_specs, check_vma=False)
```

```python
import functools
import math

import jax
import jax.numpy as jnp
from jax import lax
from jax.experimental import pallas as pl
from jax.experimental.pallas import tpu as pltpu
from jax.sharding import PartitionSpec as P

D = 1024
HEADS = 16
HEAD_DIM = 64
MB_ROWS = 128
MICRO = 2
STEP = 3


ln_eps = 1e-05
gelu_c = math.sqrt(2.0 / math.pi)
beta_one = 0.9
beta_two = 0.95
decay_rate = 0.1
adam_eps = 1e-08


def product(left, right):
    return jnp.dot(left, right, preferred_element_type=jnp.float32)


def contract(form, left, right):
    return jnp.einsum(form, left, right, preferred_element_type=jnp.float32)


def layer_norm(values, gain, shift):
    centred = values - jnp.mean(values, axis=-1, keepdims=True)
    rstd = lax.rsqrt(jnp.mean(centred * centred, axis=-1, keepdims=True) + ln_eps)
    normed = centred * rstd
    return (normed * gain + shift, normed, rstd)


def norm_back(grad_in, normed, rstd, gain):
    scaled = grad_in * gain
    inner = (
        scaled
        - jnp.mean(scaled, axis=-1, keepdims=True)
        - normed * jnp.mean(scaled * normed, axis=-1, keepdims=True)
    )
    return rstd * inner


def gelu_pair(pre):
    tanh_val = jnp.tanh(gelu_c * (pre + 0.044715 * pre * pre * pre))
    value = 0.5 * pre * (1.0 + tanh_val)
    slope = 0.5 * (1.0 + tanh_val) + 0.5 * pre * (1.0 - tanh_val * tanh_val) * gelu_c * (
        1.0 + 3.0 * 0.044715 * pre * pre
    )
    return (value, slope)


def alibi_bias(rows):
    place = jnp.arange(rows)
    dist = (place[:, None] - place[None, :]).astype(jnp.float32)
    slopes = jnp.exp2(-8.0 * (jnp.arange(HEADS) + 1).astype(jnp.float32) / HEADS)
    bias = -slopes[:, None, None] * dist[None]
    return jnp.where(dist[None] >= 0, bias, -1e30)


def attention_scores(q3, k3, alibi):
    return contract("qhd,khd->hqk", q3, k3) * (1.0 / math.sqrt(HEAD_DIM)) + alibi


def forward_block(x_rows, weights, alibi):
    vec, up_bias, qkv_w, out_w, up_w, down_w = weights
    vecf = vec.astype(jnp.float32)
    rows = x_rows.shape[0]
    xf = x_rows.astype(jnp.float32)
    ln_one, normed_one, rstd_one = layer_norm(xf, vecf[0], vecf[1])
    a_one = ln_one.astype(jnp.bfloat16)
    qkv = product(a_one, qkv_w)
    query = (qkv[:, :D] + vecf[2]).astype(jnp.bfloat16).reshape(rows, HEADS, HEAD_DIM)
    keyx = qkv[:, D : 2 * D].astype(jnp.bfloat16).reshape(rows, HEADS, HEAD_DIM)
    value = (qkv[:, 2 * D :] + vecf[3]).astype(jnp.bfloat16).reshape(rows, HEADS, HEAD_DIM)
    scores = attention_scores(query, keyx, alibi)
    top = jnp.max(scores, axis=-1, keepdims=True)
    lse = top + jnp.log(jnp.sum(jnp.exp(scores - top), axis=-1, keepdims=True))
    probs = jnp.exp(scores - lse).astype(jnp.bfloat16)
    attn = contract("hqk,khd->qhd", probs, value).reshape(rows, D).astype(jnp.bfloat16)
    h_one = xf + product(attn, out_w) + vecf[4]
    ln_two, normed_two, rstd_two = layer_norm(h_one, vecf[5], vecf[6])
    a_two = ln_two.astype(jnp.bfloat16)
    pre = product(a_two, up_w) + up_bias.astype(jnp.float32)
    act, slope = gelu_pair(pre)
    act_b = act.astype(jnp.bfloat16)
    out = (h_one + product(act_b, down_w) + vecf[7]).astype(jnp.bfloat16)
    saved = (
        normed_one,
        rstd_one,
        a_one,
        query,
        keyx,
        value,
        lse,
        attn,
        normed_two,
        rstd_two,
        a_two,
        slope,
        act_b,
    )
    return (out, saved)


def backward_block(saved, grad_rows, weights, alibi):
    vec, up_bias, qkv_w, out_w, up_w, down_w = weights
    vecf = vec.astype(jnp.float32)
    (
        normed_one,
        rstd_one,
        a_one,
        query,
        keyx,
        value,
        lse,
        attn,
        normed_two,
        rstd_two,
        a_two,
        slope,
        act_b,
    ) = saved
    rows = grad_rows.shape[0]
    scale = 1.0 / math.sqrt(HEAD_DIM)
    dyf = grad_rows.astype(jnp.float32)
    g_bdown = jnp.sum(dyf, axis=0)
    g_down = product(act_b.T, grad_rows)
    d_pre = product(grad_rows, down_w.T) * slope
    g_bup = jnp.sum(d_pre, axis=0)
    d_pre_b = d_pre.astype(jnp.bfloat16)
    g_up = product(a_two.T, d_pre_b)
    d_a2 = product(d_pre_b, up_w.T)
    g_ln2g = jnp.sum(d_a2 * normed_two, axis=0)
    g_ln2b = jnp.sum(d_a2, axis=0)
    d_h1 = dyf + norm_back(d_a2, normed_two, rstd_two, vecf[5])
    g_bout = jnp.sum(d_h1, axis=0)
    d_h1_b = d_h1.astype(jnp.bfloat16)
    g_out = product(attn.T, d_h1_b)
    d_attn = product(d_h1_b, out_w.T).astype(jnp.bfloat16).reshape(rows, HEADS, HEAD_DIM)
    probs_f = jnp.exp(attention_scores(query, keyx, alibi) - lse)
    probs = probs_f.astype(jnp.bfloat16)
    d_v = contract("hqk,qhd->khd", probs, d_attn).reshape(rows, D)
    d_probs = contract("qhd,khd->hqk", d_attn, value)
    delta = jnp.sum(
        d_attn.astype(jnp.float32) * attn.reshape(rows, HEADS, HEAD_DIM).astype(jnp.float32),
        axis=-1,
    ).T[:, :, None]
    d_scores = (probs_f * (d_probs - delta)).astype(jnp.bfloat16)
    d_q = (contract("hqk,khd->qhd", d_scores, keyx) * scale).reshape(rows, D)
    d_k = (contract("hqk,qhd->khd", d_scores, query) * scale).reshape(rows, D)
    g_bq = jnp.sum(d_q, axis=0)
    g_bv = jnp.sum(d_v, axis=0)
    d_qkv = jnp.concatenate([d_q, d_k, d_v], axis=1).astype(jnp.bfloat16)
    g_qkv = product(a_one.T, d_qkv)
    d_a1 = product(d_qkv, qkv_w.T)
    g_ln1g = jnp.sum(d_a1 * normed_one, axis=0)
    g_ln1b = jnp.sum(d_a1, axis=0)
    d_x = d_h1 + norm_back(d_a1, normed_one, rstd_one, vecf[0])
    g_vec = jnp.stack([g_ln1g, g_ln1b, g_bq, g_bv, g_bout, g_ln2g, g_ln2b, g_bdown])
    return (d_x, (g_vec, g_bup, g_qkv, g_out, g_up, g_down))


def adamw(param, moments, grad, count):
    first = beta_one * moments[0] + (1.0 - beta_one) * grad
    second = beta_two * moments[1] + (1.0 - beta_two) * grad * grad
    corr_one = 1.0 - beta_one**count
    corr_two = 1.0 - beta_two**count
    update = first / corr_one / (jnp.sqrt(second / corr_two) + adam_eps) + decay_rate * param
    return (update, first, second)


MESH_ID = pl.DeviceIdType.MESH


def grid_of(count):
    known = {32: (4, 2, 2), 128: (4, 4, 4)}
    return known.get(count, (count // 2,))


def locate(me, sizes):
    rest, coords = me // 2, []
    for size in reversed(sizes):
        coords.append(rest % size)
        rest = rest // size
    return tuple(reversed(coords)), me % 2


def device_at(coords, core, sizes):
    index = 0
    for value, size in zip(coords, sizes):
        index = index * size + value
    return index * 2 + core


def swapped(coords, dim, value):
    return tuple(value if at == dim else old for at, old in enumerate(coords))


def neighbours(coords, core, sizes):
    found = [device_at(coords, 1 - core, sizes)]
    for dim, size in enumerate(sizes):
        for step in range(1, size):
            found.append(device_at(swapped(coords, dim, (coords[dim] + step) % size), core, sizes))
    return found


def greet(others):
    barrier = pltpu.get_barrier_semaphore()
    for other in others:
        pl.semaphore_signal(barrier, inc=1, device_id=(other,), device_id_type=MESH_ID)
    pl.semaphore_wait(barrier, len(others))


class Sems:
    def __init__(self, send, recv):
        self.send, self.recv, self.used = send, recv, 0

    def pair(self):
        at = self.used
        self.used += 1
        return self.send.at[at], self.recv.at[at]


def remote(sems, src, dst, target):
    send_sem, recv_sem = sems.pair()
    copy = pltpu.make_async_remote_copy(
        src_ref=src, dst_ref=dst, send_sem=send_sem, recv_sem=recv_sem,
        device_id=(target,), device_id_type=MESH_ID,
    )
    copy.start()
    return copy


class Gather:
    def __init__(self, full, colours, sizes, coords, core, sems):
        self.full, self.colours, self.sizes = full, colours, sizes
        self.coords, self.core, self.sems = coords, core, sems
        self.axis = [[] for _ in colours]
        self.swap = []
        self.sent = []

    def view(self, colour, fixed):
        start, width, _ = colour
        place = tuple(fixed.get(dim, slice(None)) for dim in range(len(self.sizes)))
        return self.full.at[(*place, self.core, slice(None), pl.ds(start, width))]

    def start(self, stage, own=None):
        for at, colour in enumerate(self.colours):
            order = colour[2]
            dim = order[stage]
            fixed = {d: self.coords[d] for d in order[stage:]}
            held = self.view(colour, fixed)
            source = held if own is None else own.at[:, pl.ds(colour[0], colour[1])]
            self.axis[at] = []
            for step in range(1, self.sizes[dim]):
                peer = swapped(self.coords, dim, (self.coords[dim] + step) % self.sizes[dim])
                self.axis[at].append(remote(self.sems, source, held, device_at(peer, self.core, self.sizes)))
            self.sent += self.axis[at]

    def land(self, stage):
        partner = device_at(self.coords, 1 - self.core, self.sizes)
        for at, colour in enumerate(self.colours):
            order = colour[2]
            dim = order[stage]
            for copy in self.axis[at]:
                copy.wait_recv()
            fixed = {d: self.coords[d] for d in order[stage + 1:]}
            if stage == 0:
                views = [self.view(colour, fixed)]
            else:
                views = [
                    self.view(colour, {**fixed, dim: (self.coords[dim] + step) % self.sizes[dim]})
                    for step in range(1, self.sizes[dim])
                ]
            for view in views:
                self.swap.append(remote(self.sems, view, view, partner))

    def finish(self):
        for copy in self.swap:
            copy.wait_recv()

    def drain(self):
        for copy in self.sent + self.swap:
            copy.wait_send()


def colours_of(columns, sizes):
    last = len(sizes) - 1
    if last < 2:
        return [(0, columns, tuple(range(len(sizes))))]
    tiles = columns // 128
    if tiles < 8:
        return [(0, columns, (0, 1, 2))]
    third = max(1, tiles // 8)
    first = (tiles - third) // 2
    second = tiles - third - first
    return [
        (0, first * 128, (0, 1, 2)),
        (first * 128, second * 128, (0, 2, 1)),
        ((first + second) * 128, third * 128, (2, 1, 0)),
    ]


def gather_kernel(sizes, count, *refs):
    shards, fulls = refs[:count], refs[count : 2 * count]
    owns = refs[2 * count : 3 * count]
    send_sem, recv_sem, local_sem = refs[3 * count :]
    coords, core = locate(lax.axis_index("dp"), sizes)
    for shard, own in zip(shards, owns):
        own[...] = shard[...].astype(own.dtype)
    greet(neighbours(coords, core, sizes))
    sems = Sems(send_sem, recv_sem)
    items = [
        Gather(full, colours_of(full.shape[-1], sizes), sizes, coords, core, sems) for full in fulls
    ]
    local = []
    for at, (own, full) in enumerate(zip(owns, fulls)):
        copy = pltpu.make_async_copy(own, full.at[(*coords, core)], local_sem.at[at])
        copy.start()
        local.append(copy)
    stages = len(sizes)
    items[0].start(0, owns[0])
    for turn in range(count + stages):
        for stage in range(stages):
            at = turn - stage
            if 0 <= at < count:
                if stage == 0:
                    if at + 1 < count:
                        items[at + 1].start(0, owns[at + 1])
                    local[at].wait()
                items[at].land(stage)
                if stage + 1 < stages:
                    items[at].start(stage + 1)
        at = turn - stages
        if 0 <= at < count:
            items[at].finish()
    for item in items:
        item.drain()


def gather_all(shards, count):
    sizes = grid_of(count)
    copies = 400
    n = len(shards)
    fulls = pl.pallas_call(
        functools.partial(gather_kernel, sizes, n),
        out_shape=[jax.ShapeDtypeStruct((*sizes, 2, *s.shape), jnp.bfloat16) for s in shards],
        in_specs=[pl.BlockSpec(memory_space=pltpu.VMEM)] * n,
        out_specs=[pl.BlockSpec(memory_space=pltpu.HBM)] * n,
        scratch_shapes=[pltpu.VMEM(s.shape, jnp.bfloat16) for s in shards]
        + [pltpu.SemaphoreType.DMA((copies,)), pltpu.SemaphoreType.DMA((copies,)), pltpu.SemaphoreType.DMA((n,))],
        compiler_params=pltpu.CompilerParams(collective_id=0, has_side_effects=True),
        name="gather_all",
    )(*shards)
    return [full.reshape(-1, *full.shape[-2:]) for full in fulls]


def small_block(vectors, bias_up, me):
    wide = jnp.zeros((8, 128), jnp.float32)
    width = vectors.shape[1]
    per = 128 // width
    wide = lax.dynamic_update_slice(wide, vectors, (0, (me % per) * width))
    tail = jnp.zeros((8, 128), jnp.float32)
    span = bias_up.shape[0]
    tail = lax.dynamic_update_slice(tail, bias_up[None, :], (0, (me % (128 // span)) * span))
    return jnp.concatenate([wide, tail], axis=0)


def small_parts(small, vectors, bias_up):
    per = 128 // vectors.shape[1]
    span = 128 // bias_up.shape[0]
    n = small.shape[0]
    vec = jnp.sum(small[:, :8].astype(jnp.float32).reshape(n // per, per, 8, 128), axis=1)
    bias = jnp.sum(small[:, 8].astype(jnp.float32).reshape(n // span, span, 128), axis=1)
    return vec.transpose(1, 0, 2).reshape(8, -1).astype(jnp.bfloat16), bias.reshape(-1).astype(jnp.bfloat16)


F32, BF16 = jnp.float32, jnp.bfloat16


def nn(a, b):
    return lax.dot_general(a, b, (((1,), (0,)), ((), ())), preferred_element_type=F32)


def nt(a, b):
    return lax.dot_general(a, b, (((1,), (1,)), ((), ())), preferred_element_type=F32)


def tn(a, b):
    return lax.dot_general(a, b, (((0,), (0,)), ((), ())), preferred_element_type=F32)


def chunks(total, size, work):
    def step(i, carry):
        work(pl.ds(pl.multiple_of(i * size, size), size))
        return carry

    lax.fori_loop(0, total // size, step, 0)


def split_colours(start, shares, orders):
    found = []
    for order, share in zip(orders, shares):
        if share:
            found.append((start, share * 128, order))
            start += share * 128
    return found


def in_thirds(columns, last):
    tiles = columns // 128
    third = tiles * last // 8
    first = (tiles - third) // 2
    return first, tiles - third - first, third


class Spread:
    def __init__(self, full, own, rows, colours, relay, place):
        self.full, self.own, self.rows, self.colours = full, own, rows, colours
        self.sizes, self.coords, self.core = place
        self.hops = []
        for colour in colours:
            hops = []
            for at, dim in enumerate(colour[2]):
                fixed = {d: self.coords[d] for d in colour[2][at + 1:]}
                hops += [(dim, kind, fixed) for kind in ((1, 2) if dim == 0 and relay else (0,))]
            self.hops.append(hops)
        self.count = len(self.hops[0])

    def view(self, colour, fixed):
        where = tuple(fixed.get(dim, slice(None)) for dim in range(3))
        return self.full.at[(*where, self.core, pl.ds(*self.rows), pl.ds(colour[0], colour[1]))]

    def peer(self, dim, value):
        return device_at(swapped(self.coords, dim, value), self.core, self.sizes)

    def mine(self, at, hop):
        colour = self.colours[at]
        dim, kind, fixed = self.hops[at][hop]
        if kind == 2:
            low = self.coords[0] // 2 * 2
            return self.view(colour, {**fixed, 0: pl.ds(low, 2)})
        return self.view(colour, {**fixed, dim: self.coords[dim]})

    def far(self, at, hop):
        colour = self.colours[at]
        _, _, fixed = self.hops[at][hop]
        return self.view(colour, {**fixed, 0: pl.ds(2 - self.coords[0] // 2 * 2, 2)})

    def inner(self):
        return (self.coords[0] + 1) // 2 == 1

    def send(self, wires, hop, group):
        for at, colour in enumerate(self.colours):
            dim, kind, _ = self.hops[at][hop]
            held = self.mine(at, hop)
            source = held if hop else self.own.at[pl.ds(*self.rows), pl.ds(colour[0], colour[1])]
            here = self.coords[dim]
            if kind == 2:
                group.count(held)
                wires.send_if(self.inner(), source, held, self.peer(0, 3 - here), group)
            elif kind == 1:
                group.count(held)
                wires.send(source, held, self.peer(0, here + 1 - 2 * (here % 2)), group)
            else:
                for step in range(1, self.sizes[dim]):
                    group.count(held)
                    wires.send(source, held, self.peer(dim, (here + step) % self.sizes[dim]), group)

    def pass_on(self, wires, hop, group):
        here = self.coords[0]
        for at in range(len(self.colours)):
            if self.hops[at][hop][1] == 2:
                far = self.far(at, hop)
                wires.put(far, far, self.peer(0, here + 1 - 2 * (here % 2)), group, wires.sent_if)

    def arrived(self, hop):
        for at, colour in enumerate(self.colours):
            dim, kind, fixed = self.hops[at][hop]
            if hop == 0:
                yield self.view(colour, {**fixed, **({0: pl.ds(self.coords[0] // 2 * 2, 2)} if kind == 1 else {})})
            elif kind == 2:
                yield self.far(at, hop)
            elif kind == 1:
                yield self.view(colour, {**fixed, 0: self.coords[0] + 1 - 2 * (self.coords[0] % 2)})
            else:
                for step in range(1, self.sizes[dim]):
                    yield self.view(colour, {**fixed, dim: (self.coords[dim] + step) % self.sizes[dim]})


class Group:
    def __init__(self, sem, gauge):
        self.sem, self.gauge, self.units = sem, gauge, 0

    def count(self, ref):
        self.units += math.prod(ref.shape) * jnp.dtype(ref.dtype).itemsize // 256

    def wait(self):
        whole = self.gauge.at[pl.ds(0, self.units)]
        pltpu.make_async_copy(whole, whole, self.sem).wait()


class Chunk:
    def __init__(self, wires, parts):
        self.wires, self.parts = wires, parts
        self.arriving, self.swap, self.relayed = {}, wires.group(), set()
        self.hops = parts[0].count

    def start(self, hop):
        self.arriving[hop] = self.wires.group()
        for part in self.parts:
            part.send(self.wires, hop, self.arriving[hop])

    def relay(self, hop):
        def forward():
            self.arriving[hop].wait()
            for part in self.parts:
                part.pass_on(self.wires, hop, self.arriving[hop])

        pl.when(self.parts[0].inner())(forward)
        self.relayed.add(hop)

    def land(self, hop):
        if hop not in self.relayed and any(h[hop][1] == 2 for part in self.parts for h in part.hops):
            self.relay(hop)
        if hop in self.relayed:
            pl.when(jnp.logical_not(self.parts[0].inner()))(self.arriving[hop].wait)
        else:
            self.arriving[hop].wait()
        if hop + 1 < self.hops:
            self.start(hop + 1)
        for part in self.parts:
            for view in part.arrived(hop):
                self.swap.count(view)
                self.wires.send(view, view, self.wires.partner, self.swap)

    def finish(self):
        self.swap.wait()


class Wires:
    def __init__(self, send_sem, recv_sem, gauge, partner):
        self.recv_sem, self.gauge, self.partner = recv_sem, gauge, partner
        self.used, self.sent, self.sent_if = 0, Group(send_sem.at[0], gauge), Group(send_sem.at[1], gauge)
        self.condition = None

    def group(self):
        self.used += 1
        assert self.used <= self.recv_sem.shape[0]
        return Group(self.recv_sem.at[self.used - 1], self.gauge)

    def put(self, src, dst, target, group, sent=None):
        pltpu.make_async_remote_copy(
            src_ref=src, dst_ref=dst, send_sem=(sent or self.sent).sem, recv_sem=group.sem,
            device_id=(target,), device_id_type=MESH_ID,
        ).start()
        if sent is not None:
            sent.count(dst)

    def send(self, src, dst, target, group):
        self.put(src, dst, target, group, self.sent)

    def send_if(self, condition, src, dst, target, group):
        self.condition = condition
        pl.when(condition)(lambda: self.put(src, dst, target, group, self.sent_if))

    def swap(self, src, dst):
        group = self.group()
        group.count(dst)
        self.send(src, dst, self.partner, group)
        return group

    def drain(self):
        self.sent.wait()
        if self.condition is not None:
            pl.when(self.condition)(self.sent_if.wait)


class Reduce:
    def __init__(self, wires, held, rows, landing, colours, place):
        self.wires, self.held, self.rows, self.landing, self.colours = wires, held, rows, landing, colours
        self.sizes, self.coords, self.core = place

    def view(self, colour, fixed):
        where = tuple(fixed.get(dim, slice(None)) for dim in range(3))
        return self.held.at[(*where, pl.ds(*self.rows), pl.ds(colour[0], colour[1]))]

    def start(self, stage):
        self.arriving = self.wires.group()
        for at, colour in enumerate(self.colours):
            order = colour[2]
            dim = order[stage]
            fixed = {d: self.coords[d] for d in order[:stage]}
            for step in range(1, self.sizes[dim]):
                theirs = (self.coords[dim] + step) % self.sizes[dim]
                self.arriving.count(self.landing[at][stage].at[step - 1])
                peer = swapped(self.coords, dim, theirs)
                self.wires.send(
                    self.view(colour, {**fixed, dim: theirs}),
                    self.landing[at][stage].at[step - 1],
                    device_at(peer, self.core, self.sizes), self.arriving,
                )

    def land(self):
        self.arriving.wait()

    def add(self, stage, out=None):
        first, rows = self.rows
        for at, colour in enumerate(self.colours):
            order = colour[2]
            fixed = {d: self.coords[d] for d in order[:stage + 1]}
            free = [d for d in range(3) if d not in fixed]
            landing = self.landing[at][stage]
            counts = [self.sizes[d] for d in free]
            total = math.prod(counts)
            tall = min(rows, 32)

            def step(i, carry, colour=colour, fixed=fixed, free=free, landing=landing, counts=counts, tall=tall):
                where, rest, index = dict(fixed), i // (rows // tall), []
                for d, size in zip(reversed(free), reversed(counts)):
                    where[d] = rest % size
                    index.insert(0, rest % size)
                    rest = rest // size
                low = (i % (rows // tall)) * tall
                span = pl.ds(pl.multiple_of(first + low, tall), tall)
                local = pl.ds(pl.multiple_of(low, tall), tall)
                place = (where[0], where[1], where[2], span, pl.ds(colour[0], colour[1]))
                sums = self.held[place].astype(F32)
                for other in range(landing.shape[0]):
                    sums = sums + landing[(other, *index, local, slice(None))].astype(F32)
                if out is None:
                    self.held[place] = sums.astype(self.held.dtype)
                else:
                    out[span, pl.ds(colour[0], colour[1])] = sums
                return carry

            lax.fori_loop(0, total * (rows // tall), step, 0)


class LineReduce:
    def __init__(self, wires, held, columns, landing, place, last):
        self.wires, self.held, self.columns, self.landing = wires, held, columns, landing
        self.sizes, (self.z, self.y, self.x), self.core = place
        self.inner = (self.z + 1) // 2 == 1
        self.own, self.beside = self.z // 2 * 2, self.z + 1 - 2 * (self.z % 2)
        self.rest = (self.y, self.x) if last else (slice(None), slice(None))
        self.spread = (self.y, self.x) if last else ((0, 2), (0, 2))
        self.groups = [wires.group() for _ in landing]
        for group, ref in zip(self.groups, landing):
            group.count(ref)

    def push(self, at, chip, *where):
        source = self.held.at[(*where, slice(None), pl.ds(*self.columns))]
        self.wires.put(source, self.landing[at], device_at(chip, self.core, self.sizes), self.groups[at])

    def add(self, landing, *where, out=None):
        counts = list(landing.shape[:-2])
        rows, tall = landing.shape[-2], 32

        def step(i, carry):
            rest, index = i // (rows // tall), []
            for size in reversed(counts):
                index.insert(0, rest % size)
                rest = rest // size
            free, place = list(index), []
            for entry in where:
                if isinstance(entry, tuple):
                    place.append(entry[0] + free.pop(0))
                else:
                    place.append(entry)
            span = pl.ds(pl.multiple_of((i % (rows // tall)) * tall, tall), tall)
            place = (*place, span, pl.ds(*self.columns))
            sums = self.held[place].astype(F32) + landing[(*index, span, slice(None))].astype(F32)
            if out is None:
                self.held[place] = sums.astype(self.held.dtype)
            else:
                out[span, pl.ds(*self.columns)] = sums
            return carry

        lax.fori_loop(0, math.prod(counts) * (rows // tall), step, 0)

    def start(self):
        def outer():
            chip = (self.beside, self.y, self.x)
            self.push(0, chip, pl.ds(2 - self.own, 2), *self.rest)
            self.push(2, chip, self.beside, *self.rest)

        pl.when(jnp.logical_not(self.inner))(outer)
        self.wires.sent.count(self.landing[0])
        self.wires.sent.count(self.landing[2])

    def across(self):
        def middle():
            self.groups[0].wait()
            self.add(self.landing[0], (2 - self.own, 2), *self.spread)
            self.push(1, (3 - self.z, self.y, self.x), pl.ds(2 - self.own, 2), *self.rest)

        pl.when(self.inner)(middle)

    def back(self):
        def middle():
            self.groups[1].wait()
            self.add(self.landing[1], (self.own, 2), *self.spread)
            self.push(2, (self.beside, self.y, self.x), self.beside, *self.rest)

        pl.when(self.inner)(middle)

    def complete(self, out):
        self.groups[2].wait()
        self.add(self.landing[2], self.z, *self.spread, out=out)

    def second(self):
        self.complete(None)
        self.push(3, (self.z, 1 - self.y, self.x), self.z, 1 - self.y, slice(None))
        self.wires.sent.count(self.landing[3])

    def third(self):
        self.groups[3].wait()
        self.add(self.landing[3], self.z, self.y, (0, 2))
        self.push(4, (self.z, self.y, 1 - self.x), self.z, self.y, 1 - self.x)
        self.wires.sent.count(self.landing[4])

    def finish(self, out):
        self.groups[4].wait()
        self.add(self.landing[4], self.z, self.y, self.x, out=out)


def line_landing(rows, width, last):
    leads = ((2,), (2,), ()) if last else ((2, 2, 2), (2, 2, 2), (2, 2), (2,), ())
    return [pltpu.VMEM((*lead, rows, width), BF16) for lead in leads]


def landing_shapes(rows, colours, sizes, dtype, count=3):
    found = []
    for _, width, order in colours:
        stages = []
        for stage in range(count):
            free = [sizes[d] for d in range(3) if d not in order[:stage + 1]]
            stages.append(pltpu.VMEM((sizes[order[stage]] - 1, *free, rows, width), dtype))
        found.append(stages)
    return found


def stream(count, source, slots, sem, work):
    def fetch(i, slot):
        return pltpu.make_async_copy(source(i), slots(slot), sem.at[slot])

    fetch(0, 0).start()

    def step(i, carry):
        slot = lax.rem(i, 2)

        @pl.when(i + 1 < count)
        def _():
            fetch(i + 1, 1 - slot).start()

        fetch(i, slot).wait()
        work(i, slot)
        return carry

    lax.fori_loop(0, count, step, 0)


def columns_of(i, width):
    return pl.ds(pl.multiple_of(i * width, width), width)


def row_stats(values):
    mean = jnp.mean(values, axis=-1, keepdims=True)
    centred = values - mean
    rstd = lax.rsqrt(jnp.mean(centred * centred, axis=-1, keepdims=True) + ln_eps)
    return centred * rstd, rstd


SMALL, OUT, QKV, UP, DOWN = range(5)


class Box(dict):
    __getattr__ = dict.__getitem__


def leaves(tree):
    if isinstance(tree, dict):
        tree = list(tree.values())
    if isinstance(tree, list):
        return [leaf for part in tree for leaf in leaves(part)]
    return [] if tree is None else [tree]


def shape_of(tree):
    if isinstance(tree, dict):
        return {name: shape_of(part) for name, part in tree.items()}
    if isinstance(tree, list):
        return [shape_of(part) for part in tree]
    return tree is not None


def unpack(shape, refs):
    if isinstance(shape, dict):
        return {name: unpack(part, refs) for name, part in shape.items()}
    if isinstance(shape, list):
        return [unpack(part, refs) for part in shape]
    return next(refs) if shape else None


GATHER_ORDERS = ((0, 1, 2), (0, 2, 1), (2, 1, 0))
REDUCE_ORDERS = ((2, 1, 0), (1, 2, 0), (0, 1, 2))
SIZES = (4, 2, 2)
EARLY_TILES = 2
EARLY_UP = 8
LATE_TILES = 4
TILE = 512


def step_kernel(names, *refs):
    r = Box(unpack(names, iter(refs)))
    sizes = SIZES
    me = lax.axis_index("dp")
    coords, core = locate(me, sizes)
    place = (sizes, coords, core)
    partner = device_at(coords, 1 - core, sizes)
    rows, d = r.tokens.shape
    ff = r.low[UP].shape[1]
    heads2 = d // 128
    slots = rows // MB_ROWS

    others = neighbours(coords, core, sizes)
    barrier = pltpu.get_barrier_semaphore()
    for other in others:
        pl.semaphore_signal(barrier, inc=1, device_id=(other,), device_id_type=MESH_ID)
    loads = []
    for at, (source, target) in enumerate(
        [(r.own[which], r.fin[which]) for which in (OUT, QKV, UP, DOWN)]
        + [(r.cotangent, r.dy), (r.tokens_in, r.tokens)]
    ):
        copy = pltpu.make_async_copy(source, target, r.load_sem.at[at])
        copy.start()
        loads.append(copy)
    devices = math.prod(sizes) * 2
    per = devices * 128 // d
    block, narrow = r.block, 128 // per
    block[...] = jnp.zeros_like(block)
    for k in range(per):
        here = jnp.where(me % per == k, 1.0, 0.0)
        block[0:8, k * narrow:(k + 1) * narrow] = r.vectors[...] * here
    block[8:9, :] = r.bias_up[...]
    r.low[SMALL][...] = block[...].astype(BF16)

    def lower(at, which):
        loads[at].wait()
        r.low[which][...] = r.fin[which][...].astype(BF16)

    lower(0, OUT)
    pl.semaphore_wait(barrier, len(others))
    wires = Wires(r.send_sem, r.recv_sem, r.gauge, partner)

    def part(which, row_range, start, shares, relay, orders=GATHER_ORDERS):
        colours = split_colours(start, shares, orders)
        return Spread(r.full[which], r.low[which], row_range, colours, relay, place)

    short, tall = r.low[OUT].shape[0], r.low[DOWN].shape[0]
    all_short = (0, short)
    half, early, early_up = 3 * d // 2, EARLY_TILES * 128, EARLY_UP * 128
    mid_ff, end_ff = (ff - early_up) // 2, ff - early_up
    rest = in_thirds(d - early, 0)
    first = Chunk(wires, [part(SMALL, (0, 16), 0, (1,), False), part(OUT, all_short, 0, in_thirds(d, 0), False)])
    qkv0 = Chunk(wires, [part(QKV, all_short, 0, in_thirds(half, 0), True)])
    qkv1 = Chunk(wires, [part(QKV, all_short, half, in_thirds(half, 0), True)])
    up0 = Chunk(wires, [part(UP, all_short, 0, in_thirds(mid_ff, 0), True)])
    up1 = Chunk(wires, [part(UP, all_short, mid_ff, in_thirds(mid_ff, 0), True)])
    ahead_up = Chunk(wires, [part(UP, all_short, end_ff, (EARLY_UP,), True, GATHER_ORDERS[2:])])
    ahead = Chunk(wires, [part(DOWN, (0, tall), d - early, (EARLY_TILES,), True, GATHER_ORDERS[2:])])
    down0 = Chunk(wires, [part(DOWN, (0, tall // 2), 0, rest, True)])
    down1 = Chunk(wires, [part(DOWN, (tall // 2, tall // 2), 0, rest, True)])

    first.start(0)
    lower(2, UP)
    ahead_up.start(0)
    lower(1, QKV)
    qkv0.start(0)
    qkv1.start(0)
    lower(3, DOWN)
    ahead.start(0)
    mine = []
    for which in (SMALL, OUT, QKV, UP, DOWN):
        copy = pltpu.make_async_copy(r.low[which], r.full[which].at[(*coords, core)], r.mine_sem.at[which])
        copy.start()
        mine.append(copy)
    loads[4].wait()
    for slot in range(slots):
        span = pl.ds(slot * MB_ROWS, MB_ROWS)
        live = lax.broadcasted_iota(jnp.int32, (MB_ROWS, d), 0) < r.lengths[slot]
        r.dy[span, :] = jnp.where(live, r.dy[span, :].astype(F32), 0.0).astype(BF16)
    dy_swap = wires.swap(r.dy, r.dy_far)

    def norm_one(span):
        normed, _ = row_stats(r.tokens[span, :].astype(F32))
        r.da[span, :] = normed

    loads[5].wait()
    chunks(rows, 32, norm_one)
    for copy in mine:
        copy.wait()
    ahead_up.land(0)
    first.land(0)
    qkv0.land(0)
    up0.start(0)
    qkv1.land(0)
    qkv0.relay(1)
    first.land(1)
    up0.land(0)
    qkv0.land(1)
    up1.start(0)
    ahead.land(0)
    qkv1.relay(1)
    first.land(2)
    qkv1.land(1)
    up0.relay(1)
    qkv0.land(2)
    ahead_up.land(1)
    up1.land(0)
    up0.land(1)
    down0.start(0)
    up1.relay(1)
    qkv1.land(2)
    first.finish()
    ahead_up.land(2)
    qkv0.land(3)
    copy = pltpu.make_async_copy(r.full[SMALL], r.smalls, r.mine_sem.at[0])
    copy.start()
    copy.wait()
    flat = [(z, y, x, c) for z in range(sizes[0]) for y in range(sizes[1]) for x in range(sizes[2]) for c in range(2)]
    vec, bias = r.vec, r.bias
    for j in range(d // 128):
        total = 0.0
        for k in range(per):
            total = total + r.smalls[flat[j * per + k]].astype(F32)[0:8]
        vec[:, j * 128:(j + 1) * 128] = total
    for j in range(devices):
        bias[:, j * 128:(j + 1) * 128] = r.smalls[flat[j]].astype(F32)[8:9]

    def first_in(span):
        r.a[span, :] = (r.da[span, :] * vec[0:1, :] + vec[1:2, :]).astype(BF16)

    chunks(rows, 32, first_in)
    down0.land(0)
    up1.land(1)
    up0.land(2)
    down1.start(0)
    ahead.land(1)
    ahead_up.relay(3)
    down0.relay(1)
    qkv1.land(3)
    qkv0.finish()
    down1.land(0)
    down0.land(1)
    up1.land(2)
    qkv1.finish()

    def transpose_out(source, turned, far, low=0, high=16):
        block = turned.shape[2]
        group = max(1, 256 // (2 * block))

        def step(i, carry):
            value = source[:, columns_of(i, 2 * block * group)]
            flipped = value.astype(F32).T.astype(BF16)
            turned[pl.ds(i * group, group)] = flipped.reshape(group, 2, block, rows)
            return carry

        lax.fori_loop(low // group, high // group, step, 0)
        span = pl.ds(low, high - low)
        return wires.swap(turned.at[span, 1 - core], far.at[span])

    def tile_stream(which, low, high, work):
        full, slot = r.full[which], r.wide
        stream(
            (high - low) // TILE,
            lambda i: full.at[:, :, :, :, :, columns_of(i + low // TILE, TILE)],
            lambda s: slot.at[s],
            r.tile_sem,
            lambda i, s: work(i + low // TILE, slot[s].reshape(-1, TILE)),
        )

    def qkv_tile(i, tile):
        which = i * TILE // d
        values = nn(r.a[...], tile)
        shift = jnp.where(which == 0, 1.0, 0.0) * vec[2:3, columns_of(i % (d // TILE), TILE)] + jnp.where(
            which == 2, 1.0, 0.0
        ) * vec[3:4, columns_of(i % (d // TILE), TILE)]
        r.qkv[:, columns_of(i, TILE)] = (values + shift).astype(BF16)

    tile_stream(QKV, 0, 3 * d, qkv_tile)
    one_far = transpose_out(r.a, r.one_t, r.one_far)

    low_lane = lax.broadcasted_iota(jnp.int32, (MB_ROWS, 128), 1) < HEAD_DIM
    scale = 1.0 / math.sqrt(HEAD_DIM)

    def stacked(value):
        zero = jnp.zeros_like(value)
        return jnp.concatenate([jnp.where(low_lane, value, zero), jnp.where(low_lane, zero, value)], axis=0)

    def merged(value):
        return jnp.where(low_lane, value[:MB_ROWS], value[MB_ROWS:])

    def attend(p, carry):
        row = lax.broadcasted_iota(jnp.int32, (2 * MB_ROWS, 128), 0)
        dist = (row % MB_ROWS - lax.broadcasted_iota(jnp.int32, (2 * MB_ROWS, 128), 1)).astype(F32)
        head = (2 * p + row // MB_ROWS).astype(F32)
        alibi = jnp.where(dist >= 0, -jnp.exp2((head + 1.0) * (-8.0 / HEADS)) * dist, -1e30)
        for s in range(slots):
            span = pl.ds(s * MB_ROWS, MB_ROWS)
            q = r.qkv[span, columns_of(p, 128)]
            k = r.qkv[span, columns_of(p + heads2, 128)]
            v = r.qkv[span, columns_of(p + 2 * heads2, 128)]
            scores = nt(stacked(q), k) * scale + alibi
            top = jnp.max(scores, axis=-1, keepdims=True)
            grown = jnp.exp(scores - top)
            probs = grown / jnp.sum(grown, axis=-1, keepdims=True)
            r.probs[p * slots + s] = probs
            r.attn[span, columns_of(p, 128)] = merged(nn(probs.astype(BF16), v)).astype(BF16)
        return carry

    down1.relay(1)
    up0.land(3)
    ahead.land(2)
    ahead_up.land(3)
    lax.fori_loop(0, heads2 // 2, attend, 0)
    down1.land(1)
    down0.land(2)
    lax.fori_loop(heads2 // 2, heads2, attend, 0)
    attn_far = transpose_out(r.attn, r.attn_t, r.attn_far)

    def out_tile(i, tile):
        span = columns_of(i, TILE)
        r.h1[:, span] = r.tokens[:, span].astype(F32) + nn(r.attn[...], tile) + vec[4:5, span]

    tile_stream(OUT, 0, d, out_tile)
    ahead.relay(3)

    def second_in(span):
        normed, _ = row_stats(r.h1[span, :])
        r.a[span, :] = (normed * vec[5:6, :] + vec[6:7, :]).astype(BF16)

    chunks(rows, 32, second_in)
    two_far = transpose_out(r.a, r.two_t, r.two_far)

    def up_tile(i, tile):
        pre = nn(r.a[...], tile) + bias[:, columns_of(i, TILE)]
        value, slope = gelu_pair(pre)
        r.act[:, columns_of(i, TILE)] = value.astype(BF16)
        r.slope[:, columns_of(i, TILE)] = slope.astype(BF16)

    ahead_up.finish()
    tile_stream(UP, end_ff, ff, up_tile)
    up0.finish()
    down1.land(2)
    up1.land(3)
    tile_stream(UP, 0, mid_ff, up_tile)
    act_far0 = transpose_out(r.act, r.act_t, r.act_far, 0, mid_ff // 256)
    act_far2 = transpose_out(r.act, r.act_t, r.act_far, end_ff // 256, 16)
    up1.finish()
    tile_stream(UP, mid_ff, end_ff, up_tile)
    act_far1 = transpose_out(r.act, r.act_t, r.act_far, mid_ff // 256, end_ff // 256)
    down0.land(3)
    dy_swap.wait()
    act_far2.wait()
    act_far0.wait()
    act_far1.wait()

    reduces = [
        Reduce(wires, r.grad[which], span, landing, colours, place)
        for (which, span, colours), landing in zip(reduce_parts(short, tall, d, ff), r.landing)
    ]

    def weight_grad(which, turned, far, near_d, far_d, low, high):
        grad = r.grad[which]
        block = turned.shape[2]
        width = 512 if (high - low) % 512 == 0 and low % 512 == 0 else high - low
        total = (high - low) // width
        groups = max(1, 16 * block // 512)
        each = 16 // groups

        def step(i, carry):
            at, g = i // groups, i % groups
            left = turned[pl.ds(g * each, each), core].reshape(each * block, rows)
            other = far[pl.ds(g * each, each)].reshape(each * block, rows)
            span = pl.ds(pl.multiple_of(low + at * width, 128), width)
            value = nn(left, near_d[:, span]) + nn(other, far_d[:, span])
            value = value.astype(BF16)
            if groups == 1:
                grad[:, :, :, :, span] = value.reshape(*sizes, block, width)
            else:
                grad[g, :, :, :, span] = value.reshape(*sizes[1:], block, width)
            return carry

        assert groups in (1, sizes[0])
        lax.fori_loop(0, total * groups, step, 0)

    late = LATE_TILES * 128
    weight_grad(DOWN, r.act_t, r.act_far, r.dy, r.dy_far, d - late, d)
    line = LineReduce(wires, r.grad[DOWN], (d - late, late), r.line[0], place, False)
    line.start()
    weight_grad(DOWN, r.act_t, r.act_far, r.dy, r.dy_far, 0, d - late)
    reduces[0].start(0)
    reduces[1].start(0)
    ahead.land(3)
    down1.land(3)
    down0.finish()
    down1.finish()
    ahead.finish()

    sums = r.sums
    sums[...] = jnp.zeros_like(sums)
    acc = r.da

    def begin(span):
        acc[span, :] = r.h1[span, :] + vec[7:8, :]
        sums[7:8, :] += jnp.sum(r.dy[span, :].astype(F32), axis=0, keepdims=True)

    chunks(rows, 32, begin)

    def down_tile(i, s):
        tile = r.deep[s].reshape(-1, d)
        wide = tile.shape[0]
        span = columns_of(i, wide)
        acc[...] += nn(r.act[:, span], tile)
        d_pre = nt(r.dy[...], tile) * r.slope[:, span].astype(F32)
        r.bias_sum[:, span] = jnp.sum(d_pre, axis=0, keepdims=True)
        r.act[:, span] = d_pre.astype(BF16)

    full_down = r.full[DOWN]
    tiles = sizes[0] * sizes[1]

    def down_pass(low):
        stream(
            tiles // 2,
            lambda i: full_down.at[(i + low) // sizes[1], (i + low) % sizes[1]],
            lambda s: r.deep.at[s],
            r.tile_sem,
            lambda i, s: down_tile(i + low, s),
        )
        span = pl.ds(low * (ff // tiles), ff // 2)
        return wires.swap(r.act.at[:, span], r.pre_far.at[:, span])

    def advance(part, stage):
        reduces[part].land()
        reduces[part].add(stage - 1)
        reduces[part].start(stage)

    def complete(part, which):
        reduces[part].land()
        reduces[part].add(2, r.fin[which])

    down_line = LineReduce(wires, r.grad[DOWN], (0, d - late), r.line[1], place, True)
    up_lines = [
        LineReduce(wires, r.grad[UP], (at * ff // 2, ff // 2), r.line[2 + at], place, True) for at in range(2)
    ]

    def settle(part):
        reduces[part].land()
        reduces[part].add(1)

    pre_swap0 = down_pass(0)
    advance(0, 1)
    pre_swap1 = down_pass(tiles // 2)
    advance(1, 1)
    two_far.wait()
    pre_swap0.wait()
    weight_grad(UP, r.two_t, r.two_far, r.act, r.pre_far, 0, ff // 2)
    reduces[2].start(0)
    pre_swap1.wait()
    weight_grad(UP, r.two_t, r.two_far, r.act, r.pre_far, ff // 2, ff)
    reduces[3].start(0)
    r.a[...] = acc[...].astype(BF16)

    def row_stream(which, left):
        full, slot = r.full[which], r.flat
        width = full.shape[-1]

        def work(i, s):
            tile = slot[s, :, :, :, :, pl.ds(0, width)].reshape(-1, width)
            return nt(left[...], tile)

        def run(put):
            stream(
                sizes[0],
                lambda i: full.at[i],
                lambda s: slot.at[s, :, :, :, :, pl.ds(0, width)],
                r.tile_sem,
                lambda i, s: put(i, work(i, s)),
            )

        return run

    def put_da(i, value):
        r.da[:, columns_of(i, value.shape[1])] = value

    row_stream(UP, r.act)(put_da)

    line.across()

    def norm_two_back(span):
        normed, rstd = row_stats(r.h1[span, :])
        da = r.da[span, :]
        sums[5:6, :] += jnp.sum(da * normed, axis=0, keepdims=True)
        sums[6:7, :] += jnp.sum(da, axis=0, keepdims=True)
        d_h1 = r.dy[span, :].astype(F32) + norm_back(da, normed, rstd, vec[5:6, :])
        sums[4:5, :] += jnp.sum(d_h1, axis=0, keepdims=True)
        r.h1[span, :] = d_h1
        r.d_mid[span, :] = d_h1.astype(BF16)

    chunks(rows, 32, norm_two_back)
    stores = []

    def keep(source, target):
        copy = pltpu.make_async_copy(source, target, r.store_sem.at[len(stores)])
        copy.start()
        stores.append(copy)

    keep(r.a, r.output)
    mid_swap = wires.swap(r.d_mid, r.mid_far)

    def put_attn(i, value):
        r.d_attn[:, columns_of(i, value.shape[1])] = value.astype(BF16)

    row_stream(OUT, r.d_mid)(put_attn)

    advance(2, 1)
    settle(0)
    settle(1)
    down_line.start()
    attn_far.wait()
    mid_swap.wait()
    weight_grad(OUT, r.attn_t, r.attn_far, r.d_mid, r.mid_far, 0, d)

    def attend_back(p, carry):
        span_p = columns_of(p, 128)
        d_bq = jnp.zeros((1, 128), F32)
        d_bv = jnp.zeros((1, 128), F32)
        for s in range(slots):
            span = pl.ds(s * MB_ROWS, MB_ROWS)
            q = stacked(r.qkv[span, span_p])
            k = r.qkv[span, columns_of(p + heads2, 128)]
            v = r.qkv[span, columns_of(p + 2 * heads2, 128)]
            do = r.d_attn[span, span_p]
            probs = r.probs[p * slots + s]
            both = stacked(do)
            d_v = tn(probs.astype(BF16), both)
            d_probs = nt(both, v)
            weighed = do.astype(F32) * r.attn[span, span_p].astype(F32)
            delta = jnp.sum(stacked(weighed), axis=-1, keepdims=True)
            d_scores = (probs * (d_probs - delta)).astype(BF16)
            d_q = merged(nn(d_scores, k)) * scale
            d_k = tn(d_scores, q) * scale
            d_bq += jnp.sum(d_q, axis=0, keepdims=True)
            d_bv += jnp.sum(d_v, axis=0, keepdims=True)
            r.qkv[span, span_p] = d_q.astype(BF16)
            r.qkv[span, columns_of(p + heads2, 128)] = d_k.astype(BF16)
            r.qkv[span, columns_of(p + 2 * heads2, 128)] = d_v.astype(BF16)
        sums[2:3, span_p] = d_bq
        sums[3:4, span_p] = d_bv
        return carry

    lax.fori_loop(0, heads2 // 2, attend_back, 0)
    advance(3, 1)
    reduces[4].start(0)
    lax.fori_loop(heads2 // 2, heads2, attend_back, 0)
    qkv_swap = wires.swap(r.qkv, r.qkv_far)
    down_line.across()
    row_stream(QKV, r.qkv)(put_da)
    settle(2)
    up_lines[0].start()
    one_far.wait()
    qkv_swap.wait()
    weight_grad(QKV, r.one_t, r.one_far, r.qkv, r.qkv_far, 0, d)
    reduces[5].start(0)
    weight_grad(QKV, r.one_t, r.one_far, r.qkv, r.qkv_far, d, 2 * d)
    reduces[6].start(0)
    settle(3)
    up_lines[1].start()
    weight_grad(QKV, r.one_t, r.one_far, r.qkv, r.qkv_far, 2 * d, 3 * d)
    line.back()

    def norm_one_back(span):
        normed, rstd = row_stats(r.tokens[span, :].astype(F32))
        da = r.da[span, :]
        sums[0:1, :] += jnp.sum(da * normed, axis=0, keepdims=True)
        sums[1:2, :] += jnp.sum(da, axis=0, keepdims=True)
        r.h1[span, :] = r.h1[span, :] + norm_back(da, normed, rstd, vec[0:1, :])

    chunks(rows, 32, norm_one_back)
    down_line.back()

    bundle = r.bundle
    for j in range(devices):
        at = (j // per) * 128
        bundle[flat[j]] = jnp.concatenate(
            [sums[:, at:at + 128], jnp.broadcast_to(r.bias_sum[:, j * 128:(j + 1) * 128], (8, 128))], axis=0
        )
    tiny_swap = wires.swap(bundle.at[:, :, :, 1 - core], r.tiny_far)
    tiny = reduces[8]
    keep(r.h1, r.input_grad)
    advance(4, 1)
    up_lines[0].across()
    tiny_swap.wait()
    r.grad[SMALL][...] = bundle[:, :, :, core] + r.tiny_far[...]
    tiny.start(0)
    advance(5, 1)
    reduces[7].start(0)
    up_lines[1].across()
    down_line.complete(r.fin[DOWN])
    advance(6, 1)
    up_lines[0].back()
    advance(4, 2)
    advance(5, 2)
    up_lines[1].back()
    advance(7, 1)
    line.second()
    advance(6, 2)
    up_lines[0].complete(r.fin[UP])
    advance(7, 2)
    advance(8, 1)
    line.third()
    advance(8, 2)
    up_lines[1].complete(r.fin[UP])
    complete(4, OUT)
    keep(r.fin[UP], r.final[UP])
    complete(5, QKV)
    keep(r.fin[OUT], r.final[OUT])
    complete(6, QKV)
    line.finish(r.fin[DOWN])
    keep(r.fin[DOWN], r.final[DOWN])
    complete(8, SMALL)
    keep(r.fin[SMALL], r.final[SMALL])
    complete(7, QKV)
    keep(r.fin[QKV], r.final[QKV])
    for copy in stores:
        copy.wait()
    wires.drain()


def reduce_parts(short, tall, d, ff):
    rows, half_ff = (0, short), ff // 2

    def colours(start, width, last):
        return split_colours(start, in_thirds(width, last), REDUCE_ORDERS)

    return [
        (DOWN, (0, tall // 2), colours(0, d - LATE_TILES * 128, 0)),
        (DOWN, (tall // 2, tall // 2), colours(0, d - LATE_TILES * 128, 0)),
        (UP, rows, colours(0, half_ff, 0)),
        (UP, rows, colours(half_ff, half_ff, 0)),
        (OUT, rows, colours(0, d, 0)),
        (QKV, rows, colours(0, d, 0)),
        (QKV, rows, colours(d, d, 0)),
        (QKV, rows, colours(2 * d, d, 0)),
        (SMALL, (0, 16), [(0, 128, (2, 1, 0))]),
    ]


def fused_step(tokens, cotangent, lengths, vectors, bias_up, w_qkv, w_out, w_up, w_down):
    sizes = SIZES
    rows, d = tokens.shape
    ff = w_up.shape[1]
    short, tall = w_out.shape[0], w_down.shape[0]
    heads2 = d // 128
    slots = rows // MB_ROWS
    whole = lambda s: jax.ShapeDtypeStruct((*sizes, 2, *s), BF16)
    like = jax.ShapeDtypeStruct
    wide = ((16, 128), (short, d), (short, 3 * d), (short, ff), (tall, d))
    v = pltpu.VMEM
    turned, across = v((16, 2, short, rows), BF16), v((16, short, rows), BF16)
    flat, double = v((rows, d), BF16), v((rows, d), F32)
    near = dict(vectors=vectors, bias_up=bias_up)
    distant = dict(tokens_in=tokens, cotangent=cotangent, own=[None, w_out, w_qkv, w_up, w_down])
    results = dict(
        full=[whole(s) for s in wide], gauge=like((180_224, 128), BF16),
        output=like((rows, d), BF16), input_grad=like((rows, d), F32), final=[like(s, F32) for s in wide],
    )
    parts = reduce_parts(short, tall, d, ff)
    scratch = dict(
        low=[v(s, BF16) for s in wide], block=v((16, 128), F32), dy=flat, tokens=flat,
        fin=[v(s, F32) for s in wide],
        smalls=v((*sizes, 2, 16, 128), BF16), vec=v((8, d), F32), bias=v((1, ff), F32),
        dy_far=flat, da=double, a=flat, qkv=v((rows, 3 * d), BF16), qkv_far=v((rows, 3 * d), BF16),
        probs=v((heads2 * slots, 2 * MB_ROWS, 128), F32), attn=flat, h1=double,
        act=v((rows, ff), BF16), slope=v((rows, ff), BF16), pre_far=v((rows, ff), BF16),
        d_mid=flat, mid_far=flat, d_attn=flat,
        one_t=turned, one_far=across, attn_t=turned, attn_far=across, two_t=turned, two_far=across,
        act_t=v((16, 2, tall, rows), BF16), act_far=v((16, tall, rows), BF16),
        wide=v((2, *sizes, 2, short, TILE), BF16), deep=v((2, sizes[2], 2, tall, d), BF16),
        flat=v((2, *sizes[1:], 2, short, ff), BF16),
        grad=[v((*sizes, *s), BF16 if at else F32) for at, s in enumerate(wide)],
        sums=v((8, d), F32), bias_sum=v((1, ff), F32),
        bundle=v((*sizes, 2, 16, 128), F32), tiny_far=v((*sizes, 16, 128), F32),
        landing=[
            landing_shapes(span[1], colours, sizes, BF16 if which else F32, 2 if which in (UP, DOWN) else 3)
            for which, span, colours in parts
        ],
        line=[
            line_landing(tall, LATE_TILES * 128, False), line_landing(tall, d - LATE_TILES * 128, True),
            line_landing(short, ff // 2, True), line_landing(short, ff // 2, True),
        ],
        send_sem=pltpu.SemaphoreType.DMA((2,)), recv_sem=pltpu.SemaphoreType.DMA((97,)),
        mine_sem=pltpu.SemaphoreType.DMA((5,)), tile_sem=pltpu.SemaphoreType.DMA((2,)),
        load_sem=pltpu.SemaphoreType.DMA((6,)), store_sem=pltpu.SemaphoreType.DMA((7,)),
    )
    names = {**dict(lengths=lengths), **near, **distant, **results, **scratch}
    found = pl.pallas_call(
        functools.partial(step_kernel, shape_of(names)),
        out_shape=leaves(results),
        in_specs=[pl.BlockSpec(memory_space=pltpu.SMEM)]
        + [pl.BlockSpec(memory_space=v)] * len(leaves(near))
        + [pl.BlockSpec(memory_space=pltpu.HBM)] * len(leaves(distant)),
        out_specs=[pl.BlockSpec(memory_space=pltpu.HBM)] * len(leaves(results)),
        scratch_shapes=leaves(scratch),
        compiler_params=pltpu.CompilerParams(
            collective_id=1, has_side_effects=True, vmem_limit_bytes=67_000_000
        ),
        name="fused_step",
    )(lengths, *leaves(near), *leaves(distant))
    return Box(unpack(shape_of(results), iter(found)))


def adam_kernel(shape, *refs):
    r = Box(unpack(shape, iter(refs)))
    me = lax.axis_index("dp")
    count = float(STEP)

    def put(at, param, first, second, grad):
        update, new_first, new_second = adamw(param, (first, second), grad, count)
        r.grads[at][...] = grad
        r.updates[at][...] = update
        r.firsts[at][...] = new_first
        r.seconds[at][...] = new_second

    for at in range(2, 6):
        put(at, r.params[at][...], r.moments[at][0], r.moments[at][1], r.final[at - 1][...])
    r.output[...] = r.early_output[...]
    r.input_grad[...] = r.early_grad[...]

    @pl.when(pl.program_id(0) == 0)
    def _():
        narrow = r.params[0].shape[1]
        per = 128 // narrow
        grad = jnp.zeros((8, narrow), F32)
        for k in range(per):
            grad = grad + jnp.where(me % per == k, 1.0, 0.0) * r.final[SMALL][0:8, k * narrow:(k + 1) * narrow]
        put(0, r.params[0][...], r.moments[0][0], r.moments[0][1], grad)
        put(1, r.params[1][...], r.moments[1][0:1], r.moments[1][1:2], r.final[SMALL][8:9, :])


def adam(found, params, moments):
    steps = 1

    def whole(s):
        return pl.BlockSpec(s, lambda i: (0,) * len(s))

    def cut(s):
        return pl.BlockSpec((*s[:-1], s[-1] // steps), lambda i: (0,) * (len(s) - 1) + (i,))

    def tall(s):
        return pl.BlockSpec((s[0] // steps, s[1]), lambda i: (i, 0))

    def each(make):
        return [make(p.shape) for p in params]

    like = jax.ShapeDtypeStruct
    outs = each(lambda s: like(s, F32))
    specs = [whole(p.shape) if at < 2 else cut(p.shape) for at, p in enumerate(params)]
    moment_specs = [whole(m.shape) if at < 2 else cut(m.shape) for at, m in enumerate(moments)]
    inputs = dict(
        params=list(params), moments=list(moments), final=found.final,
        early_output=found.output, early_grad=found.input_grad,
    )
    input_specs = dict(
        params=specs, moments=moment_specs, final=[whole((16, 128)), *specs[2:]],
        early_output=tall(found.output.shape), early_grad=tall(found.input_grad.shape),
    )
    results = dict(
        grads=outs, updates=outs, firsts=outs, seconds=outs,
        output=like(found.output.shape, BF16), input_grad=like(found.input_grad.shape, F32),
    )
    result_specs = dict(
        grads=specs, updates=specs, firsts=specs, seconds=specs,
        output=tall(found.output.shape), input_grad=tall(found.input_grad.shape),
    )
    shape = shape_of({**inputs, **results})
    done = pl.pallas_call(
        functools.partial(adam_kernel, shape),
        grid=(steps,),
        out_shape=leaves(results),
        in_specs=leaves(input_specs),
        out_specs=leaves(result_specs),
        compiler_params=pltpu.CompilerParams(vmem_limit_bytes=67_000_000),
        name="adam",
    )(*leaves(inputs))
    return Box(unpack(shape_of(results), iter(done)))


def general_body(
    tokens,
    cotangent,
    lengths,
    vectors,
    bias_up,
    w_qkv,
    w_out,
    w_up,
    w_down,
    mom_vectors,
    mom_bias_up,
    mom_qkv,
    mom_out,
    mom_up,
    mom_down,
):
    params = (vectors, bias_up, w_qkv, w_out, w_up, w_down)
    moments = (mom_vectors, mom_bias_up, mom_qkv, mom_out, mom_up, mom_down)
    me = lax.axis_index("dp")
    count = lax.axis_size("dp")
    small, full_out, full_qkv, full_up, full_down = gather_all(
        [small_block(vectors, bias_up, me), w_out, w_qkv, w_up, w_down], count
    )
    vec_low, bias_low = small_parts(small, vectors, bias_up)
    weights = (
        vec_low,
        bias_low,
        full_qkv.reshape(-1, w_qkv.shape[1]),
        full_out.reshape(-1, w_out.shape[1]),
        full_up.reshape(-1, w_up.shape[1]),
        full_down.reshape(-1, w_down.shape[1]),
    )
    alibi = alibi_bias(MB_ROWS)
    place = jnp.arange(MB_ROWS)
    owned = tuple((jnp.zeros(p.shape, jnp.float32) for p in params))
    summed = None
    out_list = []
    dx_list = []
    for micro in range(MICRO):
        x_rows = tokens[micro * MB_ROWS : (micro + 1) * MB_ROWS]
        live = place < lengths[micro]
        grad_rows = jnp.where(
            live[:, None],
            cotangent[micro * MB_ROWS : (micro + 1) * MB_ROWS],
            jnp.zeros((), jnp.bfloat16),
        )
        out, saved = forward_block(x_rows, weights, alibi)
        d_x, grads = backward_block(saved, grad_rows, weights, alibi)
        out_list.append(out)
        dx_list.append(d_x)
        summed = grads if summed is None else tuple((a + b for a, b in zip(summed, grads)))
    owned = (
        lax.psum_scatter(summed[0], "dp", scatter_dimension=1, tiled=True),
        lax.psum_scatter(summed[1], "dp", scatter_dimension=0, tiled=True),
        lax.psum_scatter(summed[2], "dp", scatter_dimension=0, tiled=True),
        lax.psum_scatter(summed[3], "dp", scatter_dimension=0, tiled=True),
        lax.psum_scatter(summed[4], "dp", scatter_dimension=0, tiled=True),
        lax.psum_scatter(summed[5], "dp", scatter_dimension=0, tiled=True),
    )
    count = float(STEP)
    news = [adamw(p, m, g, count) for p, m, g in zip(params, moments, owned)]
    output = jnp.concatenate(out_list, axis=0)
    input_grad = jnp.concatenate(dx_list, axis=0)
    return (
        output,
        input_grad,
        owned[0],
        owned[1],
        owned[2],
        owned[3],
        owned[4],
        owned[5],
        news[0][0],
        news[1][0],
        news[2][0],
        news[3][0],
        news[4][0],
        news[5][0],
        news[0][1],
        news[1][1],
        news[2][1],
        news[3][1],
        news[4][1],
        news[5][1],
        news[0][2],
        news[1][2],
        news[2][2],
        news[3][2],
        news[4][2],
        news[5][2],
    )


def body(
    tokens, cotangent, lengths, vectors, bias_up, w_qkv, w_out, w_up, w_down,
    mom_vectors, mom_bias_up, mom_qkv, mom_out, mom_up, mom_down,
):
    if grid_of(lax.axis_size("dp")) != SIZES:
        return general_body(
            tokens, cotangent, lengths, vectors, bias_up, w_qkv, w_out, w_up, w_down,
            mom_vectors, mom_bias_up, mom_qkv, mom_out, mom_up, mom_down,
        )
    span = bias_up.shape[0]
    found = fused_step(tokens, cotangent, lengths, vectors, bias_up.reshape(1, span), w_qkv, w_out, w_up, w_down)
    found.final[OUT], found.final[QKV] = found.final[QKV], found.final[OUT]
    done = adam(
        found,
        (vectors, bias_up.reshape(1, span), w_qkv, w_out, w_up, w_down),
        (mom_vectors, mom_bias_up, mom_qkv, mom_out, mom_up, mom_down),
    )

    def six(arrays):
        return (arrays[0], arrays[1].reshape(span), *arrays[2:])

    return (
        done.output, done.input_grad, *six(done.grads), *six(done.updates), *six(done.firsts), *six(done.seconds),
    )


def solution(mesh):
    in_specs = (
        P("dp", None),
        P("dp", None),
        P("dp"),
        P(None, "dp"),
        P("dp"),
        P("dp", None),
        P("dp", None),
        P("dp", None),
        P("dp", None),
        P(None, None, "dp"),
        P(None, "dp"),
        P(None, "dp", None),
        P(None, "dp", None),
        P(None, "dp", None),
        P(None, "dp", None),
    )
    out_specs = (
        P("dp", None),
        P("dp", None),
        P(None, "dp"),
        P("dp"),
        P("dp", None),
        P("dp", None),
        P("dp", None),
        P("dp", None),
        P(None, "dp"),
        P("dp"),
        P("dp", None),
        P("dp", None),
        P("dp", None),
        P("dp", None),
        P(None, "dp"),
        P("dp"),
        P("dp", None),
        P("dp", None),
        P("dp", None),
        P("dp", None),
        P(None, "dp"),
        P("dp"),
        P("dp", None),
        P("dp", None),
        P("dp", None),
        P("dp", None),
    )
    return jax.shard_map(body, mesh=mesh, in_specs=in_specs, out_specs=out_specs, check_vma=False)
```
